8 devices in a mesh: dp: 1 (over z), fsdp: 8 (over y, x, core).
Axes of the slice: x: 2, y: 2, z: 1, core: 2. Of those that a mesh axis runs over, the one named last changes fastest.
Arguments:
- hidden: bfloat16 [8, 128, 3072], P(('dp', 'fsdp'))
- attn_norm: bfloat16 [2, 3072], P(None, 'fsdp')
- w_q: bfloat16 [2, 3072, 24, 128], P(None, 'fsdp')
- w_k: bfloat16 [2, 3072, 8, 128], P(None, 'fsdp')
- w_v: bfloat16 [2, 3072, 8, 128], P(None, 'fsdp')
- w_o: bfloat16 [2, 3072, 3072], P(None, 'fsdp')
- mlp_norm: bfloat16 [2, 3072], P(None, 'fsdp')
- w_gate: bfloat16 [2, 3072, 8192], P(None, 'fsdp')
- w_up: bfloat16 [2, 3072, 8192], P(None, 'fsdp')
- w_down: bfloat16 [2, 8192, 3072], P(None, 'fsdp')
Outputs:
- output: bfloat16 [8, 128, 3072], P(('dp', 'fsdp'))
All inputs are finite; a program needn't handle non-finite values.
Results may differ from the reference program's by a relative error of at most 0.02.
Values are sent between devices in bfloat16 or wider.
A program may use at most 1 GiB of HBM per device.

```python
import jax
import jax.numpy as jnp
from jax import lax

MODEL_DIM = 3072
HEADS = 24
KV_HEADS = 8
HEAD_DIM = 128
FFN_DIM = 8192
SEQ_LEN = 128
BATCH_DEV = 1
FSDP_SIZE = 8
LAYERS = 2

GROUP_SEQS = FSDP_SIZE * BATCH_DEV
ROPE_THETA = 500000.0
NORM_EPS = 1e-5


def setup_inputs(seed: int = 0, part: int = 0) -> dict:
    weight_keys = jax.random.split(jax.random.key(seed), 9)
    seq_key = jax.random.fold_in(jax.random.key(seed + 1), part)
    qo_width = HEADS * HEAD_DIM

    def gain_vector(rng_key):
        return (1.0 + 0.25 * jax.random.normal(rng_key, (LAYERS, MODEL_DIM), jnp.float32)).astype(jnp.bfloat16)

    def weight(rng_key, shape, fan_in, gain):
        scale = gain * fan_in ** -0.5
        return (scale * jax.random.normal(rng_key, shape, jnp.float32)).astype(jnp.bfloat16)

    hidden = (0.5 * jax.random.normal(seq_key, (GROUP_SEQS, SEQ_LEN, MODEL_DIM), jnp.float32)).astype(jnp.bfloat16)
    return {
        "hidden": hidden,
        "attn_norm": gain_vector(weight_keys[0]),
        "w_q": weight(weight_keys[1], (LAYERS, MODEL_DIM, HEADS, HEAD_DIM), MODEL_DIM, 1.5),
        "w_k": weight(weight_keys[2], (LAYERS, MODEL_DIM, KV_HEADS, HEAD_DIM), MODEL_DIM, 1.5),
        "w_v": weight(weight_keys[3], (LAYERS, MODEL_DIM, KV_HEADS, HEAD_DIM), MODEL_DIM, 1.0),
        "w_o": weight(weight_keys[4], (LAYERS, qo_width, MODEL_DIM), qo_width, 1.5),
        "mlp_norm": gain_vector(weight_keys[5]),
        "w_gate": weight(weight_keys[6], (LAYERS, MODEL_DIM, FFN_DIM), MODEL_DIM, 1.0),
        "w_up": weight(weight_keys[7], (LAYERS, MODEL_DIM, FFN_DIM), MODEL_DIM, 1.0),
        "w_down": weight(weight_keys[8], (LAYERS, FFN_DIM, MODEL_DIM), FFN_DIM, 1.0),
    }


def rms_norm(hidden, gain):
    wide_hidden = hidden.astype(jnp.float32)
    inv_rms = lax.rsqrt(jnp.mean(wide_hidden * wide_hidden, axis=-1, keepdims=True) + NORM_EPS)
    return (wide_hidden * inv_rms * gain.astype(jnp.float32)).astype(jnp.bfloat16)


def rope_tables(seq_len, head_dim):
    half = head_dim // 2
    inv_freq = jnp.power(ROPE_THETA, -(jnp.arange(half, dtype=jnp.float32) * 2.0 / head_dim))
    angles = jnp.arange(seq_len, dtype=jnp.float32)[:, None] * inv_freq[None, :]
    return jnp.cos(angles)[:, None, :], jnp.sin(angles)[:, None, :]


def apply_rope(proj, cos_table, sin_table):
    half = proj.shape[-1] // 2
    first = proj[..., :half]
    second = proj[..., half:]
    rotated = jnp.concatenate([first * cos_table - second * sin_table, second * cos_table + first * sin_table], axis=-1)
    return rotated.astype(jnp.bfloat16)


def decoder_layer(seq_hidden, weights, cos_table, sin_table):
    attn_gain, w_q, w_k, w_v, w_o, mlp_gain, w_gate, w_up, w_down = weights
    group = HEADS // KV_HEADS
    normed = rms_norm(seq_hidden, attn_gain)
    q_proj = jnp.dot(normed, w_q.reshape(MODEL_DIM, HEADS * HEAD_DIM), preferred_element_type=jnp.float32)
    k_proj = jnp.dot(normed, w_k.reshape(MODEL_DIM, KV_HEADS * HEAD_DIM), preferred_element_type=jnp.float32)
    v_proj = jnp.dot(normed, w_v.reshape(MODEL_DIM, KV_HEADS * HEAD_DIM), preferred_element_type=jnp.float32)
    queries = apply_rope(q_proj.reshape(SEQ_LEN, HEADS, HEAD_DIM), cos_table, sin_table)
    keys_rot = apply_rope(k_proj.reshape(SEQ_LEN, KV_HEADS, HEAD_DIM), cos_table, sin_table)
    values = v_proj.astype(jnp.bfloat16).reshape(SEQ_LEN, KV_HEADS, HEAD_DIM)
    q_grouped = queries.reshape(SEQ_LEN, KV_HEADS, group, HEAD_DIM)
    scores = jnp.einsum("qkgd,skd->kgqs", q_grouped.astype(jnp.float32), keys_rot.astype(jnp.float32)) * HEAD_DIM ** -0.5
    causal = jnp.arange(SEQ_LEN)[:, None] >= jnp.arange(SEQ_LEN)[None, :]
    probs = jax.nn.softmax(jnp.where(causal, scores, -jnp.inf), axis=-1).astype(jnp.bfloat16)
    attended = jnp.einsum("kgqs,skd->qkgd", probs.astype(jnp.float32), values.astype(jnp.float32)).astype(jnp.bfloat16)
    attended = attended.reshape(SEQ_LEN, HEADS * HEAD_DIM)
    after_attn = (seq_hidden.astype(jnp.float32) + jnp.dot(attended, w_o, preferred_element_type=jnp.float32)).astype(jnp.bfloat16)
    mlp_in = rms_norm(after_attn, mlp_gain)
    gate_proj = jnp.dot(mlp_in, w_gate, preferred_element_type=jnp.float32).astype(jnp.bfloat16)
    up_proj = jnp.dot(mlp_in, w_up, preferred_element_type=jnp.float32).astype(jnp.bfloat16)
    gated = (jax.nn.silu(gate_proj.astype(jnp.float32)) * up_proj.astype(jnp.float32)).astype(jnp.bfloat16)
    return (after_attn.astype(jnp.float32) + jnp.dot(gated, w_down, preferred_element_type=jnp.float32)).astype(jnp.bfloat16)


def reference(hidden, attn_norm, w_q, w_k, w_v, w_o, mlp_norm, w_gate, w_up, w_down):
    cos_table, sin_table = rope_tables(SEQ_LEN, HEAD_DIM)
    stacked = (attn_norm, w_q, w_k, w_v, w_o, mlp_norm, w_gate, w_up, w_down)

    def one_sequence(seq_hidden):
        def layer_step(carry, weights):
            return decoder_layer(carry, weights, cos_table, sin_table), None

        final, unused = lax.scan(layer_step, seq_hidden, stacked)
        return final

    return lax.map(one_sequence, hidden)
```

```python
import functools

import jax
import jax.numpy as jnp
import numpy as np
from jax import lax
from jax.experimental import pallas as pl
from jax.experimental.pallas import tpu as pltpu
from jax.sharding import PartitionSpec as P

ROPE_THETA = 500000.0
NORM_EPS = 1e-5
MESH = pl.DeviceIdType.MESH
F32 = jnp.float32
BF16 = jnp.bfloat16

DEV = 8
CHIPS = 4
SEQ = 128
DIM = 3072
HALF = DIM // 2
ROWS = DIM // DEV
HD = 128
QH = 3
QCOLS = QH * HD
QKV = QCOLS + 2 * HD
FFN = 8192
FCOLS = FFN // DEV
NCH = 4
CW = FCOLS // NCH
LAYERS = 2


def rope_tables():
    half = HD // 2
    inv_freq = np.power(np.float32(ROPE_THETA), -(np.arange(half, dtype=np.float32) * np.float32(2.0) / np.float32(HD)))
    angles = (np.arange(SEQ, dtype=np.float32)[:, None] * inv_freq.astype(np.float32)[None, :]).astype(np.float64)
    cos, sin = np.cos(angles).astype(np.float32), np.sin(angles).astype(np.float32)
    return np.concatenate([cos, cos], axis=1), np.concatenate([-sin, sin], axis=1)


def body(x_in, g_in, cos_in, sin_in, wqkv_in, wo_in, wg_in, wu_in, wd_in,
         out, land_qkv, land_gu,
         xb, u, part, rm, r1, r2, wqkv, wo, wd, wgu, qb, kb, vb, ob, zb, gains,
         ss_qkv, rs_qkv, ss_gu, rs_gu, s_gain, l_sem, ld_sem,
         ag_s, ag_r, mt_s, mt_r, r1_s, r1_r, r2_s, r2_r):
    me = lax.axis_index("fsdp")
    c = me % 2
    cx = (me // 2) % 2
    cy = me // 4
    chip = me // 2

    def dev(fy, fx, fc):
        yy = 1 - cy if fy else cy
        xx = 1 - cx if fx else cx
        cc = 1 - c if fc else c
        return yy * 4 + xx * 2 + cc

    mate, xn, yn = dev(0, 0, 1), dev(0, 1, 0), dev(1, 0, 0)
    chip_x, chip_y, chip_d = xn // 2, yn // 2, dev(1, 1, 0) // 2
    flips = ((1, 1, 0), (1, 1, 1), (0, 1, 0), (1, 0, 0), (0, 1, 1), (1, 0, 1), (0, 0, 1))

    def remote(src, dst, ssem, rsem, target):
        return pltpu.make_async_remote_copy(src, dst, ssem, rsem, device_id={"fsdp": target}, device_id_type=MESH)

    def bytes_wait(ref, sem):
        pltpu.make_async_copy(ref, ref, sem).wait()

    barrier = pltpu.get_barrier_semaphore()
    for f in flips:
        pl.semaphore_signal(barrier, inc=1, device_id={"fsdp": dev(*f)}, device_id_type=MESH)
    pl.semaphore_wait(barrier, DEV - 1)

    def send_qkv(l):
        for f in flips:
            e = dev(*f)
            remote(wqkv_in.at[l, :, pl.ds(pl.multiple_of(e * QKV, 128), QKV)],
                   land_qkv.at[l, pl.ds(pl.multiple_of(me * ROWS, ROWS), ROWS), :],
                   ss_qkv.at[l], rs_qkv.at[l], e).start()

    def send_gu(l, n):
        for f in flips:
            e = dev(*f)
            cols = pl.ds(pl.multiple_of(e * FCOLS + n * CW, 128), CW)
            rows = pl.ds(pl.multiple_of(me * ROWS, ROWS), ROWS)
            remote(wg_in.at[l, :, cols], land_gu.at[l, n, rows, pl.ds(0, CW)], ss_gu.at[l, n], rs_gu.at[l, n], e).start()
            remote(wu_in.at[l, :, cols], land_gu.at[l, n, rows, pl.ds(CW, CW)], ss_gu.at[l, n], rs_gu.at[l, n], e).start()

    OTHER = (DEV - 1) * ROWS

    def load_qkv(l):
        for f in flips:
            rows = pl.ds(pl.multiple_of(dev(*f) * ROWS, ROWS), ROWS)
            pltpu.make_async_copy(land_qkv.at[l, rows, :], wqkv.at[rows, :], ld_sem.at[0]).start()
        mine = pl.ds(pl.multiple_of(me * ROWS, ROWS), ROWS)
        pltpu.make_async_copy(wqkv_in.at[l, :, pl.ds(pl.multiple_of(me * QKV, 128), QKV)], wqkv.at[mine, :], ld_sem.at[0]).start()

    def load_gu(l, n):
        slot = n % 2
        for f in flips:
            rows = pl.ds(pl.multiple_of(dev(*f) * ROWS, ROWS), ROWS)
            pltpu.make_async_copy(land_gu.at[l, n, rows, :], wgu.at[slot, rows, :], ld_sem.at[1 + slot]).start()
        mine = pl.ds(pl.multiple_of(me * ROWS, ROWS), ROWS)
        cols = pl.ds(pl.multiple_of(me * FCOLS + n * CW, 128), CW)
        pltpu.make_async_copy(wg_in.at[l, :, cols], wgu.at[slot, mine, pl.ds(0, CW)], ld_sem.at[1 + slot]).start()
        pltpu.make_async_copy(wu_in.at[l, :, cols], wgu.at[slot, mine, pl.ds(CW, CW)], ld_sem.at[1 + slot]).start()

    my_slot = c * CHIPS + chip

    def norm(row):
        def one(i, carry):
            rows = pl.ds(pl.multiple_of(i * 16, 16), 16)
            wide = xb[rows, :].astype(F32)
            inv = lax.rsqrt(jnp.mean(wide * wide, axis=-1, keepdims=True) + NORM_EPS)
            for s in range(DEV):
                cols = slice(s * ROWS, (s + 1) * ROWS)
                g = gains[s, pl.ds(row, 1), :]
                u[my_slot, rows, cols] = (wide[:, cols] * inv * g).astype(BF16)
            return carry
        lax.fori_loop(0, SEQ // 16, one, 0)

    A, B = pl.ds(0, HALF), pl.ds(HALF, HALF)

    def u_copy(slot, cols, k, target):
        ref = u.at[slot, :, cols] if cols is not None else u.at[slot]
        return remote(ref, ref, ag_s.at[k], ag_r.at[k], target)

    def gather_start():
        u_copy(my_slot, A, 0, xn).start()
        u_copy(my_slot, B, 1, yn).start()
        u_copy(my_slot, B, 2, xn).start()
        u_copy(my_slot, A, 3, yn).start()
        u_copy(my_slot, None, 6, mate).start()

    def gather_forward():
        base = c * CHIPS
        u_copy(base + chip_x, A, 0, xn).wait_recv()
        u_copy(base + chip_x, A, 4, yn).start()
        u_copy(base + chip_y, B, 1, yn).wait_recv()
        u_copy(base + chip_y, B, 5, xn).start()

    def gather_finish():
        base = c * CHIPS
        u_copy(base + chip_x, B, 2, xn).wait_recv()
        u_copy(base + chip_x, None, 7, mate).start()
        u_copy(base + chip_y, A, 3, yn).wait_recv()
        u_copy(base + chip_y, None, 8, mate).start()
        u_copy(base + chip_d, A, 4, yn).wait_recv()
        u_copy(base + chip_d, B, 5, xn).wait_recv()
        u_copy(base + chip_d, None, 9, mate).start()
        for k in (6, 7, 8, 9):
            u_copy(my_slot, None, k, mate).wait_recv()
        for k in range(6):
            u_copy(my_slot, A, k, xn).wait_send()
        for k in (6, 7, 8, 9):
            u_copy(my_slot, None, k, mate).wait_send()

    def reduce_scatter(lhs, rhs, after_stage1, after_stage2):
        own, other = c * CHIPS, (1 - c) * CHIPS
        order = ((chip_d, chip_x, chip_y, chip), (chip_d, chip_y, chip_x, chip))
        first = (xn, yn)
        second = (yn, xn)
        TN = 512

        def hcols(h):
            return pl.ds(h * HALF, HALF)

        def mate_copy(h, k):
            return remote(part.at[other + order[h][k], :, hcols(h)], rm.at[order[h][k], :, hcols(h)],
                          mt_s.at[h, k], mt_r.at[h, k], mate)

        def stage1(h, k):
            return remote(part.at[own + order[h][k], :, hcols(h)], r1.at[h, k], r1_s.at[h, k], r1_r.at[h, k], first[h])

        def stage2(h):
            return remote(part.at[own + order[h][2], :, hcols(h)], r2.at[h], r2_s.at[h], r2_r.at[h], second[h])

        def fold(h, k, extra):
            j = order[h][k]

            def one(i, carry):
                rows = pl.ds(pl.multiple_of(i * 8, 8), 8)
                total = part[own + j, rows, hcols(h)] + rm[j, rows, hcols(h)]
                if extra is not None:
                    total = total + extra[rows, :]
                part[own + j, rows, hcols(h)] = total
                return carry
            lax.fori_loop(0, SEQ // 8, one, 0)

        for h in range(2):
            for grp in (other, own):
                a = lhs(grp)

                def tile(t, carry, grp=grp, h=h, a=a):
                    cols = pl.ds(pl.multiple_of(h * HALF + t * TN, TN), TN)
                    prod = jnp.dot(a, rhs[:, cols], preferred_element_type=F32)
                    part[pl.ds(grp, CHIPS), :, cols] = prod.reshape(CHIPS, SEQ, TN)
                    return carry
                lax.fori_loop(0, HALF // TN, tile, 0)
                if grp is other:
                    for k in range(4):
                        mate_copy(h, k).start()
            for k in (0, 1):
                mate_copy(h, k).wait_recv()
                fold(h, k, None)
                stage1(h, k).start()
        after_stage1()
        for h in range(2):
            mate_copy(h, 2).wait_recv()
            stage1(h, 0).wait_recv()
            fold(h, 2, r1.at[h, 0])
            stage2(h).start()
        after_stage2()
        for h in range(2):
            mate_copy(h, 3).wait_recv()
            stage1(h, 1).wait_recv()
            stage2(h).wait_recv()

            def last(i, carry, h=h):
                rows = pl.ds(pl.multiple_of(i * 16, 16), 16)
                total = (part[own + chip, rows, hcols(h)] + rm[chip, rows, hcols(h)]) + (r1[h, 1, rows, :] + r2[h, rows, :])
                xb[rows, hcols(h)] = (xb[rows, hcols(h)].astype(F32) + total).astype(BF16)
                return carry
            lax.fori_loop(0, SEQ // 16, last, 0)
        for h in range(2):
            for k in range(4):
                mate_copy(h, k).wait_send()
            for k in range(2):
                stage1(h, k).wait_send()
            stage2(h).wait_send()

    def nothing():
        pass

    own_x = pltpu.make_async_copy(x_in, xb, l_sem.at[2])
    own_x.start()
    for f in flips:
        remote(g_in, gains.at[me], s_gain.at[0], s_gain.at[1], dev(*f)).start()
    own_g = pltpu.make_async_copy(g_in, gains.at[me], l_sem.at[3])
    own_g.start()
    send_qkv(0)
    own_x.wait()
    own_g.wait()
    bytes_wait(gains.at[pl.ds(0, DEV - 1)], s_gain.at[1])
    bytes_wait(gains.at[pl.ds(0, DEV - 1)], s_gain.at[0])

    def layer(l, carry):
        ld_o = pltpu.make_async_copy(wo_in.at[l], wo, l_sem.at[0])
        ld_d = pltpu.make_async_copy(wd_in.at[l], wd, l_sem.at[1])
        ld_o.start()
        ld_d.start()
        norm(2 * l)
        gather_start()
        gather_forward()
        send_gu(l, 0)
        bytes_wait(land_qkv.at[l, pl.ds(0, OTHER), :], rs_qkv.at[l])
        load_qkv(l)
        gather_finish()
        bytes_wait(wqkv, ld_sem.at[0])

        def qkv_block(i, carry):
            prod = jnp.dot(u[pl.ds(i * 2, 2)].reshape(2 * SEQ, DIM), wqkv[...], preferred_element_type=F32)
            cos, sin = cos_in[...], sin_in[...]
            for s in range(2):
                rows = slice(s * SEQ, (s + 1) * SEQ)
                for h in range(QH + 1):
                    head = prod[rows, h * HD:(h + 1) * HD]
                    rot = (head * cos + pltpu.roll(head, HD // 2, 1) * sin).astype(BF16)
                    if h < QH:
                        qb[i * 2 + s, pl.ds(h * SEQ, SEQ), :] = rot
                    else:
                        kb[i * 2 + s] = rot
                vb[i * 2 + s] = prod[rows, (QH + 1) * HD:].astype(BF16)
            return carry
        lax.fori_loop(0, DEV // 2, qkv_block, 0)

        def attend(s, carry):
            scores = lax.dot_general(qb[s], kb[s], (((1,), (1,)), ((), ())), preferred_element_type=F32) * HD ** -0.5
            row = lax.broadcasted_iota(jnp.int32, (QH * SEQ, SEQ), 0) % SEQ
            col = lax.broadcasted_iota(jnp.int32, (QH * SEQ, SEQ), 1)
            scores = jnp.where(row >= col, scores, -jnp.inf)
            e = jnp.exp(scores - jnp.max(scores, axis=-1, keepdims=True))
            probs = (e / jnp.sum(e, axis=-1, keepdims=True)).astype(BF16)
            o = jnp.dot(probs, vb[s], preferred_element_type=F32).astype(BF16)
            for h in range(QH):
                ob[s, :, h * HD:(h + 1) * HD] = o[h * SEQ:(h + 1) * SEQ]
            return carry
        lax.fori_loop(0, DEV, attend, 0)

        ld_o.wait()
        reduce_scatter(lambda grp: ob[pl.ds(grp, CHIPS)].reshape(CHIPS * SEQ, QCOLS), wo,
                       lambda: send_gu(l, 1), lambda: send_gu(l, 2))

        norm(2 * l + 1)
        gather_start()
        gather_forward()
        send_gu(l, 3)
        for n in range(2):
            bytes_wait(land_gu.at[l, n, pl.ds(0, OTHER), :], rs_gu.at[l, n])
            load_gu(l, n)
        gather_finish()

        @pl.when(l + 1 < LAYERS)
        def _():
            send_qkv(l + 1)

        for n in range(NCH):
            slot = n % 2
            bytes_wait(wgu.at[slot], ld_sem.at[1 + slot])

            def mlp_block(i, carry, n=n, slot=slot):
                prod = jnp.dot(u[pl.ds(i * 4, 4)].reshape(4 * SEQ, DIM), wgu[slot], preferred_element_type=F32)
                gate = prod[:, :CW].astype(BF16).astype(F32)
                up = prod[:, CW:].astype(BF16).astype(F32)
                z = (gate * jax.nn.sigmoid(gate) * up).astype(BF16)
                zb[pl.ds(i * 4, 4), :, n * CW:(n + 1) * CW] = z.reshape(4, SEQ, CW)
                return carry
            lax.fori_loop(0, 2, mlp_block, 0)
            if n + 2 < NCH:
                bytes_wait(land_gu.at[l, n + 2, pl.ds(0, OTHER), :], rs_gu.at[l, n + 2])
                load_gu(l, n + 2)

        ld_d.wait()
        reduce_scatter(lambda grp: zb[pl.ds(grp, CHIPS)].reshape(CHIPS * SEQ, FCOLS), wd, nothing, nothing)

        bytes_wait(land_qkv.at[l, pl.ds(0, OTHER), :], ss_qkv.at[l])
        for n in range(NCH):
            bytes_wait(land_gu.at[l, n, pl.ds(0, OTHER), :], ss_gu.at[l, n])
        return carry

    lax.fori_loop(0, LAYERS, layer, 0)
    done = pltpu.make_async_copy(xb, out, l_sem.at[2])
    done.start()
    done.wait()


def solution(mesh):
    batch_spec = P(("dp", "fsdp"), None, None)
    gain_spec = P(None, "fsdp")
    proj_spec = P(None, "fsdp", None, None)
    mat_spec = P(None, "fsdp", None)
    cos, sin = rope_tables()

    def local_forward(hidden, attn_norm, w_q, w_k, w_v, w_o, mlp_norm, w_gate, w_up, w_down):
        gains = jnp.stack([attn_norm[0], mlp_norm[0], attn_norm[1], mlp_norm[1]]).astype(F32)
        gains = jnp.pad(gains, ((0, 4), (0, 0)))
        wqkv = jnp.concatenate([w_q.reshape(LAYERS, ROWS, DEV, QCOLS), w_k.reshape(LAYERS, ROWS, DEV, HD),
                                w_v.reshape(LAYERS, ROWS, DEV, HD)], axis=-1).reshape(LAYERS, ROWS, DEV * QKV)
        hbm = pl.BlockSpec(memory_space=pltpu.HBM)
        vmem = pl.BlockSpec(memory_space=pltpu.VMEM)
        dma = pltpu.SemaphoreType.DMA
        out = pl.pallas_call(
            body,
            name="two_layers",
            out_shape=(jax.ShapeDtypeStruct((SEQ, DIM), BF16),
                       jax.ShapeDtypeStruct((LAYERS, DIM, QKV), BF16),
                       jax.ShapeDtypeStruct((LAYERS, NCH, DIM, 2 * CW), BF16)),
            in_specs=[hbm, vmem, vmem, vmem, hbm, hbm, hbm, hbm, hbm],
            out_specs=(hbm, hbm, hbm),
            scratch_shapes=[
                pltpu.VMEM((SEQ, DIM), BF16),
                pltpu.VMEM((DEV, SEQ, DIM), BF16),
                pltpu.VMEM((DEV, SEQ, DIM), F32),
                pltpu.VMEM((CHIPS, SEQ, DIM), F32),
                pltpu.VMEM((2, 2, SEQ, HALF), F32),
                pltpu.VMEM((2, SEQ, HALF), F32),
                pltpu.VMEM((DIM, QKV), BF16),
                pltpu.VMEM((QCOLS, DIM), BF16),
                pltpu.VMEM((FCOLS, DIM), BF16),
                pltpu.VMEM((2, DIM, 2 * CW), BF16),
                pltpu.VMEM((DEV, QH * SEQ, HD), BF16),
                pltpu.VMEM((DEV, SEQ, HD), BF16),
                pltpu.VMEM((DEV, SEQ, HD), BF16),
                pltpu.VMEM((DEV, SEQ, QCOLS), BF16),
                pltpu.VMEM((DEV, SEQ, FCOLS), BF16),
                pltpu.VMEM((DEV, 8, ROWS), F32),
                dma((LAYERS,)), dma((LAYERS,)), dma((LAYERS, NCH)), dma((LAYERS, NCH)), dma((2,)), dma((4,)), dma((3,)),
                dma((10,)), dma((10,)), dma((2, 4)), dma((2, 4)), dma((2, 2)), dma((2, 2)), dma((2,)), dma((2,)),
            ],
            compiler_params=pltpu.CompilerParams(collective_id=0, has_side_effects=True, vmem_limit_bytes=66_000_000),
        )(hidden[0], gains, cos, sin, wqkv, w_o, w_gate, w_up, w_down)[0]
        return out[None]

    return jax.shard_map(local_forward, mesh=mesh, in_specs=(batch_spec, gain_spec, proj_spec, proj_spec, proj_spec, mat_spec, gain_spec, mat_spec, mat_spec, mat_spec), out_specs=batch_spec, check_vma=False)
```

```python
import functools

import jax
import jax.numpy as jnp
import numpy as np
from jax import lax
from jax.experimental import pallas as pl
from jax.experimental.pallas import tpu as pltpu
from jax.sharding import PartitionSpec as P

ROPE_THETA = 500000.0
NORM_EPS = 1e-5
MESH = pl.DeviceIdType.MESH
F32 = jnp.float32
BF16 = jnp.bfloat16

DEV = 8
CHIPS = 4
SEQ = 128
DIM = 3072
HALF = DIM // 2
ROWS = DIM // DEV
HD = 128
QH = 3
QCOLS = QH * HD
QKV = QCOLS + 2 * HD
FFN = 8192
FCOLS = FFN // DEV
NCH = 4
CW = FCOLS // NCH
LAYERS = 2
RB = 96
NP = 4
PW = DIM // NP


def rope_tables():
    half = HD // 2
    inv_freq = np.power(np.float32(ROPE_THETA), -(np.arange(half, dtype=np.float32) * np.float32(2.0) / np.float32(HD)))
    angles = (np.arange(SEQ, dtype=np.float32)[:, None] * inv_freq.astype(np.float32)[None, :]).astype(np.float64)
    cos, sin = np.cos(angles).astype(np.float32), np.sin(angles).astype(np.float32)
    return np.concatenate([cos, cos], axis=1), np.concatenate([-sin, sin], axis=1)


def body(x_in, g_in, cos_in, sin_in, wq_in, wk_in, wv_in, wo_in, wg_in, wu_in, wd_in,
         out, stage_qkv, land_qkv, land_gu,
         rq, rk, rv, st, xb, u, part, rm, r1, r2, wqkv, wo, wd, wgu, qb, kb, vb, ob, zb, gains,
         ss_qkv, rs_qkv, ss_gu, rs_gu, s_gain, l_sem, ld_sem,
         rl_in, rl_out, ag_s, ag_r, mt_s, mt_r, r1_s, r1_r, r2_s, r2_r):
    me = lax.axis_index("fsdp")
    c = me % 2
    cx = (me // 2) % 2
    cy = me // 4
    chip = me // 2

    def dev(fy, fx, fc):
        yy = 1 - cy if fy else cy
        xx = 1 - cx if fx else cx
        cc = 1 - c if fc else c
        return yy * 4 + xx * 2 + cc

    mate, xn, yn = dev(0, 0, 1), dev(0, 1, 0), dev(1, 0, 0)
    chip_x, chip_y, chip_d = xn // 2, yn // 2, dev(1, 1, 0) // 2
    flips = ((1, 1, 0), (1, 1, 1), (0, 1, 0), (1, 0, 0), (0, 1, 1), (1, 0, 1), (0, 0, 1))

    def remote(src, dst, ssem, rsem, target):
        return pltpu.make_async_remote_copy(src, dst, ssem, rsem, device_id={"fsdp": target}, device_id_type=MESH)

    def bytes_wait(ref, sem):
        pltpu.make_async_copy(ref, ref, sem).wait()

    barrier = pltpu.get_barrier_semaphore()
    for f in flips:
        pl.semaphore_signal(barrier, inc=1, device_id={"fsdp": dev(*f)}, device_id_type=MESH)
    pl.semaphore_wait(barrier, DEV - 1)

    def send_qkv(l):
        for f in flips:
            e = dev(*f)
            remote(stage_qkv.at[l, e],
                   land_qkv.at[l, pl.ds(pl.multiple_of(me * ROWS, ROWS), ROWS), :],
                   ss_qkv.at[l], rs_qkv.at[l], e).start()

    def send_gu(l, n):
        for f in flips:
            e = dev(*f)
            cols = pl.ds(pl.multiple_of(e * FCOLS + n * CW, 128), CW)
            rows = pl.ds(pl.multiple_of(me * ROWS, ROWS), ROWS)
            remote(wg_in.at[l, :, cols], land_gu.at[l, n, rows, pl.ds(0, CW)], ss_gu.at[l, n], rs_gu.at[l, n], e).start()
            remote(wu_in.at[l, :, cols], land_gu.at[l, n, rows, pl.ds(CW, CW)], ss_gu.at[l, n], rs_gu.at[l, n], e).start()

    OTHER = (DEV - 1) * ROWS

    def load_qkv(l):
        for f in flips:
            rows = pl.ds(pl.multiple_of(dev(*f) * ROWS, ROWS), ROWS)
            pltpu.make_async_copy(land_qkv.at[l, rows, :], wqkv.at[rows, :], ld_sem.at[0]).start()
        mine = pl.ds(pl.multiple_of(me * ROWS, ROWS), ROWS)
        pltpu.make_async_copy(stage_qkv.at[l, me], wqkv.at[mine, :], ld_sem.at[0]).start()

    def load_gu(l, n):
        slot = n % 2
        for f in flips:
            rows = pl.ds(pl.multiple_of(dev(*f) * ROWS, ROWS), ROWS)
            pltpu.make_async_copy(land_gu.at[l, n, rows, :], wgu.at[slot, rows, :], ld_sem.at[1 + slot]).start()
        mine = pl.ds(pl.multiple_of(me * ROWS, ROWS), ROWS)
        cols = pl.ds(pl.multiple_of(me * FCOLS + n * CW, 128), CW)
        pltpu.make_async_copy(wg_in.at[l, :, cols], wgu.at[slot, mine, pl.ds(0, CW)], ld_sem.at[1 + slot]).start()
        pltpu.make_async_copy(wu_in.at[l, :, cols], wgu.at[slot, mine, pl.ds(CW, CW)], ld_sem.at[1 + slot]).start()

    def relayout(l):
        def fetch(i):
            slot = i % 2
            rows = pl.ds(pl.multiple_of(i * RB, RB), RB)
            return [pltpu.make_async_copy(src.at[l, rows], dst.at[slot], rl_in.at[slot, k])
                    for k, (src, dst) in enumerate(((wq_in, rq), (wk_in, rk), (wv_in, rv)))]

        def put(i):
            slot = i % 2
            rows = pl.ds(pl.multiple_of(i * RB, RB), RB)
            return pltpu.make_async_copy(st.at[slot], stage_qkv.at[l, :, rows, :], rl_out.at[slot])

        steps = ROWS // RB
        for cp in fetch(0):
            cp.start()

        def step(i, carry):
            slot = i % 2

            @pl.when(i + 1 < steps)
            def _():
                for cp in fetch(i + 1):
                    cp.start()
            for cp in fetch(i):
                cp.wait()

            @pl.when(i >= 2)
            def _():
                put(i - 2).wait()

            def block(b, carry):
                rows = pl.ds(pl.multiple_of(b * 16, 16), 16)
                q = rq[slot, rows].astype(F32).reshape(16, DEV * QCOLS).astype(BF16)
                k = rk[slot, rows].astype(F32).reshape(16, DEV * HD).astype(BF16)
                v = rv[slot, rows].astype(F32).reshape(16, DEV * HD).astype(BF16)
                for e in range(DEV):
                    st[slot, e, rows, :QCOLS] = q[:, e * QCOLS:(e + 1) * QCOLS]
                    st[slot, e, rows, QCOLS:QCOLS + HD] = k[:, e * HD:(e + 1) * HD]
                    st[slot, e, rows, QCOLS + HD:] = v[:, e * HD:(e + 1) * HD]
                return carry
            lax.fori_loop(0, RB // 16, block, 0)
            put(i).start()
            return carry
        lax.fori_loop(0, steps, step, 0)
        put(steps - 2).wait()
        put(steps - 1).wait()

    my_slot = c * CHIPS + chip

    def norm(row):
        def one(i, carry):
            rows = pl.ds(pl.multiple_of(i * 16, 16), 16)
            wide = xb[rows, :].astype(F32)
            inv = lax.rsqrt(jnp.mean(wide * wide, axis=-1, keepdims=True) + NORM_EPS)
            for s in range(DEV):
                cols = slice(s * ROWS, (s + 1) * ROWS)
                g = gains[s, pl.ds(row, 1), :]
                u[my_slot, rows, cols] = (wide[:, cols] * inv * g).astype(BF16)
            return carry
        lax.fori_loop(0, SEQ // 16, one, 0)

    A, B = pl.ds(0, HALF), pl.ds(HALF, HALF)

    def u_copy(slot, cols, k, target):
        ref = u.at[slot, :, cols] if cols is not None else u.at[slot]
        return remote(ref, ref, ag_s.at[k], ag_r.at[k], target)

    def gather_start():
        u_copy(my_slot, A, 0, xn).start()
        u_copy(my_slot, B, 1, yn).start()
        u_copy(my_slot, B, 2, xn).start()
        u_copy(my_slot, A, 3, yn).start()
        u_copy(my_slot, None, 6, mate).start()

    def gather_forward():
        base = c * CHIPS
        u_copy(base + chip_x, A, 0, xn).wait_recv()
        u_copy(base + chip_x, A, 4, yn).start()
        u_copy(base + chip_y, B, 1, yn).wait_recv()
        u_copy(base + chip_y, B, 5, xn).start()

    def gather_finish():
        base = c * CHIPS
        u_copy(base + chip_x, B, 2, xn).wait_recv()
        u_copy(base + chip_x, None, 7, mate).start()
        u_copy(base + chip_y, A, 3, yn).wait_recv()
        u_copy(base + chip_y, None, 8, mate).start()
        u_copy(base + chip_d, A, 4, yn).wait_recv()
        u_copy(base + chip_d, B, 5, xn).wait_recv()
        u_copy(base + chip_d, None, 9, mate).start()
        for k in (6, 7, 8, 9):
            u_copy(my_slot, None, k, mate).wait_recv()
        for k in range(6):
            u_copy(my_slot, A, k, xn).wait_send()
        for k in (6, 7, 8, 9):
            u_copy(my_slot, None, k, mate).wait_send()

    def reduce_scatter(lhs, rhs, after_stage2):
        own, other = c * CHIPS, (1 - c) * CHIPS
        order = ((chip_d, chip_x, chip_y, chip), (chip_d, chip_y, chip_x, chip))
        first = (xn, yn)
        second = (yn, xn)

        def cols(p):
            return slice(p * PW, (p + 1) * PW)

        def mate_copy(p, k):
            j = order[p % 2][k]
            return remote(part.at[other + j, :, pl.ds(p * PW, PW)], rm.at[j, :, pl.ds(p * PW, PW)], mt_s.at[p, k], mt_r.at[p, k], mate)

        def stage1(p, k):
            return remote(part.at[own + order[p % 2][k], :, pl.ds(p * PW, PW)], r1.at[p, k], r1_s.at[p, k], r1_r.at[p, k], first[p % 2])

        def stage2(p):
            return remote(part.at[own + order[p % 2][2], :, pl.ds(p * PW, PW)], r2.at[p], r2_s.at[p], r2_r.at[p], second[p % 2])

        def fold(p, k, extra):
            j = order[p % 2][k]

            def one(i, carry):
                rows = pl.ds(pl.multiple_of(i * 16, 16), 16)
                total = part[own + j, rows, cols(p)] + rm[j, rows, cols(p)]
                if extra is not None:
                    total = total + extra[rows, :]
                part[own + j, rows, cols(p)] = total
                return carry
            lax.fori_loop(0, SEQ // 16, one, 0)

        for p in range(NP):
            for grp in (other, own):
                prod = jnp.dot(lhs(grp), rhs[:, cols(p)], preferred_element_type=F32)
                part[pl.ds(grp, CHIPS), :, cols(p)] = prod.reshape(CHIPS, SEQ, PW)
                if grp is other:
                    for k in range(4):
                        mate_copy(p, k).start()
            for k in (0, 1):
                mate_copy(p, k).wait_recv()
                fold(p, k, None)
                stage1(p, k).start()
        for p in range(NP):
            mate_copy(p, 2).wait_recv()
            stage1(p, 0).wait_recv()
            fold(p, 2, r1.at[p, 0])
            stage2(p).start()
        after_stage2()
        for p in range(NP):
            mate_copy(p, 3).wait_recv()
            stage1(p, 1).wait_recv()
            stage2(p).wait_recv()

            def last(i, carry, p=p):
                rows = pl.ds(pl.multiple_of(i * 16, 16), 16)
                total = (part[own + chip, rows, cols(p)] + rm[chip, rows, cols(p)]) + (r1[p, 1, rows, :] + r2[p, rows, :])
                xb[rows, cols(p)] = (xb[rows, cols(p)].astype(F32) + total).astype(BF16)
                return carry
            lax.fori_loop(0, SEQ // 16, last, 0)
        for p in range(NP):
            for k in range(4):
                mate_copy(p, k).wait_send()
            for k in range(2):
                stage1(p, k).wait_send()
            stage2(p).wait_send()

    own_x = pltpu.make_async_copy(x_in, xb, l_sem.at[2])
    own_x.start()
    for f in flips:
        remote(g_in, gains.at[me], s_gain.at[0], s_gain.at[1], dev(*f)).start()
    own_g = pltpu.make_async_copy(g_in, gains.at[me], l_sem.at[3])
    own_g.start()
    send_gu(0, 0)
    own_x.wait()
    own_g.wait()
    bytes_wait(gains.at[pl.ds(0, DEV - 1)], s_gain.at[1])
    bytes_wait(gains.at[pl.ds(0, DEV - 1)], s_gain.at[0])

    def layer(l, carry):
        ld_o = pltpu.make_async_copy(wo_in.at[l], wo, l_sem.at[0])
        ld_d = pltpu.make_async_copy(wd_in.at[l], wd, l_sem.at[1])
        ld_o.start()
        ld_d.start()
        norm(2 * l)
        gather_start()

        @pl.when(l == 0)
        def _():
            relayout(0)
            send_qkv(0)

        gather_forward()
        send_gu(l, 1)

        @pl.when(l == 0)
        def _():
            relayout(1)

        bytes_wait(land_qkv.at[l, pl.ds(0, OTHER), :], rs_qkv.at[l])
        load_qkv(l)
        gather_finish()
        bytes_wait(wqkv, ld_sem.at[0])

        def qkv_block(i, carry):
            prod = jnp.dot(u[pl.ds(i * 2, 2)].reshape(2 * SEQ, DIM), wqkv[...], preferred_element_type=F32)
            cos, sin = cos_in[...], sin_in[...]
            for s in range(2):
                rows = slice(s * SEQ, (s + 1) * SEQ)
                for h in range(QH + 1):
                    head = prod[rows, h * HD:(h + 1) * HD]
                    rot = (head * cos + pltpu.roll(head, HD // 2, 1) * sin).astype(BF16)
                    if h < QH:
                        qb[i * 2 + s, pl.ds(h * SEQ, SEQ), :] = rot
                    else:
                        kb[i * 2 + s] = rot
                vb[i * 2 + s] = prod[rows, (QH + 1) * HD:].astype(BF16)
            return carry
        lax.fori_loop(0, DEV // 2, qkv_block, 0)

        def attend(s, carry):
            scores = lax.dot_general(qb[s], kb[s], (((1,), (1,)), ((), ())), preferred_element_type=F32) * HD ** -0.5
            row = lax.broadcasted_iota(jnp.int32, (QH * SEQ, SEQ), 0) % SEQ
            col = lax.broadcasted_iota(jnp.int32, (QH * SEQ, SEQ), 1)
            scores = jnp.where(row >= col, scores, -jnp.inf)
            e = jnp.exp(scores - jnp.max(scores, axis=-1, keepdims=True))
            probs = (e / jnp.sum(e, axis=-1, keepdims=True)).astype(BF16)
            o = jnp.dot(probs, vb[s], preferred_element_type=F32).astype(BF16)
            for h in range(QH):
                ob[s, :, h * HD:(h + 1) * HD] = o[h * SEQ:(h + 1) * SEQ]
            return carry
        lax.fori_loop(0, DEV, attend, 0)

        ld_o.wait()
        reduce_scatter(lambda grp: ob[pl.ds(grp, CHIPS)].reshape(CHIPS * SEQ, QCOLS), wo,
                       lambda: send_gu(l, 2))

        norm(2 * l + 1)
        gather_start()
        gather_forward()
        send_gu(l, 3)
        for n in range(2):
            bytes_wait(land_gu.at[l, n, pl.ds(0, OTHER), :], rs_gu.at[l, n])
            load_gu(l, n)
        gather_finish()

        @pl.when(l + 1 < LAYERS)
        def _():
            send_qkv(l + 1)

        for n in range(NCH):
            slot = n % 2
            bytes_wait(wgu.at[slot], ld_sem.at[1 + slot])

            def mlp_block(i, carry, n=n, slot=slot):
                prod = jnp.dot(u[pl.ds(i * 4, 4)].reshape(4 * SEQ, DIM), wgu[slot], preferred_element_type=F32)
                gate = prod[:, :CW].astype(BF16).astype(F32)
                up = prod[:, CW:].astype(BF16).astype(F32)
                z = (gate * jax.nn.sigmoid(gate) * up).astype(BF16)
                zb[pl.ds(i * 4, 4), :, n * CW:(n + 1) * CW] = z.reshape(4, SEQ, CW)
                return carry
            lax.fori_loop(0, 2, mlp_block, 0)
            if n + 2 < NCH:
                bytes_wait(land_gu.at[l, n + 2, pl.ds(0, OTHER), :], rs_gu.at[l, n + 2])
                load_gu(l, n + 2)

        def next_chunk():
            @pl.when(l + 1 < LAYERS)
            def _():
                send_gu(l + 1, 0)

        ld_d.wait()
        reduce_scatter(lambda grp: zb[pl.ds(grp, CHIPS)].reshape(CHIPS * SEQ, FCOLS), wd, next_chunk)

        bytes_wait(land_qkv.at[l, pl.ds(0, OTHER), :], ss_qkv.at[l])
        for n in range(NCH):
            bytes_wait(land_gu.at[l, n, pl.ds(0, OTHER), :], ss_gu.at[l, n])
        return carry

    lax.fori_loop(0, LAYERS, layer, 0)
    done = pltpu.make_async_copy(xb, out, l_sem.at[2])
    done.start()
    done.wait()


def solution(mesh):
    batch_spec = P(("dp", "fsdp"), None, None)
    gain_spec = P(None, "fsdp")
    proj_spec = P(None, "fsdp", None, None)
    mat_spec = P(None, "fsdp", None)
    cos, sin = rope_tables()

    def local_forward(hidden, attn_norm, w_q, w_k, w_v, w_o, mlp_norm, w_gate, w_up, w_down):
        gains = jnp.stack([attn_norm[0], mlp_norm[0], attn_norm[1], mlp_norm[1]]).astype(F32)
        gains = jnp.pad(gains, ((0, 4), (0, 0)))
        hbm = pl.BlockSpec(memory_space=pltpu.HBM)
        vmem = pl.BlockSpec(memory_space=pltpu.VMEM)
        dma = pltpu.SemaphoreType.DMA
        out = pl.pallas_call(
            body,
            name="two_layers",
            out_shape=(jax.ShapeDtypeStruct((SEQ, DIM), BF16),
                       jax.ShapeDtypeStruct((LAYERS, DEV, ROWS, QKV), BF16),
                       jax.ShapeDtypeStruct((LAYERS, DIM, QKV), BF16),
                       jax.ShapeDtypeStruct((LAYERS, NCH, DIM, 2 * CW), BF16)),
            in_specs=[hbm, vmem, vmem, vmem, hbm, hbm, hbm, hbm, hbm, hbm, hbm],
            out_specs=(hbm, hbm, hbm, hbm),
            scratch_shapes=[
                pltpu.VMEM((2, RB, DEV * QH, HD), BF16),
                pltpu.VMEM((2, RB, DEV, HD), BF16),
                pltpu.VMEM((2, RB, DEV, HD), BF16),
                pltpu.VMEM((2, DEV, RB, QKV), BF16),
                pltpu.VMEM((SEQ, DIM), BF16),
                pltpu.VMEM((DEV, SEQ, DIM), BF16),
                pltpu.VMEM((DEV, SEQ, DIM), F32),
                pltpu.VMEM((CHIPS, SEQ, DIM), F32),
                pltpu.VMEM((NP, 2, SEQ, PW), F32),
                pltpu.VMEM((NP, SEQ, PW), F32),
                pltpu.VMEM((DIM, QKV), BF16),
                pltpu.VMEM((QCOLS, DIM), BF16),
                pltpu.VMEM((FCOLS, DIM), BF16),
                pltpu.VMEM((2, DIM, 2 * CW), BF16),
                pltpu.VMEM((DEV, QH * SEQ, HD), BF16),
                pltpu.VMEM((DEV, SEQ, HD), BF16),
                pltpu.VMEM((DEV, SEQ, HD), BF16),
                pltpu.VMEM((DEV, SEQ, QCOLS), BF16),
                pltpu.VMEM((DEV, SEQ, FCOLS), BF16),
                pltpu.VMEM((DEV, 8, ROWS), F32),
                dma((LAYERS,)), dma((LAYERS,)), dma((LAYERS, NCH)), dma((LAYERS, NCH)), dma((2,)), dma((4,)), dma((3,)),
                dma((2, 3)), dma((2,)),
                dma((10,)), dma((10,)), dma((NP, 4)), dma((NP, 4)), dma((NP, 2)), dma((NP, 2)), dma((NP,)), dma((NP,)),
            ],
            compiler_params=pltpu.CompilerParams(collective_id=0, has_side_effects=True, vmem_limit_bytes=66_000_000),
        )(hidden[0], gains, cos, sin, w_q, w_k, w_v, w_o, w_gate, w_up, w_down)[0]
        return out[None]

    return jax.shard_map(local_forward, mesh=mesh, in_specs=(batch_spec, gain_spec, proj_spec, proj_spec, proj_spec, mat_spec, gain_spec, mat_spec, mat_spec, mat_spec), out_specs=batch_spec, check_vma=False)
```

```python
import functools

import jax
import jax.numpy as jnp
import numpy as np
from jax import lax
from jax.experimental import pallas as pl
from jax.experimental.pallas import tpu as pltpu
from jax.sharding import PartitionSpec as P

ROPE_THETA = 500000.0
NORM_EPS = 1e-5
MESH = pl.DeviceIdType.MESH
F32 = jnp.float32
BF16 = jnp.bfloat16

DEV = 8
CHIPS = 4
SEQ = 128
DIM = 3072
HALF = DIM // 2
ROWS = DIM // DEV
HD = 128
QH = 3
QCOLS = QH * HD
QKV = QCOLS + 2 * HD
FFN = 8192
FCOLS = FFN // DEV
PAIR = 2 * ROWS
CHUNKS = ((0, 256), (256, 256), (512, 128), (640, 256), (896, 128))
NCH = len(CHUNKS)
LAST = NCH - 1
SLOT = (0, 1, 0, 1)
WIDE = 512
KPRE = CHUNKS[LAST][0]
LAYERS = 2
RB = 96
NP = 4
PW = DIM // NP


def rope_tables():
    half = HD // 2
    inv_freq = np.power(np.float32(ROPE_THETA), -(np.arange(half, dtype=np.float32) * np.float32(2.0) / np.float32(HD)))
    angles = (np.arange(SEQ, dtype=np.float32)[:, None] * inv_freq.astype(np.float32)[None, :]).astype(np.float64)
    cos, sin = np.cos(angles).astype(np.float32), np.sin(angles).astype(np.float32)
    return np.concatenate([cos, cos], axis=1), np.concatenate([-sin, sin], axis=1)


def body(x_in, ga_in, gm_in, cos_in, sin_in, wq_in, wk_in, wv_in, wo_in, wg_in, wu_in, wd_in,
         out, stage_qkv, land_qkv, land_gu,
         rq, rk, rv, st, xb, u, part, rm, r1, r2, wqkv, wo, wd, wgu, wlast, lsum, qb, kb, vb, ob, zb, ga, gm, cos_t, sin_t,
         ss_qkv, rs_qkv, ss_gu, rs_gu, s_gain, l_sem, ld_sem,
         rl_in, rl_out, ag_s, ag_r, mt_s, mt_r, r1_s, r1_r, r2_s, r2_r):
    me = lax.axis_index("fsdp")
    c = me % 2
    cx = (me // 2) % 2
    cy = me // 4
    chip = me // 2

    def dev(fy, fx, fc):
        yy = 1 - cy if fy else cy
        xx = 1 - cx if fx else cx
        cc = 1 - c if fc else c
        return yy * 4 + xx * 2 + cc

    mate, xn, yn = dev(0, 0, 1), dev(0, 1, 0), dev(1, 0, 0)
    chip_x, chip_y, chip_d = xn // 2, yn // 2, dev(1, 1, 0) // 2
    flips = ((0, 1, 0), (1, 0, 0), (0, 1, 1), (1, 0, 1), (1, 1, 0), (1, 1, 1), (0, 0, 1))

    def remote(src, dst, ssem, rsem, target):
        return pltpu.make_async_remote_copy(src, dst, ssem, rsem, device_id={"fsdp": target}, device_id_type=MESH)

    def bytes_wait(ref, sem):
        pltpu.make_async_copy(ref, ref, sem).wait()

    barrier = pltpu.get_barrier_semaphore()
    for f in flips:
        pl.semaphore_signal(barrier, inc=1, device_id={"fsdp": dev(*f)}, device_id_type=MESH)
    pl.semaphore_wait(barrier, DEV - 1)

    def send_qkv(l):
        for f in flips:
            e = dev(*f)
            remote(stage_qkv.at[l, e],
                   land_qkv.at[l, pl.ds(pl.multiple_of(me * ROWS, ROWS), ROWS), :],
                   ss_qkv.at[l], rs_qkv.at[l], e).start()

    def send_gu(l, n):
        off, w = CHUNKS[n]
        rows = pl.ds(pl.multiple_of(me * ROWS, ROWS), ROWS)
        for f in flips:
            e = dev(*f)
            cols = pl.ds(pl.multiple_of(e * FCOLS + off, 128), w)
            for src, k in ((wg_in, 0), (wu_in, 1)):
                dst = wlast.at[rows, pl.ds(k * w, w)] if n == LAST else land_gu.at[l, rows, pl.ds(2 * off + k * w, w)]
                got = n + 1 if n == LAST and f[0] and f[1] else n
                remote(src.at[l, :, cols], dst, ss_gu.at[l, n], rs_gu.at[l, got], e).start()

    def gu_bytes(l, n):
        off, w = CHUNKS[n]
        if n == LAST:
            return wlast.at[pl.ds(0, OTHER), :]
        return land_gu.at[l, pl.ds(0, OTHER), pl.ds(2 * off, 2 * w)]

    OTHER = (DEV - 1) * ROWS

    def load_qkv(l):
        for f in flips:
            rows = pl.ds(pl.multiple_of(dev(*f) * ROWS, ROWS), ROWS)
            pltpu.make_async_copy(land_qkv.at[l, rows, :], wqkv.at[rows, :], ld_sem.at[0]).start()
        mine = pl.ds(pl.multiple_of(me * ROWS, ROWS), ROWS)
        pltpu.make_async_copy(stage_qkv.at[l, me], wqkv.at[mine, :], ld_sem.at[0]).start()

    def own_gu(l, n):
        off, w = CHUNKS[n]
        mine = pl.ds(pl.multiple_of(me * ROWS, ROWS), ROWS)
        cols = pl.ds(pl.multiple_of(me * FCOLS + off, 128), w)
        for src, k in ((wg_in, 0), (wu_in, 1)):
            dst = wlast.at[mine, pl.ds(k * w, w)] if n == LAST else wgu.at[SLOT[n], mine, pl.ds(k * w, w)]
            pltpu.make_async_copy(src.at[l, :, cols], dst, ld_sem.at[1 + n]).start()

    def load_gu(l, n):
        off, w = CHUNKS[n]
        for f in flips:
            rows = pl.ds(pl.multiple_of(dev(*f) * ROWS, ROWS), ROWS)
            pltpu.make_async_copy(land_gu.at[l, rows, pl.ds(2 * off, 2 * w)], wgu.at[SLOT[n], rows, pl.ds(0, 2 * w)], ld_sem.at[1 + n]).start()
        own_gu(l, n)

    def relayout(l):
        def fetch(i):
            slot = i % 2
            rows = pl.ds(pl.multiple_of(i * RB, RB), RB)
            return [pltpu.make_async_copy(src.at[l, rows], dst.at[slot], rl_in.at[slot, k])
                    for k, (src, dst) in enumerate(((wq_in, rq), (wk_in, rk), (wv_in, rv)))]

        def put(i):
            slot = i % 2
            rows = pl.ds(pl.multiple_of(i * RB, RB), RB)
            return pltpu.make_async_copy(st.at[slot], stage_qkv.at[l, :, rows, :], rl_out.at[slot])

        steps = ROWS // RB
        for cp in fetch(0):
            cp.start()

        def step(i, carry):
            slot = i % 2

            @pl.when(i + 1 < steps)
            def _():
                for cp in fetch(i + 1):
                    cp.start()
            for cp in fetch(i):
                cp.wait()

            @pl.when(i >= 2)
            def _():
                put(i - 2).wait()

            def block(b, carry):
                rows = pl.ds(pl.multiple_of(b * 16, 16), 16)
                q = rq[slot, rows].astype(F32).reshape(16, DEV * QCOLS).astype(BF16)
                k = rk[slot, rows].astype(F32).reshape(16, DEV * HD).astype(BF16)
                v = rv[slot, rows].astype(F32).reshape(16, DEV * HD).astype(BF16)
                for e in range(DEV):
                    st[slot, e, rows, :QCOLS] = q[:, e * QCOLS:(e + 1) * QCOLS]
                    st[slot, e, rows, QCOLS:QCOLS + HD] = k[:, e * HD:(e + 1) * HD]
                    st[slot, e, rows, QCOLS + HD:] = v[:, e * HD:(e + 1) * HD]
                return carry
            lax.fori_loop(0, RB // 16, block, 0)
            put(i).start()
            return carry
        lax.fori_loop(0, steps, step, 0)
        put(steps - 2).wait()
        put(steps - 1).wait()

    my_slot = c * CHIPS + chip

    def norm(gains, l):
        def one(i, carry):
            rows = pl.ds(pl.multiple_of(i * 16, 16), 16)
            wide = xb[rows, :].astype(F32)
            inv = lax.rsqrt(jnp.mean(wide * wide, axis=-1, keepdims=True) + NORM_EPS)
            for s in range(DEV):
                cols = slice(s * ROWS, (s + 1) * ROWS)
                both = gains[s].astype(F32)
                g = jnp.where(l == 0, both[0:1], both[1:2])
                u[my_slot, rows, cols] = (wide[:, cols] * inv * g).astype(BF16)
            return carry
        lax.fori_loop(0, SEQ // 16, one, 0)

    A, B = pl.ds(0, HALF), pl.ds(HALF, HALF)

    def u_copy(slot, cols, k, target):
        ref = u.at[slot, :, cols] if cols is not None else u.at[slot]
        return remote(ref, ref, ag_s.at[k], ag_r.at[k], target)

    def gather_start():
        u_copy(my_slot, A, 0, xn).start()
        u_copy(my_slot, B, 1, yn).start()
        u_copy(my_slot, B, 2, xn).start()
        u_copy(my_slot, A, 3, yn).start()
        u_copy(my_slot, None, 6, mate).start()

    def gather_forward():
        base = c * CHIPS
        u_copy(base + chip_x, A, 0, xn).wait_recv()
        u_copy(base + chip_x, A, 4, yn).start()
        u_copy(base + chip_y, B, 1, yn).wait_recv()
        u_copy(base + chip_y, B, 5, xn).start()

    def gather_finish():
        base = c * CHIPS
        u_copy(base + chip_x, B, 2, xn).wait_recv()
        u_copy(base + chip_x, None, 7, mate).start()
        u_copy(base + chip_y, A, 3, yn).wait_recv()
        u_copy(base + chip_y, None, 8, mate).start()
        u_copy(base + chip_d, A, 4, yn).wait_recv()
        u_copy(base + chip_d, B, 5, xn).wait_recv()
        u_copy(base + chip_d, None, 9, mate).start()
        for k in (6, 7, 8, 9):
            u_copy(my_slot, None, k, mate).wait_recv()
        for k in range(6):
            u_copy(my_slot, A, k, xn).wait_send()
        for k in (6, 7, 8, 9):
            u_copy(my_slot, None, k, mate).wait_send()

    def reduce_scatter(act, rhs, k0, between, then):
        own, other = c * CHIPS, (1 - c) * CHIPS
        order = ((chip_d, chip_x, chip_y, chip), (chip_d, chip_y, chip_x, chip))
        first = (xn, yn)
        second = (yn, xn)

        def cols(p):
            return slice(p * PW, (p + 1) * PW)

        def mate_copy(p, k):
            j = order[p % 2][k]
            return remote(part.at[other + j, :, pl.ds(p * PW, PW)], rm.at[j, :, pl.ds(p * PW, PW)], mt_s.at[p, k], mt_r.at[p, k], mate)

        def stage1(p, k):
            return remote(part.at[own + order[p % 2][k], :, pl.ds(p * PW, PW)], r1.at[p, k], r1_s.at[p, k], r1_r.at[p, k], first[p % 2])

        def stage2(p):
            return remote(part.at[own + order[p % 2][2], :, pl.ds(p * PW, PW)], r2.at[p], r2_s.at[p], r2_r.at[p], second[p % 2])

        def fold(p, k, extra):
            j = order[p % 2][k]

            def one(i, carry):
                rows = pl.ds(pl.multiple_of(i * 16, 16), 16)
                total = part[own + j, rows, cols(p)] + rm[j, rows, cols(p)]
                if extra is not None:
                    total = total + extra[rows, :]
                part[own + j, rows, cols(p)] = total
                return carry
            lax.fori_loop(0, SEQ // 16, one, 0)

        def products(p, grp, ks):
            slots = [grp + order[p % 2][k] for k in ks]
            a = jnp.concatenate([act[slot, :, k0:] for slot in slots], axis=0)
            prod = jnp.dot(a, rhs[k0:, cols(p)], preferred_element_type=F32)
            for i, slot in enumerate(slots):
                term = prod[i * SEQ:(i + 1) * SEQ]
                part[slot, :, cols(p)] = part[slot, :, cols(p)] + term if k0 else term

        for pair in range(NP // 2):
            both = (2 * pair, 2 * pair + 1)
            for p in both:
                products(p, other, (0, 1))
                for k in (0, 1):
                    mate_copy(p, k).start()
            if pair == 0 and between is not None:
                between()
            for p in both:
                products(p, own, (0, 1))
            for k in (0, 1):
                for p in both:
                    mate_copy(p, k).wait_recv()
                    fold(p, k, None)
                    stage1(p, k).start()
        for p in range(NP):
            products(p, other, (2, 3))
            for k in (2, 3):
                mate_copy(p, k).start()
            products(p, own, (2, 3))
        for p in range(NP):
            mate_copy(p, 2).wait_recv()
            stage1(p, 0).wait_recv()
            fold(p, 2, r1.at[p, 0])
            stage2(p).start()
        for p in range(NP):
            if p == NP // 2:
                then()
            mate_copy(p, 3).wait_recv()
            stage1(p, 1).wait_recv()
            stage2(p).wait_recv()

            def last(i, carry, p=p):
                rows = pl.ds(pl.multiple_of(i * 16, 16), 16)
                total = (part[own + chip, rows, cols(p)] + rm[chip, rows, cols(p)]) + (r1[p, 1, rows, :] + r2[p, rows, :])
                xb[rows, cols(p)] = (xb[rows, cols(p)].astype(F32) + total).astype(BF16)
                return carry
            lax.fori_loop(0, SEQ // 16, last, 0)
        for p in range(NP):
            for k in range(4):
                mate_copy(p, k).wait_send()
            for k in range(2):
                stage1(p, k).wait_send()
            stage2(p).wait_send()

    for src, dst, k in ((ga_in, ga, 0), (gm_in, gm, 1)):
        for f in flips:
            remote(src, dst.at[me], s_gain.at[k], s_gain.at[2 + k], dev(*f)).start()
    send_gu(0, 0)
    starts = [pltpu.make_async_copy(src, dst, l_sem.at[2 + k]) for k, (src, dst) in enumerate(
        ((x_in, xb), (ga_in, ga.at[me]), (gm_in, gm.at[me]), (cos_in, cos_t), (sin_in, sin_t)))]
    for cp in starts:
        cp.start()
    for cp in starts:
        cp.wait()
    bytes_wait(ga.at[pl.ds(0, DEV - 1)], s_gain.at[2])
    bytes_wait(gm.at[pl.ds(0, DEV - 1)], s_gain.at[3])

    def layer(l, carry):
        ld_o = pltpu.make_async_copy(wo_in.at[l], wo, l_sem.at[0])
        ld_d = pltpu.make_async_copy(wd_in.at[l], wd, l_sem.at[1])
        ld_o.start()
        ld_d.start()
        norm(ga, l)
        gather_start()

        @pl.when(l == 0)
        def _():
            relayout(0)
            send_qkv(0)

        gather_forward()
        send_gu(l, 1)

        @pl.when(l == 0)
        def _():
            relayout(1)

        bytes_wait(land_qkv.at[l, pl.ds(0, OTHER), :], rs_qkv.at[l])
        load_qkv(l)
        gather_finish()
        bytes_wait(wqkv, ld_sem.at[0])

        def qkv_block(i, carry):
            prod = jnp.dot(u[pl.ds(i * 2, 2)].reshape(2 * SEQ, DIM), wqkv[...], preferred_element_type=F32)
            cos, sin = cos_t[...], sin_t[...]
            for s in range(2):
                rows = slice(s * SEQ, (s + 1) * SEQ)
                for h in range(QH + 1):
                    head = prod[rows, h * HD:(h + 1) * HD]
                    rot = (head * cos + pltpu.roll(head, HD // 2, 1) * sin).astype(BF16)
                    if h < QH:
                        qb[i * 2 + s, pl.ds(h * SEQ, SEQ), :] = rot
                    else:
                        kb[i * 2 + s] = rot
                vb[i * 2 + s] = prod[rows, (QH + 1) * HD:].astype(BF16)
            return carry
        lax.fori_loop(0, DEV // 2, qkv_block, 0)

        def attend(s, carry):
            scores = lax.dot_general(qb[s], kb[s], (((1,), (1,)), ((), ())), preferred_element_type=F32) * HD ** -0.5
            row = lax.broadcasted_iota(jnp.int32, (QH * SEQ, SEQ), 0) % SEQ
            col = lax.broadcasted_iota(jnp.int32, (QH * SEQ, SEQ), 1)
            scores = jnp.where(row >= col, scores, -jnp.inf)
            e = jnp.exp(scores - jnp.max(scores, axis=-1, keepdims=True))
            probs = (e / jnp.sum(e, axis=-1, keepdims=True)).astype(BF16)
            o = jnp.dot(probs, vb[s], preferred_element_type=F32).astype(BF16)
            for h in range(QH):
                ob[s, :, h * HD:(h + 1) * HD] = o[h * SEQ:(h + 1) * SEQ]
            return carry
        lax.fori_loop(0, DEV, attend, 0)

        ld_o.wait()
        reduce_scatter(ob, wo, 0, None, lambda: send_gu(l, 2))

        norm(gm, l)
        gather_start()
        gather_forward()
        send_gu(l, 3)
        send_gu(l, LAST)

        @pl.when(l + 1 < LAYERS)
        def _():
            send_qkv(l + 1)

        def chunk_arrives(n):
            bytes_wait(gu_bytes(l, n), rs_gu.at[l, n])
            load_gu(l, n)

        chunk_arrives(0)
        chunk_arrives(1)
        own_gu(l, LAST)
        gather_finish()

        def activate(prod, n, i):
            off, w = CHUNKS[n]
            gate = prod[:, :w].astype(BF16).astype(F32)
            up = prod[:, w:].astype(BF16).astype(F32)
            z = (gate * jax.nn.sigmoid(gate) * up).astype(BF16)
            zb[pl.ds(i * CHIPS, CHIPS), :, off:off + w] = z.reshape(CHIPS, SEQ, w)

        def mlp_block(n, i):
            rows = u[pl.ds(i * CHIPS, CHIPS)].reshape(CHIPS * SEQ, DIM)
            activate(jnp.dot(rows, wgu[SLOT[n], :, :2 * CHUNKS[n][1]], preferred_element_type=F32), n, i)

        def last_term(i, k):
            depth = pl.ds(pl.multiple_of(k * PAIR, PAIR), PAIR)
            rows = u[pl.ds(i * CHIPS, CHIPS), :, depth].reshape(CHIPS * SEQ, PAIR)
            return jnp.dot(rows, wlast[depth, :], preferred_element_type=F32)

        def last_near(i, carry):
            lsum[i] = (last_term(i, chip) + last_term(i, chip_x)) + last_term(i, chip_y)
            return carry

        def last_block(i):
            activate(lsum[i] + last_term(i, chip_d), LAST, i)

        def mlp_chunk(n):
            bytes_wait(wgu.at[SLOT[n], :, pl.ds(0, 2 * CHUNKS[n][1])], ld_sem.at[1 + n])

            def block(i, carry):
                mlp_block(n, i)
                return carry
            lax.fori_loop(0, 2, block, 0)

        mlp_chunk(0)
        chunk_arrives(2)
        mlp_chunk(1)
        mlp_chunk(2)
        chunk_arrives(3)
        mlp_chunk(3)
        ld_d.wait()

        def before_last(i, carry):
            slots = pl.ds(i * CHIPS, CHIPS)
            z = zb[slots, :, :KPRE].reshape(CHIPS * SEQ, KPRE)
            for p in range(NP):
                prod = jnp.dot(z, wd[:KPRE, p * PW:(p + 1) * PW], preferred_element_type=F32)
                part[slots, :, p * PW:(p + 1) * PW] = prod.reshape(CHIPS, SEQ, PW)
            return carry
        lax.fori_loop(0, 2, before_last, 0)
        bytes_wait(wlast.at[pl.ds(0, OTHER - PAIR), :], rs_gu.at[l, LAST])
        bytes_wait(wlast.at[pl.ds(0, ROWS), :], ld_sem.at[1 + LAST])
        lax.fori_loop(0, 2, last_near, 0)
        bytes_wait(wlast.at[pl.ds(0, PAIR), :], rs_gu.at[l, LAST + 1])
        last_block(1 - c)

        def next_chunk():
            @pl.when(l + 1 < LAYERS)
            def _():
                send_gu(l + 1, 0)

        reduce_scatter(zb, wd, KPRE, lambda: last_block(c), next_chunk)

        bytes_wait(land_qkv.at[l, pl.ds(0, OTHER), :], ss_qkv.at[l])
        for n in range(NCH):
            bytes_wait(gu_bytes(l, n), ss_gu.at[l, n])
        return carry

    lax.fori_loop(0, LAYERS, layer, 0)
    bytes_wait(ga.at[pl.ds(0, DEV - 1)], s_gain.at[0])
    bytes_wait(gm.at[pl.ds(0, DEV - 1)], s_gain.at[1])
    out[...] = xb[...]


def solution(mesh):
    batch_spec = P(("dp", "fsdp"), None, None)
    gain_spec = P(None, "fsdp")
    proj_spec = P(None, "fsdp", None, None)
    mat_spec = P(None, "fsdp", None)
    cos, sin = rope_tables()

    def local_forward(hidden, attn_norm, w_q, w_k, w_v, w_o, mlp_norm, w_gate, w_up, w_down):
        hbm = pl.BlockSpec(memory_space=pltpu.HBM)
        vmem = pl.BlockSpec(memory_space=pltpu.VMEM)
        dma = pltpu.SemaphoreType.DMA
        out = pl.pallas_call(
            body,
            name="two_layers",
            out_shape=(pltpu.VMEM((SEQ, DIM), BF16),
                       jax.ShapeDtypeStruct((LAYERS, DEV, ROWS, QKV), BF16),
                       jax.ShapeDtypeStruct((LAYERS, DIM, QKV), BF16),
                       jax.ShapeDtypeStruct((LAYERS, DIM, 2 * FCOLS), BF16)),
            in_specs=[hbm] * 12,
            out_specs=(vmem, hbm, hbm, hbm),
            scratch_shapes=[
                pltpu.VMEM((2, RB, DEV * QH, HD), BF16),
                pltpu.VMEM((2, RB, DEV, HD), BF16),
                pltpu.VMEM((2, RB, DEV, HD), BF16),
                pltpu.VMEM((2, DEV, RB, QKV), BF16),
                pltpu.VMEM((SEQ, DIM), BF16),
                pltpu.VMEM((DEV, SEQ, DIM), BF16),
                pltpu.VMEM((DEV, SEQ, DIM), F32),
                pltpu.VMEM((CHIPS, SEQ, DIM), F32),
                pltpu.VMEM((NP, 2, SEQ, PW), F32),
                pltpu.VMEM((NP, SEQ, PW), F32),
                pltpu.VMEM((DIM, QKV), BF16),
                pltpu.VMEM((QCOLS, DIM), BF16),
                pltpu.VMEM((FCOLS, DIM), BF16),
                pltpu.VMEM((2, DIM, WIDE), BF16),
                pltpu.VMEM((DIM, 2 * CHUNKS[LAST][1]), BF16),
                pltpu.VMEM((2, CHIPS * SEQ, 2 * CHUNKS[LAST][1]), F32),
                pltpu.VMEM((DEV, QH * SEQ, HD), BF16),
                pltpu.VMEM((DEV, SEQ, HD), BF16),
                pltpu.VMEM((DEV, SEQ, HD), BF16),
                pltpu.VMEM((DEV, SEQ, QCOLS), BF16),
                pltpu.VMEM((DEV, SEQ, FCOLS), BF16),
                pltpu.VMEM((DEV, LAYERS, ROWS), BF16),
                pltpu.VMEM((DEV, LAYERS, ROWS), BF16),
                pltpu.VMEM((SEQ, HD), F32),
                pltpu.VMEM((SEQ, HD), F32),
                dma((LAYERS,)), dma((LAYERS,)), dma((LAYERS, NCH)), dma((LAYERS, NCH + 1)), dma((4,)), dma((7,)), dma((1 + NCH,)),
                dma((2, 3)), dma((2,)),
                dma((10,)), dma((10,)), dma((NP, 4)), dma((NP, 4)), dma((NP, 2)), dma((NP, 2)), dma((NP,)), dma((NP,)),
            ],
            compiler_params=pltpu.CompilerParams(collective_id=0, has_side_effects=True, vmem_limit_bytes=65_000_000),
        )(hidden[0], attn_norm, mlp_norm, cos, sin, w_q, w_k, w_v, w_o, w_gate, w_up, w_down)[0]
        return out[None]

    return jax.shard_map(local_forward, mesh=mesh, in_specs=(batch_spec, gain_spec, proj_spec, proj_spec, proj_spec, mat_spec, gain_spec, mat_spec, mat_spec, mat_spec), out_specs=batch_spec, check_vma=False)
```

```python
import functools

import jax
import jax.numpy as jnp
import numpy as np
from jax import lax
from jax.experimental import pallas as pl
from jax.experimental.pallas import tpu as pltpu
from jax.sharding import PartitionSpec as P

ROPE_THETA = 500000.0
NORM_EPS = 1e-5
MESH = pl.DeviceIdType.MESH
F32 = jnp.float32
BF16 = jnp.bfloat16

DEV = 8
CHIPS = 4
SEQ = 128
DIM = 3072
HALF = DIM // 2
ROWS = DIM // DEV
HD = 128
QH = 3
QCOLS = QH * HD
QKV = QCOLS + 2 * HD
FFN = 8192
FCOLS = FFN // DEV
PAIR = 2 * ROWS
CHUNKS = ((0, 128), (256, 256), (512, 256), (128, 128), (768, 128), (896, 128))
NCH = len(CHUNKS)
LAST = NCH - 1
GROUPS = (((1,), 0), ((2,), 1), ((0, 3), 0), ((4,), 1))
AHEAD = 3
WIDE = 512
SPLIT = (1, 2, 3, 4)
KPRE = CHUNKS[LAST][0]
LAYERS = 2
RB = 96
NP = 4
PW = DIM // NP


def rope_tables():
    half = HD // 2
    inv_freq = np.power(np.float32(ROPE_THETA), -(np.arange(half, dtype=np.float32) * np.float32(2.0) / np.float32(HD)))
    angles = (np.arange(SEQ, dtype=np.float32)[:, None] * inv_freq.astype(np.float32)[None, :]).astype(np.float64)
    cos, sin = np.cos(angles).astype(np.float32), np.sin(angles).astype(np.float32)
    return np.concatenate([cos, cos], axis=1), np.concatenate([-sin, sin], axis=1)


def body(x_in, ga_in, gm_in, cos_in, sin_in, wq_in, wk_in, wv_in, wo_in, wg_in, wu_in, wd_in,
         out, stage_qkv, land_qkv, land_gu, land_wo,
         rq, rk, rv, st, xcol, u, part, rm, r1, r2, wqkv, wo, wd, wgu, wlast, lsum, qb, kb, vb, ob, ob2, zb, ga, gm, cos_t, sin_t,
         ss_qkv, rs_qkv, ss_wo, rs_wo, oe_s, oe_r, ss_gu, rs_gu, s_gain, l_sem, ld_sem,
         rl_in, rl_out, ag_s, ag_r, mt_s, mt_r, r1_s, r1_r, r2_s, r2_r):
    me = lax.axis_index("fsdp")
    c = me % 2
    cx = (me // 2) % 2
    cy = me // 4
    chip = me // 2

    def dev(fy, fx, fc):
        yy = 1 - cy if fy else cy
        xx = 1 - cx if fx else cx
        cc = 1 - c if fc else c
        return yy * 4 + xx * 2 + cc

    mate, xn, yn = dev(0, 0, 1), dev(0, 1, 0), dev(1, 0, 0)
    dn = dev(1, 1, 0)
    chip_x, chip_y, chip_d = xn // 2, yn // 2, dn // 2
    mycols = pl.ds(pl.multiple_of(me * ROWS, 128), ROWS)

    def axes(l):
        return yn + l * (xn - yn), xn + l * (yn - xn)
    flips = ((0, 1, 0), (1, 0, 0), (0, 1, 1), (1, 0, 1), (1, 1, 0), (1, 1, 1), (0, 0, 1))

    def remote(src, dst, ssem, rsem, target):
        return pltpu.make_async_remote_copy(src, dst, ssem, rsem, device_id={"fsdp": target}, device_id_type=MESH)

    def bytes_wait(ref, sem):
        pltpu.make_async_copy(ref, ref, sem).wait()

    barrier = pltpu.get_barrier_semaphore()
    for f in flips:
        pl.semaphore_signal(barrier, inc=1, device_id={"fsdp": dev(*f)}, device_id_type=MESH)
    pl.semaphore_wait(barrier, DEV - 1)

    def targets(l, which):
        if which is None:
            return [(dev(*f), f[0] and f[1]) for f in flips]
        an, bn = axes(l)
        e = {"a": an, "b": bn, "d": dn}[which]
        return [(e, which == "d"), (e + 1 - 2 * c, which == "d")] + ([(mate, False)] if which == "b" else [])

    def send_qkv(l, which=None):
        for e, diagonal in targets(l, which):
            remote(stage_qkv.at[l, e],
                   land_qkv.at[l, pl.ds(pl.multiple_of(me * ROWS, ROWS), ROWS), :],
                   ss_qkv.at[l], rs_qkv.at[l], e).start()

    def send_wo(l):
        an = axes(l)[0]
        for k, to in ((0, an // 2), (1, chip_d)):
            remote(wo_in.at[l, :, pl.ds(pl.multiple_of(to * PAIR, 128), PAIR)], land_wo.at[l, :, pl.ds(k * PAIR, PAIR)],
                   ss_wo.at[l], rs_wo.at[l], an).start()

    def load_wo(l):
        for k, of in ((0, chip), (1, axes(l)[1] // 2)):
            pltpu.make_async_copy(wo_in.at[l, :, pl.ds(pl.multiple_of(of * PAIR, 128), PAIR)],
                                  wo.at[pl.ds(0, ROWS), pl.ds(k * PAIR, PAIR)], l_sem.at[0]).start()
        pltpu.make_async_copy(land_wo.at[l], wo.at[pl.ds(ROWS, ROWS), :], l_sem.at[0]).start()

    def send_gu(l, n, which=None):
        off, w = CHUNKS[n]
        rows = pl.ds(pl.multiple_of(me * ROWS, ROWS), ROWS)
        for e, diagonal in targets(l, which):
            cols = pl.ds(pl.multiple_of(e * FCOLS + off, 128), w)
            for src, k in ((wg_in, 0), (wu_in, 1)):
                dst = wlast.at[rows, pl.ds(k * w, w)] if n == LAST else land_gu.at[l, rows, pl.ds(2 * off + k * w, w)]
                got = n + 1 if n == LAST and diagonal else n
                remote(src.at[l, :, cols], dst, ss_gu.at[l, n], rs_gu.at[l, got], e).start()

    def gu_bytes(l, n):
        off, w = CHUNKS[n]
        if n == LAST:
            return wlast.at[pl.ds(0, OTHER), :]
        return land_gu.at[l, pl.ds(0, OTHER), pl.ds(2 * off, 2 * w)]

    OTHER = (DEV - 1) * ROWS

    def load_qkv(l):
        for f in flips:
            rows = pl.ds(pl.multiple_of(dev(*f) * ROWS, ROWS), ROWS)
            pltpu.make_async_copy(land_qkv.at[l, rows, :], wqkv.at[rows, :], ld_sem.at[0]).start()
        mine = pl.ds(pl.multiple_of(me * ROWS, ROWS), ROWS)
        pltpu.make_async_copy(stage_qkv.at[l, me], wqkv.at[mine, :], ld_sem.at[0]).start()

    def own_gu(l, n, dst_of, sem):
        off, w = CHUNKS[n]
        cols = pl.ds(pl.multiple_of(me * FCOLS + off, 128), w)
        for src, k in ((wg_in, 0), (wu_in, 1)):
            pltpu.make_async_copy(src.at[l, :, cols], dst_of(k * w, w), sem).start()

    def own_last(l):
        mine = pl.ds(pl.multiple_of(me * ROWS, ROWS), ROWS)
        own_gu(l, LAST, lambda at, w: wlast.at[mine, pl.ds(at, w)], ld_sem.at[1 + len(GROUPS)])

    def group_cols(g):
        chunks = GROUPS[g][0]
        return 2 * CHUNKS[chunks[0]][0], 2 * sum(CHUNKS[n][1] for n in chunks)

    def group_arrives(l, g):
        chunks, slot = GROUPS[g]
        first, width = group_cols(g)
        sem = ld_sem.at[1 + g]
        for n in chunks:
            bytes_wait(gu_bytes(l, n), rs_gu.at[l, n])
        for f in flips:
            rows = pl.ds(pl.multiple_of(dev(*f) * ROWS, ROWS), ROWS)
            pltpu.make_async_copy(land_gu.at[l, rows, pl.ds(first, width)], wgu.at[slot, rows, pl.ds(0, width)], sem).start()
        mine = pl.ds(pl.multiple_of(me * ROWS, ROWS), ROWS)
        for n in chunks:
            base = 2 * CHUNKS[n][0] - first
            own_gu(l, n, lambda at, w, base=base: wgu.at[slot, mine, pl.ds(base + at, w)], sem)

    def relayout(l):
        def fetch(i):
            slot = i % 2
            rows = pl.ds(pl.multiple_of(i * RB, RB), RB)
            return [pltpu.make_async_copy(src.at[l, rows], dst.at[slot], rl_in.at[slot, k])
                    for k, (src, dst) in enumerate(((wq_in, rq), (wk_in, rk), (wv_in, rv)))]

        def put(i):
            slot = i % 2
            rows = pl.ds(pl.multiple_of(i * RB, RB), RB)
            return pltpu.make_async_copy(st.at[slot], stage_qkv.at[l, :, rows, :], rl_out.at[slot])

        steps = ROWS // RB
        for cp in fetch(0):
            cp.start()

        def step(i, carry):
            slot = i % 2

            @pl.when(i + 1 < steps)
            def _():
                for cp in fetch(i + 1):
                    cp.start()
            for cp in fetch(i):
                cp.wait()

            @pl.when(i >= 2)
            def _():
                put(i - 2).wait()

            def block(b, carry):
                rows = pl.ds(pl.multiple_of(b * 16, 16), 16)
                q = rq[slot, rows].astype(F32).reshape(16, DEV * QCOLS).astype(BF16)
                k = rk[slot, rows].astype(F32).reshape(16, DEV * HD).astype(BF16)
                v = rv[slot, rows].astype(F32).reshape(16, DEV * HD).astype(BF16)
                for e in range(DEV):
                    st[slot, e, rows, :QCOLS] = q[:, e * QCOLS:(e + 1) * QCOLS]
                    st[slot, e, rows, QCOLS:QCOLS + HD] = k[:, e * HD:(e + 1) * HD]
                    st[slot, e, rows, QCOLS + HD:] = v[:, e * HD:(e + 1) * HD]
                return carry
            lax.fori_loop(0, RB // 16, block, 0)
            put(i).start()
            return carry
        lax.fori_loop(0, steps, step, 0)
        put(steps - 2).wait()
        put(steps - 1).wait()

    my_slot = c * CHIPS + chip

    def norm_all(gains, l):
        def one(i, carry):
            slot = i // (SEQ // 16)
            rows = pl.ds(pl.multiple_of((i % (SEQ // 16)) * 16, 16), 16)
            wide = u[slot, rows, :].astype(F32)
            inv = lax.rsqrt(jnp.mean(wide * wide, axis=-1, keepdims=True) + NORM_EPS)
            for s in range(DEV):
                cols = slice(s * ROWS, (s + 1) * ROWS)
                both = gains[s].astype(F32)
                g = jnp.where(l == 0, both[0:1], both[1:2])
                u[slot, rows, cols] = (wide[:, cols] * inv * g).astype(BF16)
            return carry
        lax.fori_loop(0, DEV * SEQ // 16, one, 0)

    def by_rows(who, half):
        slot = c * CHIPS + {"me": chip, "x": chip_x, "y": chip_y, "d": chip_d}[who]
        return u.at[slot] if half is None else u.at[slot, :, pl.ds(half * HALF, HALF)]

    def by_cols(who, half):
        e = {"me": me, "x": xn, "y": yn, "d": dn}[who]
        cols = pl.ds(pl.multiple_of(e * ROWS, 128), ROWS)
        return u.at[:, :, cols] if half is None else u.at[pl.ds(half * CHIPS, CHIPS), :, cols]

    def u_copy(ref, k, target):
        return remote(ref, ref, ag_s.at[k], ag_r.at[k], target)

    def gather_start(at):
        u_copy(at("me", 0), 0, xn).start()
        u_copy(at("me", 1), 1, yn).start()
        u_copy(at("me", 1), 2, xn).start()
        u_copy(at("me", 0), 3, yn).start()
        u_copy(at("me", None), 6, mate).start()

    def gather_forward(at):
        u_copy(at("x", 0), 0, xn).wait_recv()
        u_copy(at("x", 0), 4, yn).start()
        u_copy(at("y", 1), 1, yn).wait_recv()
        u_copy(at("y", 1), 5, xn).start()

    def gather_finish(at):
        u_copy(at("x", 1), 2, xn).wait_recv()
        u_copy(at("x", None), 7, mate).start()
        u_copy(at("y", 0), 3, yn).wait_recv()
        u_copy(at("y", None), 8, mate).start()
        u_copy(at("d", 0), 4, yn).wait_recv()
        u_copy(at("d", 1), 5, xn).wait_recv()
        u_copy(at("d", None), 9, mate).start()
        for k in (6, 7, 8, 9):
            u_copy(at("me", None), k, mate).wait_recv()
        for k in range(6):
            u_copy(at("me", 0), k, xn).wait_send()
        for k in (6, 7, 8, 9):
            u_copy(at("me", None), k, mate).wait_send()

    def keep(slot, total):
        new = (xcol[slot].astype(F32) + total).astype(BF16)
        xcol[slot] = new
        u[slot, :, mycols] = new

    def out_proj(l, after_exchange, after_sums):
        an, bn = axes(l)

        def o_copy(g):
            return remote(ob.at[pl.ds(g * CHIPS, CHIPS)], ob2.at[pl.ds(g * CHIPS, CHIPS)], oe_s.at[g], oe_r.at[g], an)

        def mate_copy(p, b):
            return remote(part.at[pl.ds(2 * p, 2), :, pl.ds(pl.multiple_of(b * PAIR + (1 - c) * ROWS, 128), ROWS)], rm.at[p, b],
                          mt_s.at[p, b], mt_r.at[p, b], mate)

        def sums(p):
            return remote(part.at[pl.ds(2 * p, 2), :, pl.ds(pl.multiple_of(PAIR + c * ROWS, 128), ROWS)], r1.at[p, 0],
                          r1_s.at[p, 0], r1_r.at[p, 0], bn)

        def fold(p):
            mate_copy(p, 1).wait_recv()
            for t in range(2):
                cols = pl.ds(pl.multiple_of(PAIR + c * ROWS, 128), ROWS)
                part[2 * p + t, :, cols] = part[2 * p + t, :, cols] + rm[p, 1, t]
            sums(p).start()

        for g in range(2):
            o_copy(g).start()
        after_exchange()
        for p in range(NP):
            if p % 2 == 0:
                o_copy(p // 2).wait_recv()
            a = jnp.concatenate([r[pl.ds(2 * p, 2)].reshape(2 * SEQ, QCOLS) for r in (ob, ob2)], axis=1)
            for b in (1, 0):
                prod = jnp.dot(a, wo[:, b * PAIR:(b + 1) * PAIR], preferred_element_type=F32)
                part[pl.ds(2 * p, 2), :, b * PAIR:(b + 1) * PAIR] = prod.reshape(2, SEQ, PAIR)
                mate_copy(p, b).start()
            if p:
                fold(p - 1)
        fold(NP - 1)
        after_sums()
        for p in range(NP):
            mate_copy(p, 0).wait_recv()
            sums(p).wait_recv()
            for t in range(2):
                keep(2 * p + t, (part[2 * p + t, :, pl.ds(pl.multiple_of(c * ROWS, 128), ROWS)] + rm[p, 0, t]) + r1[p, 0, t])
        for g in range(2):
            o_copy(g).wait_send()
        for p in range(NP):
            for b in range(2):
                mate_copy(p, b).wait_send()
            sums(p).wait_send()

    def reduce_scatter(rows_form, act, rhs, k0, between, then):
        own, other = c, 1 - c
        order = ((chip_d, chip_x, chip_y, chip), (chip_d, chip_y, chip_x, chip))
        first = (xn, yn)
        second = (yn, xn)

        def sub(p, j, core, t):
            if rows_form:
                return core * CHIPS + j, pl.ds(p * PW + t * ROWS, ROWS)
            return 2 * p + t, pl.ds(pl.multiple_of(j * PAIR + core * ROWS, 128), ROWS)

        def pieces(p, j, core, dst, ssem, rsem, target):
            for t in range(2):
                slot, cols = sub(p, j, core, t)
                remote(part.at[slot, :, cols], dst.at[t], ssem, rsem, target).start()

        def unit(sem):
            bytes_wait(r2.at[0], sem)

        def send_mate(p, k):
            j = order[p % 2][k]
            pieces(p, j, other, rm.at[p, j], mt_s.at[p, k], mt_r.at[p, k], mate)

        def fold(p, k, extra):
            j = order[p % 2][k]
            for t in range(2):
                slot, cols = sub(p, j, own, t)
                total = part[slot, :, cols] + rm[p, j, t]
                part[slot, :, cols] = total if extra is None else total + extra[t]

        def products(p, grp, ks):
            slots = [grp * CHIPS + order[p % 2][k] for k in ks]
            a = jnp.concatenate([act[slot, :, k0:] for slot in slots], axis=0)
            cols = slice(p * PW, (p + 1) * PW)
            prod = jnp.dot(a, rhs[k0:, cols], preferred_element_type=F32)
            for i, slot in enumerate(slots):
                part[slot, :, cols] = part[slot, :, cols] + prod[i * SEQ:(i + 1) * SEQ]

        def column_products(p, k):
            cols = pl.ds(pl.multiple_of(order[p % 2][k] * PAIR, 128), PAIR)
            slots = pl.ds(2 * p, 2)
            prod = jnp.dot(act[slots, :, k0:].reshape(2 * SEQ, FCOLS - k0), rhs[k0:, cols], preferred_element_type=F32)
            part[slots, :, cols] = part[slots, :, cols] + prod.reshape(2, SEQ, PAIR)

        for pair in range(NP // 2):
            both = (2 * pair, 2 * pair + 1)
            for p in both:
                if rows_form:
                    products(p, other, (0, 1))
                for k in (0, 1):
                    if not rows_form:
                        column_products(p, k)
                    send_mate(p, k)
            if pair == 0 and between is not None:
                between()
            if rows_form:
                for p in both:
                    products(p, own, (0, 1))
            for k in (0, 1):
                for p in both:
                    unit(mt_r.at[p, k])
                    fold(p, k, None)
                    pieces(p, order[p % 2][k], own, r1.at[p, k], r1_s.at[p, k], r1_r.at[p, k], first[p % 2])
        for p in range(NP):
            if rows_form:
                products(p, other, (2, 3))
            for k in (2, 3):
                if not rows_form:
                    column_products(p, k)
                send_mate(p, k)
            if rows_form:
                products(p, own, (2, 3))
        for p in range(NP):
            unit(mt_r.at[p, 2])
            unit(r1_r.at[p, 0])
            fold(p, 2, r1.at[p, 0])
            pieces(p, order[p % 2][2], own, r2.at[p], r2_s.at[p], r2_r.at[p], second[p % 2])
        for p in range(NP):
            if p == NP // 2:
                then()
            unit(mt_r.at[p, 3])
            unit(r1_r.at[p, 1])
            unit(r2_r.at[p])
            for t in range(2):
                slot, cols = sub(p, chip, own, t)
                total = (part[slot, :, cols] + rm[p, chip, t]) + (r1[p, 1, t] + r2[p, t])
                if rows_form:
                    out[:, cols] = total.astype(BF16)
                else:
                    keep(slot, total)
        for p in range(NP):
            for k in range(4):
                unit(mt_s.at[p, k])
            for k in range(2):
                unit(r1_s.at[p, k])
            unit(r2_s.at[p])

    def send_direct(l, which):
        for n in SPLIT:
            send_gu(l, n, which)

    for src, dst, k in ((ga_in, ga, 0), (gm_in, gm, 1)):
        for f in flips:
            remote(src, dst.at[me], s_gain.at[k], s_gain.at[2 + k], dev(*f)).start()
    send_gu(0, 0)
    starts = [pltpu.make_async_copy(src, dst, l_sem.at[2 + k]) for k, (src, dst) in enumerate(
        ((x_in, u.at[my_slot]), (ga_in, ga.at[me]), (gm_in, gm.at[me]), (cos_in, cos_t), (sin_in, sin_t)))]
    for cp in starts:
        cp.start()
    for cp in starts:
        cp.wait()
    gather_start(by_rows)
    relayout(0)
    gather_forward(by_rows)
    send_qkv(0)
    send_wo(0)
    send_direct(0, "b")
    relayout(1)
    gather_finish(by_rows)
    bytes_wait(ga.at[pl.ds(0, DEV - 1)], s_gain.at[2])
    bytes_wait(gm.at[pl.ds(0, DEV - 1)], s_gain.at[3])

    def column_block(slot, carry):
        xcol[slot] = u[slot, :, mycols]
        return carry
    lax.fori_loop(0, DEV, column_block, 0)
    norm_all(ga, 0)

    def layer(l, carry):
        ld_d = pltpu.make_async_copy(wd_in.at[l], wd, l_sem.at[1])
        ld_d.start()
        bytes_wait(land_qkv.at[l, pl.ds(0, OTHER), :], rs_qkv.at[l])
        load_qkv(l)
        bytes_wait(wqkv, ld_sem.at[0])

        def qkv_block(i, carry):
            prod = jnp.dot(u[pl.ds(i * 2, 2)].reshape(2 * SEQ, DIM), wqkv[...], preferred_element_type=F32)
            cos, sin = cos_t[...], sin_t[...]
            for s in range(2):
                rows = slice(s * SEQ, (s + 1) * SEQ)
                for h in range(QH + 1):
                    head = prod[rows, h * HD:(h + 1) * HD]
                    rot = (head * cos + pltpu.roll(head, HD // 2, 1) * sin).astype(BF16)
                    if h < QH:
                        qb[i * 2 + s, pl.ds(h * SEQ, SEQ), :] = rot
                    else:
                        kb[i * 2 + s] = rot
                vb[i * 2 + s] = prod[rows, (QH + 1) * HD:].astype(BF16)
            return carry
        lax.fori_loop(0, DEV // 2, qkv_block, 0)

        def attend(s, carry):
            scores = lax.dot_general(qb[s], kb[s], (((1,), (1,)), ((), ())), preferred_element_type=F32) * HD ** -0.5
            row = lax.broadcasted_iota(jnp.int32, (QH * SEQ, SEQ), 0) % SEQ
            col = lax.broadcasted_iota(jnp.int32, (QH * SEQ, SEQ), 1)
            scores = jnp.where(row >= col, scores, -jnp.inf)
            e = jnp.exp(scores - jnp.max(scores, axis=-1, keepdims=True))
            probs = (e / jnp.sum(e, axis=-1, keepdims=True)).astype(BF16)
            o = jnp.dot(probs, vb[s], preferred_element_type=F32).astype(BF16)
            for h in range(QH):
                ob[s, :, h * HD:(h + 1) * HD] = o[h * SEQ:(h + 1) * SEQ]
            return carry
        lax.fori_loop(0, DEV, attend, 0)

        def after_exchange():
            for n in SPLIT:
                if n != AHEAD:
                    send_gu(l, n, "a")

            @pl.when(l == 0)
            def _():
                send_gu(l, AHEAD, "a")

            bytes_wait(land_wo.at[l], rs_wo.at[l])
            load_wo(l)
            bytes_wait(wo, l_sem.at[0])

        out_proj(l, after_exchange, lambda: None)

        gather_start(by_cols)
        gather_forward(by_cols)
        for which in ("a", "b"):
            send_gu(l, LAST, which)
        send_direct(l, "d")
        send_gu(l, LAST, "d")

        @pl.when(l + 1 < LAYERS)
        def _():
            send_qkv(l + 1)

        own_last(l)
        gather_finish(by_cols)
        norm_all(gm, l)
        group_arrives(l, 0)
        group_arrives(l, 1)

        def activate(prod, n, i):
            off, w = CHUNKS[n]
            gate = prod[:, :w].astype(BF16).astype(F32)
            up = prod[:, w:].astype(BF16).astype(F32)
            z = (gate * jax.nn.sigmoid(gate) * up).astype(BF16)
            zb[pl.ds(i * CHIPS, CHIPS), :, off:off + w] = z.reshape(CHIPS, SEQ, w)

        def mlp_group(g):
            chunks, slot = GROUPS[g]
            first, width = group_cols(g)
            bytes_wait(wgu.at[slot, :, pl.ds(0, width)], ld_sem.at[1 + g])

            def block(i, carry):
                rows = u[pl.ds(i * CHIPS, CHIPS)].reshape(CHIPS * SEQ, DIM)
                prod = jnp.dot(rows, wgu[slot, :, :width], preferred_element_type=F32)
                for n in chunks:
                    base = 2 * CHUNKS[n][0] - first
                    activate(prod[:, base:base + 2 * CHUNKS[n][1]], n, i)
                return carry
            lax.fori_loop(0, 2, block, 0)

        def last_term(i, k):
            depth = pl.ds(pl.multiple_of(k * PAIR, PAIR), PAIR)
            rows = u[pl.ds(i * CHIPS, CHIPS), :, depth].reshape(CHIPS * SEQ, PAIR)
            return jnp.dot(rows, wlast[depth, :], preferred_element_type=F32)

        def last_near(i, carry):
            lsum[i] = (last_term(i, chip) + last_term(i, chip_x)) + last_term(i, chip_y)
            return carry

        def last_block(i):
            activate(lsum[i] + last_term(i, chip_d), LAST, i)

        mlp_group(0)
        group_arrives(l, 2)
        mlp_group(1)
        mlp_group(2)
        group_arrives(l, 3)
        mlp_group(3)
        ld_d.wait()

        def before_last(i, carry):
            slots = pl.ds(i * CHIPS, CHIPS)
            z = zb[slots, :, :KPRE].reshape(CHIPS * SEQ, KPRE)
            for p in range(NP):
                prod = jnp.dot(z, wd[:KPRE, p * PW:(p + 1) * PW], preferred_element_type=F32)
                part[slots, :, p * PW:(p + 1) * PW] = prod.reshape(CHIPS, SEQ, PW)
            return carry
        lax.fori_loop(0, 2, before_last, 0)
        bytes_wait(wlast.at[pl.ds(0, OTHER - PAIR), :], rs_gu.at[l, LAST])
        bytes_wait(wlast.at[pl.ds(0, ROWS), :], ld_sem.at[1 + len(GROUPS)])
        lax.fori_loop(0, 2, last_near, 0)
        bytes_wait(wlast.at[pl.ds(0, PAIR), :], rs_gu.at[l, LAST + 1])

        @pl.when(l + 1 < LAYERS)
        def _():
            last_block(0)
            last_block(1)
            reduce_scatter(False, zb, wd, KPRE, None, lambda: send_gu(l + 1, 0))
            gather_start(by_cols)
            gather_forward(by_cols)
            send_wo(l + 1)
            send_gu(l + 1, AHEAD, "a")
            send_direct(l + 1, "b")
            gather_finish(by_cols)
            norm_all(ga, l + 1)

        @pl.when(l + 1 == LAYERS)
        def _():
            def residual(slot, carry):
                part[slot, :, mycols] = part[slot, :, mycols] + xcol[slot].astype(F32)
                return carry
            lax.fori_loop(0, DEV, residual, 0)
            last_block(1 - c)
            reduce_scatter(True, zb, wd, KPRE, lambda: last_block(c), lambda: None)

        bytes_wait(land_wo.at[l], ss_wo.at[l])
        bytes_wait(land_qkv.at[l, pl.ds(0, OTHER), :], ss_qkv.at[l])
        for n in range(NCH):
            bytes_wait(gu_bytes(l, n), ss_gu.at[l, n])
        return carry

    lax.fori_loop(0, LAYERS, layer, 0)
    bytes_wait(ga.at[pl.ds(0, DEV - 1)], s_gain.at[0])
    bytes_wait(gm.at[pl.ds(0, DEV - 1)], s_gain.at[1])


def solution(mesh):
    batch_spec = P(("dp", "fsdp"), None, None)
    gain_spec = P(None, "fsdp")
    proj_spec = P(None, "fsdp", None, None)
    mat_spec = P(None, "fsdp", None)
    cos, sin = rope_tables()

    def local_forward(hidden, attn_norm, w_q, w_k, w_v, w_o, mlp_norm, w_gate, w_up, w_down):
        hbm = pl.BlockSpec(memory_space=pltpu.HBM)
        vmem = pl.BlockSpec(memory_space=pltpu.VMEM)
        dma = pltpu.SemaphoreType.DMA
        out = pl.pallas_call(
            body,
            name="two_layers",
            out_shape=(pltpu.VMEM((SEQ, DIM), BF16),
                       jax.ShapeDtypeStruct((LAYERS, DEV, ROWS, QKV), BF16),
                       jax.ShapeDtypeStruct((LAYERS, DIM, QKV), BF16),
                       jax.ShapeDtypeStruct((LAYERS, DIM, 2 * FCOLS), BF16),
                       jax.ShapeDtypeStruct((LAYERS, ROWS, 2 * PAIR), BF16)),
            in_specs=[hbm] * 12,
            out_specs=(vmem, hbm, hbm, hbm, hbm),
            scratch_shapes=[
                pltpu.VMEM((2, RB, DEV * QH, HD), BF16),
                pltpu.VMEM((2, RB, DEV, HD), BF16),
                pltpu.VMEM((2, RB, DEV, HD), BF16),
                pltpu.VMEM((2, DEV, RB, QKV), BF16),
                pltpu.VMEM((DEV, SEQ, ROWS), BF16),
                pltpu.VMEM((DEV, SEQ, DIM), BF16),
                pltpu.VMEM((DEV, SEQ, DIM), F32),
                pltpu.VMEM((NP, CHIPS, 2, SEQ, ROWS), F32),
                pltpu.VMEM((NP, 2, 2, SEQ, ROWS), F32),
                pltpu.VMEM((NP, 2, SEQ, ROWS), F32),
                pltpu.VMEM((DIM, QKV), BF16),
                pltpu.VMEM((2 * ROWS, 2 * PAIR), BF16),
                pltpu.VMEM((FCOLS, DIM), BF16),
                pltpu.VMEM((2, DIM, WIDE), BF16),
                pltpu.VMEM((DIM, 2 * CHUNKS[LAST][1]), BF16),
                pltpu.VMEM((2, CHIPS * SEQ, 2 * CHUNKS[LAST][1]), F32),
                pltpu.VMEM((DEV, QH * SEQ, HD), BF16),
                pltpu.VMEM((DEV, SEQ, HD), BF16),
                pltpu.VMEM((DEV, SEQ, HD), BF16),
                pltpu.VMEM((DEV, SEQ, QCOLS), BF16),
                pltpu.VMEM((DEV, SEQ, QCOLS), BF16),
                pltpu.VMEM((DEV, SEQ, FCOLS), BF16),
                pltpu.VMEM((DEV, LAYERS, ROWS), BF16),
                pltpu.VMEM((DEV, LAYERS, ROWS), BF16),
                pltpu.VMEM((SEQ, HD), F32),
                pltpu.VMEM((SEQ, HD), F32),
                dma((LAYERS,)), dma((LAYERS,)), dma((LAYERS,)), dma((LAYERS,)), dma((2,)), dma((2,)), dma((LAYERS, NCH)), dma((LAYERS, NCH + 1)), dma((4,)), dma((7,)), dma((2 + len(GROUPS),)),
                dma((2, 3)), dma((2,)),
                dma((10,)), dma((10,)), dma((NP, 4)), dma((NP, 4)), dma((NP, 2)), dma((NP, 2)), dma((NP,)), dma((NP,)),
            ],
            compiler_params=pltpu.CompilerParams(collective_id=0, has_side_effects=True, vmem_limit_bytes=65_000_000),
        )(hidden[0], attn_norm, mlp_norm, cos, sin, w_q, w_k, w_v, w_o, w_gate, w_up, w_down)[0]
        return out[None]

    return jax.shard_map(local_forward, mesh=mesh, in_specs=(batch_spec, gain_spec, proj_spec, proj_spec, proj_spec, mat_spec, gain_spec, mat_spec, mat_spec, mat_spec), out_specs=batch_spec, check_vma=False)
```

```python
import functools

import jax
import jax.numpy as jnp
import numpy as np
from jax import lax
from jax.experimental import pallas as pl
from jax.experimental.pallas import tpu as pltpu
from jax.sharding import PartitionSpec as P

ROPE_THETA = 500000.0
NORM_EPS = 1e-5
MESH = pl.DeviceIdType.MESH
F32 = jnp.float32
BF16 = jnp.bfloat16

DEV = 8
CHIPS = 4
SEQ = 128
DIM = 3072
HALF = DIM // 2
ROWS = DIM // DEV
HD = 128
QH = 3
QCOLS = QH * HD
QKV = QCOLS + 2 * HD
FFN = 8192
FCOLS = FFN // DEV
PAIR = 2 * ROWS
CHUNKS = ((0, 128), (256, 256), (512, 256), (128, 128), (768, 128), (896, 128))
NCH = len(CHUNKS)
LAST = NCH - 1
GROUPS = (((1,), 0), ((2,), 1), ((0, 3), 0), ((4,), 1))
AHEAD = 3
WIDE = 512
SPLIT = (1, 2, 3, 4)
KPRE = CHUNKS[LAST - 1][0]
LAYERS = 2
RB = 96
NP = 4
PW = DIM // NP


def rope_tables():
    half = HD // 2
    inv_freq = np.power(np.float32(ROPE_THETA), -(np.arange(half, dtype=np.float32) * np.float32(2.0) / np.float32(HD)))
    angles = (np.arange(SEQ, dtype=np.float32)[:, None] * inv_freq.astype(np.float32)[None, :]).astype(np.float64)
    cos, sin = np.cos(angles).astype(np.float32), np.sin(angles).astype(np.float32)
    return np.concatenate([cos, cos], axis=1), np.concatenate([-sin, sin], axis=1)


def body(x_in, ga_in, gm_in, cos_in, sin_in, wq_in, wk_in, wv_in, wo_in, wg_in, wu_in, wd_in,
         out, stage_qkv, land_qkv, land_gu, land_wo,
         rq, rk, rv, st, xcol, u, part, rm, r1, r2, wqkv, wo, wd, wgu, wlast, lsum, qb, kb, vb, ob, ob2, zb, ga, gm, cos_t, sin_t,
         ss_qkv, rs_qkv, ss_wo, rs_wo, oe_s, oe_r, ss_gu, rs_gu, s_gain, l_sem, ld_sem,
         rl_in, rl_out, ag_s, ag_r, mt_s, mt_r, r1_s, r1_r, r2_s, r2_r):
    me = lax.axis_index("fsdp")
    c = me % 2
    cx = (me // 2) % 2
    cy = me // 4
    chip = me // 2

    def dev(fy, fx, fc):
        yy = 1 - cy if fy else cy
        xx = 1 - cx if fx else cx
        cc = 1 - c if fc else c
        return yy * 4 + xx * 2 + cc

    mate, xn, yn = dev(0, 0, 1), dev(0, 1, 0), dev(1, 0, 0)
    dn = dev(1, 1, 0)
    chip_x, chip_y, chip_d = xn // 2, yn // 2, dn // 2
    mycols = pl.ds(pl.multiple_of(me * ROWS, 128), ROWS)

    def axes(l):
        return yn + l * (xn - yn), xn + l * (yn - xn)
    flips = ((0, 1, 0), (1, 0, 0), (0, 1, 1), (1, 0, 1), (1, 1, 0), (1, 1, 1), (0, 0, 1))

    def remote(src, dst, ssem, rsem, target):
        return pltpu.make_async_remote_copy(src, dst, ssem, rsem, device_id={"fsdp": target}, device_id_type=MESH)

    def bytes_wait(ref, sem):
        pltpu.make_async_copy(ref, ref, sem).wait()

    barrier = pltpu.get_barrier_semaphore()
    for f in flips:
        pl.semaphore_signal(barrier, inc=1, device_id={"fsdp": dev(*f)}, device_id_type=MESH)
    pl.semaphore_wait(barrier, DEV - 1)

    def targets(l, which):
        if which is None:
            return [(dev(*f), f[0] and f[1]) for f in flips]
        an, bn = axes(l)
        e = {"a": an, "b": bn, "d": dn}[which]
        return [(e, which == "d"), (e + 1 - 2 * c, which == "d")] + ([(mate, False)] if which == "b" else [])

    def send_qkv(l, which=None):
        for e, diagonal in targets(l, which):
            remote(stage_qkv.at[l, e],
                   land_qkv.at[l, pl.ds(pl.multiple_of(me * ROWS, ROWS), ROWS), :],
                   ss_qkv.at[l], rs_qkv.at[l], e).start()

    def send_wo(l):
        an = axes(l)[0]
        for k, to in ((0, an // 2), (1, chip_d)):
            remote(wo_in.at[l, :, pl.ds(pl.multiple_of(to * PAIR, 128), PAIR)], land_wo.at[l, :, pl.ds(k * PAIR, PAIR)],
                   ss_wo.at[l], rs_wo.at[l], an).start()

    def load_wo(l):
        for k, of in ((0, chip), (1, axes(l)[1] // 2)):
            pltpu.make_async_copy(wo_in.at[l, :, pl.ds(pl.multiple_of(of * PAIR, 128), PAIR)],
                                  wo.at[pl.ds(0, ROWS), pl.ds(k * PAIR, PAIR)], l_sem.at[0]).start()
        pltpu.make_async_copy(land_wo.at[l], wo.at[pl.ds(ROWS, ROWS), :], l_sem.at[0]).start()

    def send_gu(l, n, which=None):
        off, w = CHUNKS[n]
        rows = pl.ds(pl.multiple_of(me * ROWS, ROWS), ROWS)
        for e, diagonal in targets(l, which):
            cols = pl.ds(pl.multiple_of(e * FCOLS + off, 128), w)
            for src, k in ((wg_in, 0), (wu_in, 1)):
                dst = wlast.at[rows, pl.ds(k * w, w)] if n == LAST else land_gu.at[l, rows, pl.ds(2 * off + k * w, w)]
                got = n + 1 if n == LAST and diagonal else n
                remote(src.at[l, :, cols], dst, ss_gu.at[l, n], rs_gu.at[l, got], e).start()

    def gu_bytes(l, n):
        off, w = CHUNKS[n]
        if n == LAST:
            return wlast.at[pl.ds(0, OTHER), :]
        return land_gu.at[l, pl.ds(0, OTHER), pl.ds(2 * off, 2 * w)]

    OTHER = (DEV - 1) * ROWS

    def load_qkv(l):
        for f in flips:
            rows = pl.ds(pl.multiple_of(dev(*f) * ROWS, ROWS), ROWS)
            pltpu.make_async_copy(land_qkv.at[l, rows, :], wqkv.at[rows, :], ld_sem.at[0]).start()
        mine = pl.ds(pl.multiple_of(me * ROWS, ROWS), ROWS)
        pltpu.make_async_copy(stage_qkv.at[l, me], wqkv.at[mine, :], ld_sem.at[0]).start()

    def own_gu(l, n, dst_of, sem):
        off, w = CHUNKS[n]
        cols = pl.ds(pl.multiple_of(me * FCOLS + off, 128), w)
        for src, k in ((wg_in, 0), (wu_in, 1)):
            pltpu.make_async_copy(src.at[l, :, cols], dst_of(k * w, w), sem).start()

    def own_last(l):
        mine = pl.ds(pl.multiple_of(me * ROWS, ROWS), ROWS)
        own_gu(l, LAST, lambda at, w: wlast.at[mine, pl.ds(at, w)], ld_sem.at[1 + len(GROUPS)])

    def group_cols(g):
        chunks = GROUPS[g][0]
        return 2 * CHUNKS[chunks[0]][0], 2 * sum(CHUNKS[n][1] for n in chunks)

    def group_arrives(l, g):
        chunks, slot = GROUPS[g]
        first, width = group_cols(g)
        sem = ld_sem.at[1 + g]
        for n in chunks:
            bytes_wait(gu_bytes(l, n), rs_gu.at[l, n])
        for f in flips:
            rows = pl.ds(pl.multiple_of(dev(*f) * ROWS, ROWS), ROWS)
            pltpu.make_async_copy(land_gu.at[l, rows, pl.ds(first, width)], wgu.at[slot, rows, pl.ds(0, width)], sem).start()
        mine = pl.ds(pl.multiple_of(me * ROWS, ROWS), ROWS)
        for n in chunks:
            base = 2 * CHUNKS[n][0] - first
            own_gu(l, n, lambda at, w, base=base: wgu.at[slot, mine, pl.ds(base + at, w)], sem)

    def relayout(l):
        def fetch(i):
            slot = i % 2
            rows = pl.ds(pl.multiple_of(i * RB, RB), RB)
            return [pltpu.make_async_copy(src.at[l, rows], dst.at[slot], rl_in.at[slot, k])
                    for k, (src, dst) in enumerate(((wq_in, rq), (wk_in, rk), (wv_in, rv)))]

        def put(i):
            slot = i % 2
            rows = pl.ds(pl.multiple_of(i * RB, RB), RB)
            return pltpu.make_async_copy(st.at[slot], stage_qkv.at[l, :, rows, :], rl_out.at[slot])

        steps = ROWS // RB
        for cp in fetch(0):
            cp.start()

        def step(i, carry):
            slot = i % 2

            @pl.when(i + 1 < steps)
            def _():
                for cp in fetch(i + 1):
                    cp.start()
            for cp in fetch(i):
                cp.wait()

            @pl.when(i >= 2)
            def _():
                put(i - 2).wait()

            def block(b, carry):
                rows = pl.ds(pl.multiple_of(b * 16, 16), 16)
                q = rq[slot, rows].astype(F32).reshape(16, DEV * QCOLS).astype(BF16)
                k = rk[slot, rows].astype(F32).reshape(16, DEV * HD).astype(BF16)
                v = rv[slot, rows].astype(F32).reshape(16, DEV * HD).astype(BF16)
                for e in range(DEV):
                    st[slot, e, rows, :QCOLS] = q[:, e * QCOLS:(e + 1) * QCOLS]
                    st[slot, e, rows, QCOLS:QCOLS + HD] = k[:, e * HD:(e + 1) * HD]
                    st[slot, e, rows, QCOLS + HD:] = v[:, e * HD:(e + 1) * HD]
                return carry
            lax.fori_loop(0, RB // 16, block, 0)
            put(i).start()
            return carry
        lax.fori_loop(0, steps, step, 0)
        put(steps - 2).wait()
        put(steps - 1).wait()

    my_slot = c * CHIPS + chip

    def norm_all(gains, l):
        def one(i, carry):
            slot = i // (SEQ // 16)
            rows = pl.ds(pl.multiple_of((i % (SEQ // 16)) * 16, 16), 16)
            wide = u[slot, rows, :].astype(F32)
            inv = lax.rsqrt(jnp.mean(wide * wide, axis=-1, keepdims=True) + NORM_EPS)
            for s in range(DEV):
                cols = slice(s * ROWS, (s + 1) * ROWS)
                both = gains[s].astype(F32)
                g = jnp.where(l == 0, both[0:1], both[1:2])
                u[slot, rows, cols] = (wide[:, cols] * inv * g).astype(BF16)
            return carry
        lax.fori_loop(0, DEV * SEQ // 16, one, 0)

    def by_rows(who, half):
        slot = c * CHIPS + {"me": chip, "x": chip_x, "y": chip_y, "d": chip_d}[who]
        return u.at[slot] if half is None else u.at[slot, :, pl.ds(half * HALF, HALF)]

    def by_cols(who, half):
        e = {"me": me, "x": xn, "y": yn, "d": dn}[who]
        cols = pl.ds(pl.multiple_of(e * ROWS, 128), ROWS)
        return u.at[:, :, cols] if half is None else u.at[pl.ds(half * CHIPS, CHIPS), :, cols]

    def u_copy(ref, k, target):
        return remote(ref, ref, ag_s.at[k], ag_r.at[k], target)

    def gather_start(at):
        u_copy(at("me", 0), 0, xn).start()
        u_copy(at("me", 1), 1, yn).start()
        u_copy(at("me", 1), 2, xn).start()
        u_copy(at("me", 0), 3, yn).start()
        u_copy(at("me", None), 6, mate).start()

    def gather_forward(at):
        u_copy(at("x", 0), 0, xn).wait_recv()
        u_copy(at("x", 0), 4, yn).start()
        u_copy(at("y", 1), 1, yn).wait_recv()
        u_copy(at("y", 1), 5, xn).start()

    def gather_finish(at):
        u_copy(at("x", 1), 2, xn).wait_recv()
        u_copy(at("x", None), 7, mate).start()
        u_copy(at("y", 0), 3, yn).wait_recv()
        u_copy(at("y", None), 8, mate).start()
        u_copy(at("d", 0), 4, yn).wait_recv()
        u_copy(at("d", 1), 5, xn).wait_recv()
        u_copy(at("d", None), 9, mate).start()
        for k in (6, 7, 8, 9):
            u_copy(at("me", None), k, mate).wait_recv()
        for k in range(6):
            u_copy(at("me", 0), k, xn).wait_send()
        for k in (6, 7, 8, 9):
            u_copy(at("me", None), k, mate).wait_send()

    def keep(slot, total):
        new = (xcol[slot].astype(F32) + total).astype(BF16)
        xcol[slot] = new
        u[slot, :, mycols] = new

    def out_proj(l, after_exchange, after_sums):
        an, bn = axes(l)

        def o_copy(g):
            return remote(ob.at[pl.ds(g * CHIPS, CHIPS)], ob2.at[pl.ds(g * CHIPS, CHIPS)], oe_s.at[g], oe_r.at[g], an)

        def mate_copy(p, b):
            return remote(part.at[pl.ds(2 * p, 2), :, pl.ds(pl.multiple_of(b * PAIR + (1 - c) * ROWS, 128), ROWS)], rm.at[p, b],
                          mt_s.at[p, b], mt_r.at[p, b], mate)

        def sums(p):
            return remote(part.at[pl.ds(2 * p, 2), :, pl.ds(pl.multiple_of(PAIR + c * ROWS, 128), ROWS)], r1.at[p, 0],
                          r1_s.at[p, 0], r1_r.at[p, 0], bn)

        def fold(p):
            mate_copy(p, 1).wait_recv()
            for t in range(2):
                cols = pl.ds(pl.multiple_of(PAIR + c * ROWS, 128), ROWS)
                part[2 * p + t, :, cols] = part[2 * p + t, :, cols] + rm[p, 1, t]
            sums(p).start()

        for g in range(2):
            o_copy(g).start()
        after_exchange()
        for p in range(NP):
            if p % 2 == 0:
                o_copy(p // 2).wait_recv()
            a = jnp.concatenate([r[pl.ds(2 * p, 2)].reshape(2 * SEQ, QCOLS) for r in (ob, ob2)], axis=1)
            for b in (1, 0):
                prod = jnp.dot(a, wo[:, b * PAIR:(b + 1) * PAIR], preferred_element_type=F32)
                part[pl.ds(2 * p, 2), :, b * PAIR:(b + 1) * PAIR] = prod.reshape(2, SEQ, PAIR)
                mate_copy(p, b).start()
            if p:
                fold(p - 1)
        fold(NP - 1)
        after_sums()
        for p in range(NP):
            mate_copy(p, 0).wait_recv()
            sums(p).wait_recv()
            for t in range(2):
                keep(2 * p + t, (part[2 * p + t, :, pl.ds(pl.multiple_of(c * ROWS, 128), ROWS)] + rm[p, 0, t]) + r1[p, 0, t])
        for g in range(2):
            o_copy(g).wait_send()
        for p in range(NP):
            for b in range(2):
                mate_copy(p, b).wait_send()
            sums(p).wait_send()

    def reduce_scatter(rows_form, act, rhs, k0, between, then):
        own, other = c, 1 - c
        order = ((chip_d, chip_x, chip_y, chip), (chip_d, chip_y, chip_x, chip))
        first = (xn, yn)
        second = (yn, xn)

        def sub(p, j, core, t):
            if rows_form:
                return core * CHIPS + j, pl.ds(p * PW + t * ROWS, ROWS)
            return 2 * p + t, pl.ds(pl.multiple_of(j * PAIR + core * ROWS, 128), ROWS)

        def pieces(p, j, core, dst, ssem, rsem, target):
            for t in range(2):
                slot, cols = sub(p, j, core, t)
                remote(part.at[slot, :, cols], dst.at[t], ssem, rsem, target).start()

        def unit(sem):
            bytes_wait(r2.at[0], sem)

        def send_mate(p, k):
            j = order[p % 2][k]
            pieces(p, j, other, rm.at[p, j], mt_s.at[p, k], mt_r.at[p, k], mate)

        def fold(p, k, extra):
            j = order[p % 2][k]
            for t in range(2):
                slot, cols = sub(p, j, own, t)
                total = part[slot, :, cols] + rm[p, j, t]
                part[slot, :, cols] = total if extra is None else total + extra[t]

        def products(p, grp, ks):
            slots = [grp * CHIPS + order[p % 2][k] for k in ks]
            a = jnp.concatenate([act[slot, :, k0:] for slot in slots], axis=0)
            cols = slice(p * PW, (p + 1) * PW)
            prod = jnp.dot(a, rhs[k0:, cols], preferred_element_type=F32)
            for i, slot in enumerate(slots):
                part[slot, :, cols] = part[slot, :, cols] + prod[i * SEQ:(i + 1) * SEQ]

        def column_products(p, k):
            cols = pl.ds(pl.multiple_of(order[p % 2][k] * PAIR, 128), PAIR)
            slots = pl.ds(2 * p, 2)
            prod = jnp.dot(act[slots, :, k0:].reshape(2 * SEQ, FCOLS - k0), rhs[k0:, cols], preferred_element_type=F32)
            part[slots, :, cols] = part[slots, :, cols] + prod.reshape(2, SEQ, PAIR)

        for pair in range(NP // 2):
            both = (2 * pair, 2 * pair + 1)
            for p in both:
                if rows_form:
                    products(p, other, (0, 1))
                for k in (0, 1):
                    if not rows_form:
                        column_products(p, k)
                    send_mate(p, k)
            if pair == 0 and between is not None:
                between()
            if rows_form:
                for p in both:
                    products(p, own, (0, 1))
            for k in (0, 1):
                for p in both:
                    unit(mt_r.at[p, k])
                    fold(p, k, None)
                    pieces(p, order[p % 2][k], own, r1.at[p, k], r1_s.at[p, k], r1_r.at[p, k], first[p % 2])
        for p in range(NP):
            if rows_form:
                products(p, other, (2, 3))
            for k in (2, 3):
                if not rows_form:
                    column_products(p, k)
                send_mate(p, k)
            if rows_form:
                products(p, own, (2, 3))
        for p in range(NP):
            unit(mt_r.at[p, 2])
            unit(r1_r.at[p, 0])
            fold(p, 2, r1.at[p, 0])
            pieces(p, order[p % 2][2], own, r2.at[p], r2_s.at[p], r2_r.at[p], second[p % 2])
        for p in range(NP):
            if p == NP // 2:
                then()
            unit(mt_r.at[p, 3])
            unit(r1_r.at[p, 1])
            unit(r2_r.at[p])
            for t in range(2):
                slot, cols = sub(p, chip, own, t)
                total = (part[slot, :, cols] + rm[p, chip, t]) + (r1[p, 1, t] + r2[p, t])
                if rows_form:
                    out[:, cols] = total.astype(BF16)
                else:
                    keep(slot, total)
        for p in range(NP):
            for k in range(4):
                unit(mt_s.at[p, k])
            for k in range(2):
                unit(r1_s.at[p, k])
            unit(r2_s.at[p])

    def send_direct(l, which):
        for n in SPLIT:
            send_gu(l, n, which)

    for src, dst, k in ((ga_in, ga, 0), (gm_in, gm, 1)):
        for f in flips:
            remote(src, dst.at[me], s_gain.at[k], s_gain.at[2 + k], dev(*f)).start()
    send_gu(0, 0)
    starts = [pltpu.make_async_copy(src, dst, l_sem.at[2 + k]) for k, (src, dst) in enumerate(
        ((x_in, u.at[my_slot]), (ga_in, ga.at[me]), (gm_in, gm.at[me]), (cos_in, cos_t), (sin_in, sin_t)))]
    for cp in starts:
        cp.start()
    for cp in starts:
        cp.wait()
    gather_start(by_rows)
    relayout(0)
    gather_forward(by_rows)
    send_qkv(0)
    send_wo(0)
    send_direct(0, "b")
    relayout(1)
    gather_finish(by_rows)
    bytes_wait(ga.at[pl.ds(0, DEV - 1)], s_gain.at[2])
    bytes_wait(gm.at[pl.ds(0, DEV - 1)], s_gain.at[3])

    def column_block(slot, carry):
        xcol[slot] = u[slot, :, mycols]
        return carry
    lax.fori_loop(0, DEV, column_block, 0)
    norm_all(ga, 0)

    def layer(l, carry):
        ld_d = pltpu.make_async_copy(wd_in.at[l], wd, l_sem.at[1])
        ld_d.start()
        bytes_wait(land_qkv.at[l, pl.ds(0, OTHER), :], rs_qkv.at[l])
        load_qkv(l)
        bytes_wait(wqkv, ld_sem.at[0])

        def qkv_block(i, carry):
            prod = jnp.dot(u[pl.ds(i * 2, 2)].reshape(2 * SEQ, DIM), wqkv[...], preferred_element_type=F32)
            cos, sin = cos_t[...], sin_t[...]
            for s in range(2):
                rows = slice(s * SEQ, (s + 1) * SEQ)
                for h in range(QH + 1):
                    head = prod[rows, h * HD:(h + 1) * HD]
                    rot = (head * cos + pltpu.roll(head, HD // 2, 1) * sin).astype(BF16)
                    if h < QH:
                        qb[i * 2 + s, pl.ds(h * SEQ, SEQ), :] = rot
                    else:
                        kb[i * 2 + s] = rot
                vb[i * 2 + s] = prod[rows, (QH + 1) * HD:].astype(BF16)
            return carry
        lax.fori_loop(0, DEV // 2, qkv_block, 0)

        def attend(s, carry):
            scores = lax.dot_general(qb[s], kb[s], (((1,), (1,)), ((), ())), preferred_element_type=F32) * HD ** -0.5
            row = lax.broadcasted_iota(jnp.int32, (QH * SEQ, SEQ), 0) % SEQ
            col = lax.broadcasted_iota(jnp.int32, (QH * SEQ, SEQ), 1)
            scores = jnp.where(row >= col, scores, -jnp.inf)
            e = jnp.exp(scores - jnp.max(scores, axis=-1, keepdims=True))
            probs = (e / jnp.sum(e, axis=-1, keepdims=True)).astype(BF16)
            o = jnp.dot(probs, vb[s], preferred_element_type=F32).astype(BF16)
            for h in range(QH):
                ob[s, :, h * HD:(h + 1) * HD] = o[h * SEQ:(h + 1) * SEQ]
            return carry
        lax.fori_loop(0, DEV, attend, 0)

        def after_exchange():
            for n in SPLIT:
                if n != AHEAD:
                    send_gu(l, n, "a")

            @pl.when(l == 0)
            def _():
                send_gu(l, AHEAD, "a")

            bytes_wait(land_wo.at[l], rs_wo.at[l])
            load_wo(l)
            bytes_wait(wo, l_sem.at[0])

        out_proj(l, after_exchange, lambda: None)

        gather_start(by_cols)
        gather_forward(by_cols)
        for which in ("a", "b"):
            send_gu(l, LAST, which)
        send_direct(l, "d")
        send_gu(l, LAST, "d")

        @pl.when(l + 1 < LAYERS)
        def _():
            send_qkv(l + 1)

        own_last(l)
        gather_finish(by_cols)
        norm_all(gm, l)
        group_arrives(l, 0)

        def activate(prod, n, i):
            off, w = CHUNKS[n]
            gate = prod[:, :w].astype(BF16).astype(F32)
            up = prod[:, w:].astype(BF16).astype(F32)
            z = (gate * jax.nn.sigmoid(gate) * up).astype(BF16)
            zb[pl.ds(i * CHIPS, CHIPS), :, off:off + w] = z.reshape(CHIPS, SEQ, w)

        def mlp_group(g):
            chunks, slot = GROUPS[g]
            first, width = group_cols(g)
            bytes_wait(wgu.at[slot, :, pl.ds(0, width)], ld_sem.at[1 + g])

            def block(i, carry):
                rows = u[pl.ds(i * CHIPS, CHIPS)].reshape(CHIPS * SEQ, DIM)
                prod = jnp.dot(rows, wgu[slot, :, :width], preferred_element_type=F32)
                for n in chunks:
                    base = 2 * CHUNKS[n][0] - first
                    activate(prod[:, base:base + 2 * CHUNKS[n][1]], n, i)
                return carry
            lax.fori_loop(0, 2, block, 0)

        def last_term(i, k):
            depth = pl.ds(pl.multiple_of(k * PAIR, PAIR), PAIR)
            rows = u[pl.ds(i * CHIPS, CHIPS), :, depth].reshape(CHIPS * SEQ, PAIR)
            return jnp.dot(rows, wlast[depth, :], preferred_element_type=F32)

        def last_near(i, carry):
            lsum[i] = (last_term(i, chip) + last_term(i, chip_x)) + last_term(i, chip_y)
            return carry

        def last_block(i):
            activate(lsum[i] + last_term(i, chip_d), LAST, i)

        mlp_group(0)
        group_arrives(l, 1)
        mlp_group(1)
        group_arrives(l, 2)
        mlp_group(2)
        ld_d.wait()

        def before_last(i, carry):
            slots = pl.ds(i * CHIPS, CHIPS)
            z = zb[slots, :, :KPRE].reshape(CHIPS * SEQ, KPRE)
            for p in range(NP):
                prod = jnp.dot(z, wd[:KPRE, p * PW:(p + 1) * PW], preferred_element_type=F32)
                part[slots, :, p * PW:(p + 1) * PW] = prod.reshape(CHIPS, SEQ, PW)
            return carry
        lax.fori_loop(0, 2, before_last, 0)
        group_arrives(l, 3)
        bytes_wait(wlast.at[pl.ds(0, OTHER - PAIR), :], rs_gu.at[l, LAST])
        bytes_wait(wlast.at[pl.ds(0, ROWS), :], ld_sem.at[1 + len(GROUPS)])
        lax.fori_loop(0, 2, last_near, 0)
        mlp_group(3)
        bytes_wait(wlast.at[pl.ds(0, PAIR), :], rs_gu.at[l, LAST + 1])

        @pl.when(l + 1 < LAYERS)
        def _():
            last_block(0)
            last_block(1)
            reduce_scatter(False, zb, wd, KPRE, None, lambda: send_gu(l + 1, 0))
            gather_start(by_cols)
            gather_forward(by_cols)
            send_wo(l + 1)
            send_gu(l + 1, AHEAD, "a")
            send_direct(l + 1, "b")
            gather_finish(by_cols)
            norm_all(ga, l + 1)

        @pl.when(l + 1 == LAYERS)
        def _():
            def residual(slot, carry):
                part[slot, :, mycols] = part[slot, :, mycols] + xcol[slot].astype(F32)
                return carry
            lax.fori_loop(0, DEV, residual, 0)
            last_block(1 - c)
            reduce_scatter(True, zb, wd, KPRE, lambda: last_block(c), lambda: None)

        bytes_wait(land_wo.at[l], ss_wo.at[l])
        bytes_wait(land_qkv.at[l, pl.ds(0, OTHER), :], ss_qkv.at[l])
        for n in range(NCH):
            bytes_wait(gu_bytes(l, n), ss_gu.at[l, n])
        return carry

    lax.fori_loop(0, LAYERS, layer, 0)
    bytes_wait(ga.at[pl.ds(0, DEV - 1)], s_gain.at[0])
    bytes_wait(gm.at[pl.ds(0, DEV - 1)], s_gain.at[1])


def solution(mesh):
    batch_spec = P(("dp", "fsdp"), None, None)
    gain_spec = P(None, "fsdp")
    proj_spec = P(None, "fsdp", None, None)
    mat_spec = P(None, "fsdp", None)
    cos, sin = rope_tables()

    def local_forward(hidden, attn_norm, w_q, w_k, w_v, w_o, mlp_norm, w_gate, w_up, w_down):
        hbm = pl.BlockSpec(memory_space=pltpu.HBM)
        vmem = pl.BlockSpec(memory_space=pltpu.VMEM)
        dma = pltpu.SemaphoreType.DMA
        out = pl.pallas_call(
            body,
            name="two_layers",
            out_shape=(pltpu.VMEM((SEQ, DIM), BF16),
                       jax.ShapeDtypeStruct((LAYERS, DEV, ROWS, QKV), BF16),
                       jax.ShapeDtypeStruct((LAYERS, DIM, QKV), BF16),
                       jax.ShapeDtypeStruct((LAYERS, DIM, 2 * FCOLS), BF16),
                       jax.ShapeDtypeStruct((LAYERS, ROWS, 2 * PAIR), BF16)),
            in_specs=[hbm] * 12,
            out_specs=(vmem, hbm, hbm, hbm, hbm),
            scratch_shapes=[
                pltpu.VMEM((2, RB, DEV * QH, HD), BF16),
                pltpu.VMEM((2, RB, DEV, HD), BF16),
                pltpu.VMEM((2, RB, DEV, HD), BF16),
                pltpu.VMEM((2, DEV, RB, QKV), BF16),
                pltpu.VMEM((DEV, SEQ, ROWS), BF16),
                pltpu.VMEM((DEV, SEQ, DIM), BF16),
                pltpu.VMEM((DEV, SEQ, DIM), F32),
                pltpu.VMEM((NP, CHIPS, 2, SEQ, ROWS), F32),
                pltpu.VMEM((NP, 2, 2, SEQ, ROWS), F32),
                pltpu.VMEM((NP, 2, SEQ, ROWS), F32),
                pltpu.VMEM((DIM, QKV), BF16),
                pltpu.VMEM((2 * ROWS, 2 * PAIR), BF16),
                pltpu.VMEM((FCOLS, DIM), BF16),
                pltpu.VMEM((2, DIM, WIDE), BF16),
                pltpu.VMEM((DIM, 2 * CHUNKS[LAST][1]), BF16),
                pltpu.VMEM((2, CHIPS * SEQ, 2 * CHUNKS[LAST][1]), F32),
                pltpu.VMEM((DEV, QH * SEQ, HD), BF16),
                pltpu.VMEM((DEV, SEQ, HD), BF16),
                pltpu.VMEM((DEV, SEQ, HD), BF16),
                pltpu.VMEM((DEV, SEQ, QCOLS), BF16),
                pltpu.VMEM((DEV, SEQ, QCOLS), BF16),
                pltpu.VMEM((DEV, SEQ, FCOLS), BF16),
                pltpu.VMEM((DEV, LAYERS, ROWS), BF16),
                pltpu.VMEM((DEV, LAYERS, ROWS), BF16),
                pltpu.VMEM((SEQ, HD), F32),
                pltpu.VMEM((SEQ, HD), F32),
                dma((LAYERS,)), dma((LAYERS,)), dma((LAYERS,)), dma((LAYERS,)), dma((2,)), dma((2,)), dma((LAYERS, NCH)), dma((LAYERS, NCH + 1)), dma((4,)), dma((7,)), dma((2 + len(GROUPS),)),
                dma((2, 3)), dma((2,)),
                dma((10,)), dma((10,)), dma((NP, 4)), dma((NP, 4)), dma((NP, 2)), dma((NP, 2)), dma((NP,)), dma((NP,)),
            ],
            compiler_params=pltpu.CompilerParams(collective_id=0, has_side_effects=True, vmem_limit_bytes=65_000_000),
        )(hidden[0], attn_norm, mlp_norm, cos, sin, w_q, w_k, w_v, w_o, w_gate, w_up, w_down)[0]
        return out[None]

    return jax.shard_map(local_forward, mesh=mesh, in_specs=(batch_spec, gain_spec, proj_spec, proj_spec, proj_spec, mat_spec, gain_spec, mat_spec, mat_spec, mat_spec), out_specs=batch_spec, check_vma=False)
```

```python
import functools

import jax
import jax.numpy as jnp
import numpy as np
from jax import lax
from jax.experimental import pallas as pl
from jax.experimental.pallas import tpu as pltpu
from jax.sharding import PartitionSpec as P

ROPE_THETA = 500000.0
NORM_EPS = 1e-5
MESH = pl.DeviceIdType.MESH
F32 = jnp.float32
BF16 = jnp.bfloat16

DEV = 8
CHIPS = 4
SEQ = 128
DIM = 3072
HALF = DIM // 2
ROWS = DIM // DEV
HD = 128
QH = 3
QCOLS = QH * HD
QKV = QCOLS + 2 * HD
FFN = 8192
FCOLS = FFN // DEV
PAIR = 2 * ROWS
CHUNKS = ((0, 128), (256, 256), (512, 256), (128, 128), (768, 128), (896, 128))
NCH = len(CHUNKS)
LAST = NCH - 1
GROUPS = (((1,), 0), ((2,), 1), ((0, 3), 0), ((4,), 1))
AHEAD = 3
WIDE = 512
SPLIT = (1, 2, 3, 4)
KPRE = CHUNKS[LAST - 1][0]
LAYERS = 2
RB = 96
NP = 4
PW = DIM // NP


def rope_tables():
    half = HD // 2
    inv_freq = np.power(np.float32(ROPE_THETA), -(np.arange(half, dtype=np.float32) * np.float32(2.0) / np.float32(HD)))
    angles = (np.arange(SEQ, dtype=np.float32)[:, None] * inv_freq.astype(np.float32)[None, :]).astype(np.float64)
    cos, sin = np.cos(angles).astype(np.float32), np.sin(angles).astype(np.float32)
    return np.concatenate([cos, cos], axis=1), np.concatenate([-sin, sin], axis=1)


def body(x_in, ga_in, gm_in, cos_in, sin_in, wq_in, wk_in, wv_in, wo_in, wg_in, wu_in, wd_in,
         out, stage_qkv, land_qkv, land_gu, land_wo,
         rq, rk, rv, st, xcol, u, part, rm, r1, r2, wqkv, wo, wd, wgu, wlast, lsum, qb, kb, vb, ob, ob2, zb, ga, gm, cos_t, sin_t,
         ss_qkv, rs_qkv, ss_wo, rs_wo, oe_s, oe_r, ss_gu, rs_gu, s_gain, l_sem, ld_sem,
         rl_in, rl_out, ag_s, ag_r, mt_s, mt_r, r1_s, r1_r, r2_s, r2_r):
    me = lax.axis_index("fsdp")
    c = me % 2
    cx = (me // 2) % 2
    cy = me // 4
    chip = me // 2

    def dev(fy, fx, fc):
        yy = 1 - cy if fy else cy
        xx = 1 - cx if fx else cx
        cc = 1 - c if fc else c
        return yy * 4 + xx * 2 + cc

    mate, xn, yn = dev(0, 0, 1), dev(0, 1, 0), dev(1, 0, 0)
    dn = dev(1, 1, 0)
    chip_x, chip_y, chip_d = xn // 2, yn // 2, dn // 2
    mycols = pl.ds(pl.multiple_of(me * ROWS, 128), ROWS)

    def axes(l):
        return yn + l * (xn - yn), xn + l * (yn - xn)
    flips = ((0, 1, 0), (1, 0, 0), (0, 1, 1), (1, 0, 1), (1, 1, 0), (1, 1, 1), (0, 0, 1))

    def remote(src, dst, ssem, rsem, target):
        return pltpu.make_async_remote_copy(src, dst, ssem, rsem, device_id={"fsdp": target}, device_id_type=MESH)

    def bytes_wait(ref, sem):
        pltpu.make_async_copy(ref, ref, sem).wait()

    barrier = pltpu.get_barrier_semaphore()
    for f in flips:
        pl.semaphore_signal(barrier, inc=1, device_id={"fsdp": dev(*f)}, device_id_type=MESH)
    pl.semaphore_wait(barrier, DEV - 1)

    def targets(l, which):
        if which is None:
            return [(dev(*f), f[0] and f[1]) for f in flips]
        an, bn = axes(l)
        e = {"a": an, "b": bn, "d": dn}[which]
        return [(e, which == "d"), (e + 1 - 2 * c, which == "d")] + ([(mate, False)] if which == "b" else [])

    def send_qkv(l, which=None):
        for e, diagonal in targets(l, which):
            remote(stage_qkv.at[l, e],
                   land_qkv.at[l, pl.ds(pl.multiple_of(me * ROWS, ROWS), ROWS), :],
                   ss_qkv.at[l], rs_qkv.at[l], e).start()

    def send_wo(l):
        an = axes(l)[0]
        for k, to in ((0, an // 2), (1, chip_d)):
            remote(wo_in.at[l, :, pl.ds(pl.multiple_of(to * PAIR, 128), PAIR)], land_wo.at[l, :, pl.ds(k * PAIR, PAIR)],
                   ss_wo.at[l], rs_wo.at[l], an).start()

    def load_wo(l):
        for k, of in ((0, chip), (1, axes(l)[1] // 2)):
            pltpu.make_async_copy(wo_in.at[l, :, pl.ds(pl.multiple_of(of * PAIR, 128), PAIR)],
                                  wo.at[pl.ds(0, ROWS), pl.ds(k * PAIR, PAIR)], l_sem.at[0]).start()
        pltpu.make_async_copy(land_wo.at[l], wo.at[pl.ds(ROWS, ROWS), :], l_sem.at[0]).start()

    def send_gu(l, n, which=None):
        off, w = CHUNKS[n]
        rows = pl.ds(pl.multiple_of(me * ROWS, ROWS), ROWS)
        for e, diagonal in targets(l, which):
            cols = pl.ds(pl.multiple_of(e * FCOLS + off, 128), w)
            for src, k in ((wg_in, 0), (wu_in, 1)):
                dst = wlast.at[rows, pl.ds(k * w, w)] if n == LAST else land_gu.at[l, rows, pl.ds(2 * off + k * w, w)]
                got = n + 1 if n == LAST and diagonal else n
                remote(src.at[l, :, cols], dst, ss_gu.at[l, n], rs_gu.at[l, got], e).start()

    def gu_bytes(l, n):
        off, w = CHUNKS[n]
        if n == LAST:
            return wlast.at[pl.ds(0, OTHER), :]
        return land_gu.at[l, pl.ds(0, OTHER), pl.ds(2 * off, 2 * w)]

    OTHER = (DEV - 1) * ROWS

    def load_qkv(l):
        for f in flips:
            rows = pl.ds(pl.multiple_of(dev(*f) * ROWS, ROWS), ROWS)
            pltpu.make_async_copy(land_qkv.at[l, rows, :], wqkv.at[rows, :], ld_sem.at[0]).start()
        mine = pl.ds(pl.multiple_of(me * ROWS, ROWS), ROWS)
        pltpu.make_async_copy(stage_qkv.at[l, me], wqkv.at[mine, :], ld_sem.at[0]).start()

    def own_gu(l, n, dst_of, sem):
        off, w = CHUNKS[n]
        cols = pl.ds(pl.multiple_of(me * FCOLS + off, 128), w)
        for src, k in ((wg_in, 0), (wu_in, 1)):
            pltpu.make_async_copy(src.at[l, :, cols], dst_of(k * w, w), sem).start()

    def own_last(l):
        mine = pl.ds(pl.multiple_of(me * ROWS, ROWS), ROWS)
        own_gu(l, LAST, lambda at, w: wlast.at[mine, pl.ds(at, w)], ld_sem.at[1 + len(GROUPS)])

    def group_cols(g):
        chunks = GROUPS[g][0]
        return 2 * CHUNKS[chunks[0]][0], 2 * sum(CHUNKS[n][1] for n in chunks)

    def group_arrives(l, g):
        chunks, slot = GROUPS[g]
        first, width = group_cols(g)
        sem = ld_sem.at[1 + g]
        for n in chunks:
            bytes_wait(gu_bytes(l, n), rs_gu.at[l, n])
        for f in flips:
            rows = pl.ds(pl.multiple_of(dev(*f) * ROWS, ROWS), ROWS)
            pltpu.make_async_copy(land_gu.at[l, rows, pl.ds(first, width)], wgu.at[slot, rows, pl.ds(0, width)], sem).start()
        mine = pl.ds(pl.multiple_of(me * ROWS, ROWS), ROWS)
        for n in chunks:
            base = 2 * CHUNKS[n][0] - first
            own_gu(l, n, lambda at, w, base=base: wgu.at[slot, mine, pl.ds(base + at, w)], sem)

    def relayout(l):
        def fetch(i):
            slot = i % 2
            rows = pl.ds(pl.multiple_of(i * RB, RB), RB)
            return [pltpu.make_async_copy(src.at[l, rows], dst.at[slot], rl_in.at[slot, k])
                    for k, (src, dst) in enumerate(((wq_in, rq), (wk_in, rk), (wv_in, rv)))]

        def put(i):
            slot = i % 2
            rows = pl.ds(pl.multiple_of(i * RB, RB), RB)
            return pltpu.make_async_copy(st.at[slot], stage_qkv.at[l, :, rows, :], rl_out.at[slot])

        steps = ROWS // RB
        for cp in fetch(0):
            cp.start()

        def step(i, carry):
            slot = i % 2

            @pl.when(i + 1 < steps)
            def _():
                for cp in fetch(i + 1):
                    cp.start()
            for cp in fetch(i):
                cp.wait()

            @pl.when(i >= 2)
            def _():
                put(i - 2).wait()

            def block(b, carry):
                rows = pl.ds(pl.multiple_of(b * 16, 16), 16)
                q = rq[slot, rows].astype(F32).reshape(16, DEV * QCOLS).astype(BF16)
                k = rk[slot, rows].astype(F32).reshape(16, DEV * HD).astype(BF16)
                v = rv[slot, rows].astype(F32).reshape(16, DEV * HD).astype(BF16)
                for e in range(DEV):
                    st[slot, e, rows, :QCOLS] = q[:, e * QCOLS:(e + 1) * QCOLS]
                    st[slot, e, rows, QCOLS:QCOLS + HD] = k[:, e * HD:(e + 1) * HD]
                    st[slot, e, rows, QCOLS + HD:] = v[:, e * HD:(e + 1) * HD]
                return carry
            lax.fori_loop(0, RB // 16, block, 0)
            put(i).start()
            return carry
        lax.fori_loop(0, steps, step, 0)
        put(steps - 2).wait()
        put(steps - 1).wait()

    my_slot = c * CHIPS + chip

    def norm_all(gains, l):
        def one(i, carry):
            slot = i // (SEQ // 16)
            rows = pl.ds(pl.multiple_of((i % (SEQ // 16)) * 16, 16), 16)
            wide = u[slot, rows, :].astype(F32)
            inv = lax.rsqrt(jnp.mean(wide * wide, axis=-1, keepdims=True) + NORM_EPS)
            for s in range(DEV):
                cols = slice(s * ROWS, (s + 1) * ROWS)
                both = gains[s].astype(F32)
                g = jnp.where(l == 0, both[0:1], both[1:2])
                u[slot, rows, cols] = (wide[:, cols] * inv * g).astype(BF16)
            return carry
        lax.fori_loop(0, DEV * SEQ // 16, one, 0)

    def by_rows(who, half):
        slot = c * CHIPS + {"me": chip, "x": chip_x, "y": chip_y, "d": chip_d}[who]
        return u.at[slot] if half is None else u.at[slot, :, pl.ds(half * HALF, HALF)]

    def by_cols(who, half):
        e = {"me": me, "x": xn, "y": yn, "d": dn}[who]
        cols = pl.ds(pl.multiple_of(e * ROWS, 128), ROWS)
        return u.at[:, :, cols] if half is None else u.at[pl.ds(half * CHIPS, CHIPS), :, cols]

    def u_copy(ref, k, target):
        return remote(ref, ref, ag_s.at[k], ag_r.at[k], target)

    def gather_start(at):
        u_copy(at("me", 0), 0, xn).start()
        u_copy(at("me", 1), 1, yn).start()
        u_copy(at("me", 1), 2, xn).start()
        u_copy(at("me", 0), 3, yn).start()
        u_copy(at("me", None), 6, mate).start()

    def gather_forward(at):
        u_copy(at("x", 0), 0, xn).wait_recv()
        u_copy(at("x", 0), 4, yn).start()
        u_copy(at("y", 1), 1, yn).wait_recv()
        u_copy(at("y", 1), 5, xn).start()

    def gather_finish(at):
        u_copy(at("x", 1), 2, xn).wait_recv()
        u_copy(at("x", None), 7, mate).start()
        u_copy(at("y", 0), 3, yn).wait_recv()
        u_copy(at("y", None), 8, mate).start()
        u_copy(at("d", 0), 4, yn).wait_recv()
        u_copy(at("d", 1), 5, xn).wait_recv()
        u_copy(at("d", None), 9, mate).start()
        for k in (6, 7, 8, 9):
            u_copy(at("me", None), k, mate).wait_recv()
        for k in range(6):
            u_copy(at("me", 0), k, xn).wait_send()
        for k in (6, 7, 8, 9):
            u_copy(at("me", None), k, mate).wait_send()

    def keep(slot, total):
        new = (xcol[slot].astype(F32) + total).astype(BF16)
        xcol[slot] = new
        u[slot, :, mycols] = new

    def out_proj(l, after_exchange, after_sums):
        an, bn = axes(l)

        def o_copy(g):
            return remote(ob.at[pl.ds(g * CHIPS, CHIPS)], ob2.at[pl.ds(g * CHIPS, CHIPS)], oe_s.at[g], oe_r.at[g], an)

        def mate_copy(p, b):
            return remote(part.at[pl.ds(2 * p, 2), :, pl.ds(pl.multiple_of(b * PAIR + (1 - c) * ROWS, 128), ROWS)], rm.at[p, b],
                          mt_s.at[p, b], mt_r.at[p, b], mate)

        def sums(p):
            return remote(part.at[pl.ds(2 * p, 2), :, pl.ds(pl.multiple_of(PAIR + c * ROWS, 128), ROWS)], r1.at[p, 0],
                          r1_s.at[p, 0], r1_r.at[p, 0], bn)

        def fold(p):
            mate_copy(p, 1).wait_recv()
            for t in range(2):
                cols = pl.ds(pl.multiple_of(PAIR + c * ROWS, 128), ROWS)
                part[2 * p + t, :, cols] = part[2 * p + t, :, cols] + rm[p, 1, t]
            sums(p).start()

        for g in range(2):
            o_copy(g).start()
        after_exchange()
        for p in range(NP):
            if p % 2 == 0:
                o_copy(p // 2).wait_recv()
            a = jnp.concatenate([r[pl.ds(2 * p, 2)].reshape(2 * SEQ, QCOLS) for r in (ob, ob2)], axis=1)
            for b in (1, 0):
                prod = jnp.dot(a, wo[:, b * PAIR:(b + 1) * PAIR], preferred_element_type=F32)
                part[pl.ds(2 * p, 2), :, b * PAIR:(b + 1) * PAIR] = prod.reshape(2, SEQ, PAIR)
                mate_copy(p, b).start()
            if p:
                fold(p - 1)
        fold(NP - 1)
        after_sums()
        for p in range(NP):
            mate_copy(p, 0).wait_recv()
            sums(p).wait_recv()
            for t in range(2):
                keep(2 * p + t, (part[2 * p + t, :, pl.ds(pl.multiple_of(c * ROWS, 128), ROWS)] + rm[p, 0, t]) + r1[p, 0, t])
        for g in range(2):
            o_copy(g).wait_send()
        for p in range(NP):
            for b in range(2):
                mate_copy(p, b).wait_send()
            sums(p).wait_send()

    def reduce_scatter(rows_form, act, rhs, k0, between, then):
        own, other = c, 1 - c
        order = ((chip_d, chip_x, chip_y, chip), (chip_d, chip_y, chip_x, chip))
        first = (xn, yn)
        second = (yn, xn)

        def sub(p, j, core, t):
            if rows_form:
                return core * CHIPS + j, pl.ds(p * PW + t * ROWS, ROWS)
            return 2 * p + t, pl.ds(pl.multiple_of(j * PAIR + core * ROWS, 128), ROWS)

        def pieces(p, j, core, dst, ssem, rsem, target):
            for t in range(2):
                slot, cols = sub(p, j, core, t)
                remote(part.at[slot, :, cols], dst.at[t], ssem, rsem, target).start()

        def unit(sem):
            bytes_wait(r2.at[0], sem)

        def send_mate(p, k):
            j = order[p % 2][k]
            pieces(p, j, other, rm.at[p, j], mt_s.at[p, k], mt_r.at[p, k], mate)

        def fold(p, k, extra):
            j = order[p % 2][k]
            for t in range(2):
                slot, cols = sub(p, j, own, t)
                total = part[slot, :, cols] + rm[p, j, t]
                part[slot, :, cols] = total if extra is None else total + extra[t]

        def products(p, grp, ks):
            slots = [grp * CHIPS + order[p % 2][k] for k in ks]
            a = jnp.concatenate([act[slot, :, k0:] for slot in slots], axis=0)
            cols = slice(p * PW, (p + 1) * PW)
            prod = jnp.dot(a, rhs[k0:, cols], preferred_element_type=F32)
            for i, slot in enumerate(slots):
                part[slot, :, cols] = part[slot, :, cols] + prod[i * SEQ:(i + 1) * SEQ]

        def column_products(p, k):
            cols = pl.ds(pl.multiple_of(order[p % 2][k] * PAIR, 128), PAIR)
            slots = pl.ds(2 * p, 2)
            prod = jnp.dot(act[slots, :, k0:].reshape(2 * SEQ, FCOLS - k0), rhs[k0:, cols], preferred_element_type=F32)
            part[slots, :, cols] = part[slots, :, cols] + prod.reshape(2, SEQ, PAIR)

        for pair in range(NP // 2):
            both = (2 * pair, 2 * pair + 1)
            for p in both:
                if rows_form:
                    products(p, other, (0, 1))
                else:
                    column_products(p, 0)
                send_mate(p, 0)
            for p in both:
                if not rows_form:
                    column_products(p, 1)
                send_mate(p, 1)
            if pair == 0 and between is not None:
                between()
            if rows_form:
                for p in both:
                    products(p, own, (0, 1))
            for k in (0, 1):
                for p in both:
                    unit(mt_r.at[p, k])
                    fold(p, k, None)
                    pieces(p, order[p % 2][k], own, r1.at[p, k], r1_s.at[p, k], r1_r.at[p, k], first[p % 2])
        for p in range(NP):
            if rows_form:
                products(p, other, (2, 3))
            for k in (2, 3):
                if not rows_form:
                    column_products(p, k)
                send_mate(p, k)
            if rows_form:
                products(p, own, (2, 3))
        for p in range(NP):
            unit(mt_r.at[p, 2])
            unit(r1_r.at[p, 0])
            fold(p, 2, r1.at[p, 0])
            pieces(p, order[p % 2][2], own, r2.at[p], r2_s.at[p], r2_r.at[p], second[p % 2])
        for p in range(NP):
            if p == NP // 2:
                then()
            unit(mt_r.at[p, 3])
            unit(r1_r.at[p, 1])
            unit(r2_r.at[p])
            for t in range(2):
                slot, cols = sub(p, chip, own, t)
                total = (part[slot, :, cols] + rm[p, chip, t]) + (r1[p, 1, t] + r2[p, t])
                if rows_form:
                    out[:, cols] = total.astype(BF16)
                else:
                    keep(slot, total)
        for p in range(NP):
            for k in range(4):
                unit(mt_s.at[p, k])
            for k in range(2):
                unit(r1_s.at[p, k])
            unit(r2_s.at[p])

    def send_direct(l, which):
        for n in SPLIT:
            send_gu(l, n, which)

    send_gu(0, 0)
    starts = [pltpu.make_async_copy(src, dst, l_sem.at[2 + k]) for k, (src, dst) in enumerate(
        ((x_in, u.at[my_slot]), (ga_in, ga.at[me]), (gm_in, gm.at[me]), (cos_in, cos_t), (sin_in, sin_t)))]
    for cp in starts:
        cp.start()
    for cp in starts:
        cp.wait()
    gather_start(by_rows)
    for src, dst, k in ((ga_in, ga, 0), (gm_in, gm, 1)):
        for f in flips:
            remote(src, dst.at[me], s_gain.at[k], s_gain.at[2 + k], dev(*f)).start()
    relayout(0)
    gather_forward(by_rows)
    send_qkv(0)
    send_wo(0)
    send_direct(0, "b")
    relayout(1)
    gather_finish(by_rows)
    bytes_wait(ga.at[pl.ds(0, DEV - 1)], s_gain.at[2])
    bytes_wait(gm.at[pl.ds(0, DEV - 1)], s_gain.at[3])

    def column_block(slot, carry):
        xcol[slot] = u[slot, :, mycols]
        return carry
    lax.fori_loop(0, DEV, column_block, 0)
    norm_all(ga, 0)

    def layer(l, carry):
        ld_d = pltpu.make_async_copy(wd_in.at[l], wd, l_sem.at[1])
        ld_d.start()
        bytes_wait(land_qkv.at[l, pl.ds(0, OTHER), :], rs_qkv.at[l])
        load_qkv(l)
        bytes_wait(wqkv, ld_sem.at[0])

        def qkv_block(i, carry):
            prod = jnp.dot(u[pl.ds(i * 2, 2)].reshape(2 * SEQ, DIM), wqkv[...], preferred_element_type=F32)
            cos, sin = cos_t[...], sin_t[...]
            for s in range(2):
                rows = slice(s * SEQ, (s + 1) * SEQ)
                for h in range(QH + 1):
                    head = prod[rows, h * HD:(h + 1) * HD]
                    rot = (head * cos + pltpu.roll(head, HD // 2, 1) * sin).astype(BF16)
                    if h < QH:
                        qb[i * 2 + s, pl.ds(h * SEQ, SEQ), :] = rot
                    else:
                        kb[i * 2 + s] = rot
                vb[i * 2 + s] = prod[rows, (QH + 1) * HD:].astype(BF16)
            return carry
        lax.fori_loop(0, DEV // 2, qkv_block, 0)

        def attend(s, carry):
            scores = lax.dot_general(qb[s], kb[s], (((1,), (1,)), ((), ())), preferred_element_type=F32) * HD ** -0.5
            row = lax.broadcasted_iota(jnp.int32, (QH * SEQ, SEQ), 0) % SEQ
            col = lax.broadcasted_iota(jnp.int32, (QH * SEQ, SEQ), 1)
            scores = jnp.where(row >= col, scores, -jnp.inf)
            e = jnp.exp(scores - jnp.max(scores, axis=-1, keepdims=True))
            probs = (e / jnp.sum(e, axis=-1, keepdims=True)).astype(BF16)
            o = jnp.dot(probs, vb[s], preferred_element_type=F32).astype(BF16)
            for h in range(QH):
                ob[s, :, h * HD:(h + 1) * HD] = o[h * SEQ:(h + 1) * SEQ]
            return carry
        lax.fori_loop(0, DEV, attend, 0)

        def after_exchange():
            for n in SPLIT:
                if n != AHEAD:
                    send_gu(l, n, "a")

            @pl.when(l == 0)
            def _():
                send_gu(l, AHEAD, "a")

            bytes_wait(land_wo.at[l], rs_wo.at[l])
            load_wo(l)
            bytes_wait(wo, l_sem.at[0])

        out_proj(l, after_exchange, lambda: None)

        gather_start(by_cols)
        gather_forward(by_cols)
        for which in ("a", "b"):
            send_gu(l, LAST, which)
        send_direct(l, "d")
        send_gu(l, LAST, "d")

        @pl.when(l + 1 < LAYERS)
        def _():
            send_qkv(l + 1)

        own_last(l)
        gather_finish(by_cols)
        norm_all(gm, l)
        group_arrives(l, 0)

        def activate(prod, n, i):
            off, w = CHUNKS[n]
            gate = prod[:, :w].astype(BF16).astype(F32)
            up = prod[:, w:].astype(BF16).astype(F32)
            z = (gate * jax.nn.sigmoid(gate) * up).astype(BF16)
            zb[pl.ds(i * CHIPS, CHIPS), :, off:off + w] = z.reshape(CHIPS, SEQ, w)

        def mlp_group(g):
            chunks, slot = GROUPS[g]
            first, width = group_cols(g)
            bytes_wait(wgu.at[slot, :, pl.ds(0, width)], ld_sem.at[1 + g])

            def block(i, carry):
                rows = u[pl.ds(i * CHIPS, CHIPS)].reshape(CHIPS * SEQ, DIM)
                prod = jnp.dot(rows, wgu[slot, :, :width], preferred_element_type=F32)
                for n in chunks:
                    base = 2 * CHUNKS[n][0] - first
                    activate(prod[:, base:base + 2 * CHUNKS[n][1]], n, i)
                return carry
            lax.fori_loop(0, 2, block, 0)

        def last_term(i, k):
            depth = pl.ds(pl.multiple_of(k * PAIR, PAIR), PAIR)
            rows = u[pl.ds(i * CHIPS, CHIPS), :, depth].reshape(CHIPS * SEQ, PAIR)
            return jnp.dot(rows, wlast[depth, :], preferred_element_type=F32)

        def last_near(i, carry):
            lsum[i] = (last_term(i, chip) + last_term(i, chip_x)) + last_term(i, chip_y)
            return carry

        def last_block(i):
            activate(lsum[i] + last_term(i, chip_d), LAST, i)

        mlp_group(0)
        group_arrives(l, 1)
        mlp_group(1)
        group_arrives(l, 2)
        mlp_group(2)
        ld_d.wait()

        def before_last(i, carry):
            slots = pl.ds(i * CHIPS, CHIPS)
            z = zb[slots, :, :KPRE].reshape(CHIPS * SEQ, KPRE)
            for p in range(NP):
                prod = jnp.dot(z, wd[:KPRE, p * PW:(p + 1) * PW], preferred_element_type=F32)
                part[slots, :, p * PW:(p + 1) * PW] = prod.reshape(CHIPS, SEQ, PW)
            return carry
        lax.fori_loop(0, 2, before_last, 0)
        group_arrives(l, 3)
        bytes_wait(wlast.at[pl.ds(0, OTHER - PAIR), :], rs_gu.at[l, LAST])
        bytes_wait(wlast.at[pl.ds(0, ROWS), :], ld_sem.at[1 + len(GROUPS)])
        lax.fori_loop(0, 2, last_near, 0)
        mlp_group(3)
        bytes_wait(wlast.at[pl.ds(0, PAIR), :], rs_gu.at[l, LAST + 1])

        @pl.when(l + 1 < LAYERS)
        def _():
            last_block(0)
            last_block(1)
            reduce_scatter(False, zb, wd, KPRE, None, lambda: send_gu(l + 1, 0))
            gather_start(by_cols)
            gather_forward(by_cols)
            send_wo(l + 1)
            send_gu(l + 1, AHEAD, "a")
            send_direct(l + 1, "b")
            gather_finish(by_cols)
            norm_all(ga, l + 1)

        @pl.when(l + 1 == LAYERS)
        def _():
            def residual(slot, carry):
                part[slot, :, mycols] = part[slot, :, mycols] + xcol[slot].astype(F32)
                return carry
            lax.fori_loop(0, DEV, residual, 0)
            last_block(1 - c)
            reduce_scatter(True, zb, wd, KPRE, lambda: last_block(c), lambda: None)

        bytes_wait(land_wo.at[l], ss_wo.at[l])
        bytes_wait(land_qkv.at[l, pl.ds(0, OTHER), :], ss_qkv.at[l])
        for n in range(NCH):
            bytes_wait(gu_bytes(l, n), ss_gu.at[l, n])
        return carry

    lax.fori_loop(0, LAYERS, layer, 0)
    bytes_wait(ga.at[pl.ds(0, DEV - 1)], s_gain.at[0])
    bytes_wait(gm.at[pl.ds(0, DEV - 1)], s_gain.at[1])


def solution(mesh):
    batch_spec = P(("dp", "fsdp"), None, None)
    gain_spec = P(None, "fsdp")
    proj_spec = P(None, "fsdp", None, None)
    mat_spec = P(None, "fsdp", None)
    cos, sin = rope_tables()

    def local_forward(hidden, attn_norm, w_q, w_k, w_v, w_o, mlp_norm, w_gate, w_up, w_down):
        hbm = pl.BlockSpec(memory_space=pltpu.HBM)
        vmem = pl.BlockSpec(memory_space=pltpu.VMEM)
        dma = pltpu.SemaphoreType.DMA
        out = pl.pallas_call(
            body,
            name="two_layers",
            out_shape=(pltpu.VMEM((SEQ, DIM), BF16),
                       jax.ShapeDtypeStruct((LAYERS, DEV, ROWS, QKV), BF16),
                       jax.ShapeDtypeStruct((LAYERS, DIM, QKV), BF16),
                       jax.ShapeDtypeStruct((LAYERS, DIM, 2 * FCOLS), BF16),
                       jax.ShapeDtypeStruct((LAYERS, ROWS, 2 * PAIR), BF16)),
            in_specs=[hbm] * 12,
            out_specs=(vmem, hbm, hbm, hbm, hbm),
            scratch_shapes=[
                pltpu.VMEM((2, RB, DEV * QH, HD), BF16),
                pltpu.VMEM((2, RB, DEV, HD), BF16),
                pltpu.VMEM((2, RB, DEV, HD), BF16),
                pltpu.VMEM((2, DEV, RB, QKV), BF16),
                pltpu.VMEM((DEV, SEQ, ROWS), BF16),
                pltpu.VMEM((DEV, SEQ, DIM), BF16),
                pltpu.VMEM((DEV, SEQ, DIM), F32),
                pltpu.VMEM((NP, CHIPS, 2, SEQ, ROWS), F32),
                pltpu.VMEM((NP, 2, 2, SEQ, ROWS), F32),
                pltpu.VMEM((NP, 2, SEQ, ROWS), F32),
                pltpu.VMEM((DIM, QKV), BF16),
                pltpu.VMEM((2 * ROWS, 2 * PAIR), BF16),
                pltpu.VMEM((FCOLS, DIM), BF16),
                pltpu.VMEM((2, DIM, WIDE), BF16),
                pltpu.VMEM((DIM, 2 * CHUNKS[LAST][1]), BF16),
                pltpu.VMEM((2, CHIPS * SEQ, 2 * CHUNKS[LAST][1]), F32),
                pltpu.VMEM((DEV, QH * SEQ, HD), BF16),
                pltpu.VMEM((DEV, SEQ, HD), BF16),
                pltpu.VMEM((DEV, SEQ, HD), BF16),
                pltpu.VMEM((DEV, SEQ, QCOLS), BF16),
                pltpu.VMEM((DEV, SEQ, QCOLS), BF16),
                pltpu.VMEM((DEV, SEQ, FCOLS), BF16),
                pltpu.VMEM((DEV, LAYERS, ROWS), BF16),
                pltpu.VMEM((DEV, LAYERS, ROWS), BF16),
                pltpu.VMEM((SEQ, HD), F32),
                pltpu.VMEM((SEQ, HD), F32),
                dma((LAYERS,)), dma((LAYERS,)), dma((LAYERS,)), dma((LAYERS,)), dma((2,)), dma((2,)), dma((LAYERS, NCH)), dma((LAYERS, NCH + 1)), dma((4,)), dma((7,)), dma((2 + len(GROUPS),)),
                dma((2, 3)), dma((2,)),
                dma((10,)), dma((10,)), dma((NP, 4)), dma((NP, 4)), dma((NP, 2)), dma((NP, 2)), dma((NP,)), dma((NP,)),
            ],
            compiler_params=pltpu.CompilerParams(collective_id=0, has_side_effects=True, vmem_limit_bytes=65_000_000),
        )(hidden[0], attn_norm, mlp_norm, cos, sin, w_q, w_k, w_v, w_o, w_gate, w_up, w_down)[0]
        return out[None]

    return jax.shard_map(local_forward, mesh=mesh, in_specs=(batch_spec, gain_spec, proj_spec, proj_spec, proj_spec, mat_spec, gain_spec, mat_spec, mat_spec, mat_spec), out_specs=batch_spec, check_vma=False)
```

```python
import functools

import jax
import jax.numpy as jnp
import numpy as np
from jax import lax
from jax.experimental import pallas as pl
from jax.experimental.pallas import tpu as pltpu
from jax.sharding import PartitionSpec as P

ROPE_THETA = 500000.0
NORM_EPS = 1e-5
MESH = pl.DeviceIdType.MESH
F32 = jnp.float32
BF16 = jnp.bfloat16

DEV = 8
CHIPS = 4
SEQ = 128
DIM = 3072
HALF = DIM // 2
ROWS = DIM // DEV
HD = 128
QH = 3
QCOLS = QH * HD
QKV = QCOLS + 2 * HD
FFN = 8192
FCOLS = FFN // DEV
PAIR = 2 * ROWS
CHUNKS = ((0, 128), (256, 256), (512, 256), (128, 128), (768, 128), (896, 128))
NCH = len(CHUNKS)
LAST = NCH - 1
GROUPS = (((1,), 0), ((2,), 1), ((0, 3), 0), ((4,), 1))
AHEAD = (3, 4)
WIDE = 512
SPLIT = (1, 2, 3, 4)
KPRE = CHUNKS[LAST - 1][0]
LAYERS = 2
RB = 96
NP = 4
PW = DIM // NP


def rope_tables():
    half = HD // 2
    inv_freq = np.power(np.float32(ROPE_THETA), -(np.arange(half, dtype=np.float32) * np.float32(2.0) / np.float32(HD)))
    angles = (np.arange(SEQ, dtype=np.float32)[:, None] * inv_freq.astype(np.float32)[None, :]).astype(np.float64)
    cos, sin = np.cos(angles).astype(np.float32), np.sin(angles).astype(np.float32)
    return np.concatenate([cos, cos], axis=1), np.concatenate([-sin, sin], axis=1)


def body(x_in, ga_in, gm_in, cos_in, sin_in, wq_in, wk_in, wv_in, wo_in, wg_in, wu_in, wd_in,
         out, stage_qkv, land_qkv, land_gu, land_wo,
         rq, rk, rv, st, xcol, u, part, rm, r1, r2, wqkv, wo, wd, wgu, wlast, lsum, qb, kb, vb, ob, ob2, zb, ga, gm, cos_t, sin_t,
         ss_qkv, rs_qkv, ss_wo, rs_wo, oe_s, oe_r, ss_gu, rs_gu, s_gain, l_sem, ld_sem,
         rl_in, rl_out, ag_s, ag_r, mt_s, mt_r, r1_s, r1_r, r2_s, r2_r):
    me = lax.axis_index("fsdp")
    c = me % 2
    cx = (me // 2) % 2
    cy = me // 4
    chip = me // 2

    def dev(fy, fx, fc):
        yy = 1 - cy if fy else cy
        xx = 1 - cx if fx else cx
        cc = 1 - c if fc else c
        return yy * 4 + xx * 2 + cc

    mate, xn, yn = dev(0, 0, 1), dev(0, 1, 0), dev(1, 0, 0)
    dn = dev(1, 1, 0)
    chip_x, chip_y, chip_d = xn // 2, yn // 2, dn // 2
    mycols = pl.ds(pl.multiple_of(me * ROWS, 128), ROWS)

    def axes(l):
        return yn + l * (xn - yn), xn + l * (yn - xn)
    flips = ((0, 1, 0), (1, 0, 0), (0, 1, 1), (1, 0, 1), (1, 1, 0), (1, 1, 1), (0, 0, 1))

    def remote(src, dst, ssem, rsem, target):
        return pltpu.make_async_remote_copy(src, dst, ssem, rsem, device_id={"fsdp": target}, device_id_type=MESH)

    def bytes_wait(ref, sem):
        pltpu.make_async_copy(ref, ref, sem).wait()

    barrier = pltpu.get_barrier_semaphore()
    for f in flips:
        pl.semaphore_signal(barrier, inc=1, device_id={"fsdp": dev(*f)}, device_id_type=MESH)
    pl.semaphore_wait(barrier, DEV - 1)

    def targets(l, which):
        if which is None:
            return [(dev(*f), f[0] and f[1]) for f in flips]
        an, bn = axes(l)
        e = {"a": an, "b": bn, "d": dn}[which]
        return [(e, which == "d"), (e + 1 - 2 * c, which == "d")] + ([(mate, False)] if which == "b" else [])

    def send_qkv(l, which=None):
        for e, diagonal in targets(l, which):
            remote(stage_qkv.at[l, e],
                   land_qkv.at[l, pl.ds(pl.multiple_of(me * ROWS, ROWS), ROWS), :],
                   ss_qkv.at[l], rs_qkv.at[l], e).start()

    def send_wo(l):
        an = axes(l)[0]
        for k, to in ((0, an // 2), (1, chip_d)):
            remote(wo_in.at[l, :, pl.ds(pl.multiple_of(to * PAIR, 128), PAIR)], land_wo.at[l, :, pl.ds(k * PAIR, PAIR)],
                   ss_wo.at[l], rs_wo.at[l], an).start()

    def load_wo(l):
        for k, of in ((0, chip), (1, axes(l)[1] // 2)):
            pltpu.make_async_copy(wo_in.at[l, :, pl.ds(pl.multiple_of(of * PAIR, 128), PAIR)],
                                  wo.at[pl.ds(0, ROWS), pl.ds(k * PAIR, PAIR)], l_sem.at[0]).start()
        pltpu.make_async_copy(land_wo.at[l], wo.at[pl.ds(ROWS, ROWS), :], l_sem.at[0]).start()

    def send_gu(l, n, which=None):
        off, w = CHUNKS[n]
        rows = pl.ds(pl.multiple_of(me * ROWS, ROWS), ROWS)
        for e, diagonal in targets(l, which):
            cols = pl.ds(pl.multiple_of(e * FCOLS + off, 128), w)
            for src, k in ((wg_in, 0), (wu_in, 1)):
                dst = wlast.at[rows, pl.ds(k * w, w)] if n == LAST else land_gu.at[l, rows, pl.ds(2 * off + k * w, w)]
                got = n + 1 if n == LAST and diagonal else n
                remote(src.at[l, :, cols], dst, ss_gu.at[l, n], rs_gu.at[l, got], e).start()

    def gu_bytes(l, n):
        off, w = CHUNKS[n]
        if n == LAST:
            return wlast.at[pl.ds(0, OTHER), :]
        return land_gu.at[l, pl.ds(0, OTHER), pl.ds(2 * off, 2 * w)]

    OTHER = (DEV - 1) * ROWS

    def load_qkv(l):
        for f in flips:
            rows = pl.ds(pl.multiple_of(dev(*f) * ROWS, ROWS), ROWS)
            pltpu.make_async_copy(land_qkv.at[l, rows, :], wqkv.at[rows, :], ld_sem.at[0]).start()
        mine = pl.ds(pl.multiple_of(me * ROWS, ROWS), ROWS)
        pltpu.make_async_copy(stage_qkv.at[l, me], wqkv.at[mine, :], ld_sem.at[0]).start()

    def own_gu(l, n, dst_of, sem):
        off, w = CHUNKS[n]
        cols = pl.ds(pl.multiple_of(me * FCOLS + off, 128), w)
        for src, k in ((wg_in, 0), (wu_in, 1)):
            pltpu.make_async_copy(src.at[l, :, cols], dst_of(k * w, w), sem).start()

    def own_last(l):
        mine = pl.ds(pl.multiple_of(me * ROWS, ROWS), ROWS)
        own_gu(l, LAST, lambda at, w: wlast.at[mine, pl.ds(at, w)], ld_sem.at[1 + len(GROUPS)])

    def group_cols(g):
        chunks = GROUPS[g][0]
        return 2 * CHUNKS[chunks[0]][0], 2 * sum(CHUNKS[n][1] for n in chunks)

    def group_arrives(l, g):
        chunks, slot = GROUPS[g]
        first, width = group_cols(g)
        sem = ld_sem.at[1 + g]
        for n in chunks:
            bytes_wait(gu_bytes(l, n), rs_gu.at[l, n])
        for f in flips:
            rows = pl.ds(pl.multiple_of(dev(*f) * ROWS, ROWS), ROWS)
            pltpu.make_async_copy(land_gu.at[l, rows, pl.ds(first, width)], wgu.at[slot, rows, pl.ds(0, width)], sem).start()
        mine = pl.ds(pl.multiple_of(me * ROWS, ROWS), ROWS)
        for n in chunks:
            base = 2 * CHUNKS[n][0] - first
            own_gu(l, n, lambda at, w, base=base: wgu.at[slot, mine, pl.ds(base + at, w)], sem)

    def relayout(l):
        def fetch(i):
            slot = i % 2
            rows = pl.ds(pl.multiple_of(i * RB, RB), RB)
            return [pltpu.make_async_copy(src.at[l, rows], dst.at[slot], rl_in.at[slot, k])
                    for k, (src, dst) in enumerate(((wq_in, rq), (wk_in, rk), (wv_in, rv)))]

        def put(i):
            slot = i % 2
            rows = pl.ds(pl.multiple_of(i * RB, RB), RB)
            return pltpu.make_async_copy(st.at[slot], stage_qkv.at[l, :, rows, :], rl_out.at[slot])

        steps = ROWS // RB
        for cp in fetch(0):
            cp.start()

        def step(i, carry):
            slot = i % 2

            @pl.when(i + 1 < steps)
            def _():
                for cp in fetch(i + 1):
                    cp.start()
            for cp in fetch(i):
                cp.wait()

            @pl.when(i >= 2)
            def _():
                put(i - 2).wait()

            def block(b, carry):
                rows = pl.ds(pl.multiple_of(b * 16, 16), 16)
                q = rq[slot, rows].astype(F32).reshape(16, DEV * QCOLS).astype(BF16)
                k = rk[slot, rows].astype(F32).reshape(16, DEV * HD).astype(BF16)
                v = rv[slot, rows].astype(F32).reshape(16, DEV * HD).astype(BF16)
                for e in range(DEV):
                    st[slot, e, rows, :QCOLS] = q[:, e * QCOLS:(e + 1) * QCOLS]
                    st[slot, e, rows, QCOLS:QCOLS + HD] = k[:, e * HD:(e + 1) * HD]
                    st[slot, e, rows, QCOLS + HD:] = v[:, e * HD:(e + 1) * HD]
                return carry
            lax.fori_loop(0, RB // 16, block, 0)
            put(i).start()
            return carry
        lax.fori_loop(0, steps, step, 0)
        put(steps - 2).wait()
        put(steps - 1).wait()

    my_slot = c * CHIPS + chip

    def norm_all(gains, l):
        def one(i, carry):
            slot = i // (SEQ // 16)
            rows = pl.ds(pl.multiple_of((i % (SEQ // 16)) * 16, 16), 16)
            wide = u[slot, rows, :].astype(F32)
            inv = lax.rsqrt(jnp.mean(wide * wide, axis=-1, keepdims=True) + NORM_EPS)
            for s in range(DEV):
                cols = slice(s * ROWS, (s + 1) * ROWS)
                both = gains[s].astype(F32)
                g = jnp.where(l == 0, both[0:1], both[1:2])
                u[slot, rows, cols] = (wide[:, cols] * inv * g).astype(BF16)
            return carry
        lax.fori_loop(0, DEV * SEQ // 16, one, 0)

    def by_rows(who, half):
        slot = c * CHIPS + {"me": chip, "x": chip_x, "y": chip_y, "d": chip_d}[who]
        return u.at[slot] if half is None else u.at[slot, :, pl.ds(half * HALF, HALF)]

    def by_cols(who, half):
        e = {"me": me, "x": xn, "y": yn, "d": dn}[who]
        cols = pl.ds(pl.multiple_of(e * ROWS, 128), ROWS)
        return u.at[:, :, cols] if half is None else u.at[pl.ds(half * CHIPS, CHIPS), :, cols]

    def u_copy(ref, k, target):
        return remote(ref, ref, ag_s.at[k], ag_r.at[k], target)

    def gather_start(at):
        u_copy(at("me", 0), 0, xn).start()
        u_copy(at("me", 1), 1, yn).start()
        u_copy(at("me", 1), 2, xn).start()
        u_copy(at("me", 0), 3, yn).start()
        u_copy(at("me", None), 6, mate).start()

    def gather_forward(at):
        u_copy(at("x", 0), 0, xn).wait_recv()
        u_copy(at("x", 0), 4, yn).start()
        u_copy(at("y", 1), 1, yn).wait_recv()
        u_copy(at("y", 1), 5, xn).start()

    def gather_finish(at):
        u_copy(at("x", 1), 2, xn).wait_recv()
        u_copy(at("x", None), 7, mate).start()
        u_copy(at("y", 0), 3, yn).wait_recv()
        u_copy(at("y", None), 8, mate).start()
        u_copy(at("d", 0), 4, yn).wait_recv()
        u_copy(at("d", 1), 5, xn).wait_recv()
        u_copy(at("d", None), 9, mate).start()
        for k in (6, 7, 8, 9):
            u_copy(at("me", None), k, mate).wait_recv()
        for k in range(6):
            u_copy(at("me", 0), k, xn).wait_send()
        for k in (6, 7, 8, 9):
            u_copy(at("me", None), k, mate).wait_send()

    def keep(slot, total):
        new = (xcol[slot].astype(F32) + total).astype(BF16)
        xcol[slot] = new
        u[slot, :, mycols] = new

    def out_proj(l, after_exchange, after_sums):
        an, bn = axes(l)

        def o_copy(g):
            return remote(ob.at[pl.ds(g * CHIPS, CHIPS)], ob2.at[pl.ds(g * CHIPS, CHIPS)], oe_s.at[g], oe_r.at[g], an)

        def mate_copy(p, b):
            return remote(part.at[pl.ds(2 * p, 2), :, pl.ds(pl.multiple_of(b * PAIR + (1 - c) * ROWS, 128), ROWS)], rm.at[p, b],
                          mt_s.at[p, b], mt_r.at[p, b], mate)

        def sums(p):
            return remote(part.at[pl.ds(2 * p, 2), :, pl.ds(pl.multiple_of(PAIR + c * ROWS, 128), ROWS)], r1.at[p, 0],
                          r1_s.at[p, 0], r1_r.at[p, 0], bn)

        def fold(p):
            mate_copy(p, 1).wait_recv()
            for t in range(2):
                cols = pl.ds(pl.multiple_of(PAIR + c * ROWS, 128), ROWS)
                part[2 * p + t, :, cols] = part[2 * p + t, :, cols] + rm[p, 1, t]
            sums(p).start()

        for g in range(2):
            o_copy(g).start()
        after_exchange()
        for p in range(NP):
            if p % 2 == 0:
                o_copy(p // 2).wait_recv()
            a = jnp.concatenate([r[pl.ds(2 * p, 2)].reshape(2 * SEQ, QCOLS) for r in (ob, ob2)], axis=1)
            for b in (1, 0):
                prod = jnp.dot(a, wo[:, b * PAIR:(b + 1) * PAIR], preferred_element_type=F32)
                part[pl.ds(2 * p, 2), :, b * PAIR:(b + 1) * PAIR] = prod.reshape(2, SEQ, PAIR)
                mate_copy(p, b).start()
            if p:
                fold(p - 1)
        fold(NP - 1)
        after_sums()
        for p in range(NP):
            mate_copy(p, 0).wait_recv()
            sums(p).wait_recv()
            for t in range(2):
                keep(2 * p + t, (part[2 * p + t, :, pl.ds(pl.multiple_of(c * ROWS, 128), ROWS)] + rm[p, 0, t]) + r1[p, 0, t])
        for g in range(2):
            o_copy(g).wait_send()
        for p in range(NP):
            for b in range(2):
                mate_copy(p, b).wait_send()
            sums(p).wait_send()

    def reduce_scatter(rows_form, act, rhs, k0, between, then):
        own, other = c, 1 - c
        order = ((chip_d, chip_x, chip_y, chip), (chip_d, chip_y, chip_x, chip))
        first = (xn, yn)
        second = (yn, xn)

        def sub(p, j, core, t):
            if rows_form:
                return core * CHIPS + j, pl.ds(p * PW + t * ROWS, ROWS)
            return 2 * p + t, pl.ds(pl.multiple_of(j * PAIR + core * ROWS, 128), ROWS)

        def pieces(p, j, core, dst, ssem, rsem, target):
            for t in range(2):
                slot, cols = sub(p, j, core, t)
                remote(part.at[slot, :, cols], dst.at[t], ssem, rsem, target).start()

        def unit(sem):
            bytes_wait(r2.at[0], sem)

        def send_mate(p, k):
            j = order[p % 2][k]
            pieces(p, j, other, rm.at[p, j], mt_s.at[p, k], mt_r.at[p, k], mate)

        def fold(p, k, extra):
            j = order[p % 2][k]
            for t in range(2):
                slot, cols = sub(p, j, own, t)
                total = part[slot, :, cols] + rm[p, j, t]
                part[slot, :, cols] = total if extra is None else total + extra[t]

        def products(p, grp, ks):
            slots = [grp * CHIPS + order[p % 2][k] for k in ks]
            a = jnp.concatenate([act[slot, :, k0:] for slot in slots], axis=0)
            cols = slice(p * PW, (p + 1) * PW)
            prod = jnp.dot(a, rhs[k0:, cols], preferred_element_type=F32)
            for i, slot in enumerate(slots):
                part[slot, :, cols] = part[slot, :, cols] + prod[i * SEQ:(i + 1) * SEQ]

        def column_products(p, k):
            cols = pl.ds(pl.multiple_of(order[p % 2][k] * PAIR, 128), PAIR)
            slots = pl.ds(2 * p, 2)
            prod = jnp.dot(act[slots, :, k0:].reshape(2 * SEQ, FCOLS - k0), rhs[k0:, cols], preferred_element_type=F32)
            part[slots, :, cols] = part[slots, :, cols] + prod.reshape(2, SEQ, PAIR)

        for pair in range(NP // 2):
            both = (2 * pair, 2 * pair + 1)
            for p in both:
                if rows_form:
                    products(p, other, (0, 1))
                else:
                    column_products(p, 0)
                send_mate(p, 0)
            for p in both:
                if not rows_form:
                    column_products(p, 1)
                send_mate(p, 1)
            if pair == 0 and between is not None:
                between()
            if rows_form:
                for p in both:
                    products(p, own, (0, 1))
            for k in (0, 1):
                for p in both:
                    unit(mt_r.at[p, k])
                    fold(p, k, None)
                    pieces(p, order[p % 2][k], own, r1.at[p, k], r1_s.at[p, k], r1_r.at[p, k], first[p % 2])
        for p in range(NP):
            if rows_form:
                products(p, other, (2, 3))
            for k in (2, 3):
                if not rows_form:
                    column_products(p, k)
                send_mate(p, k)
            if rows_form:
                products(p, own, (2, 3))
        for p in range(NP):
            unit(mt_r.at[p, 2])
            unit(r1_r.at[p, 0])
            fold(p, 2, r1.at[p, 0])
            pieces(p, order[p % 2][2], own, r2.at[p], r2_s.at[p], r2_r.at[p], second[p % 2])
        for p in range(NP):
            if p == NP // 2:
                then()
            unit(mt_r.at[p, 3])
            unit(r1_r.at[p, 1])
            unit(r2_r.at[p])
            for t in range(2):
                slot, cols = sub(p, chip, own, t)
                total = (part[slot, :, cols] + rm[p, chip, t]) + (r1[p, 1, t] + r2[p, t])
                if rows_form:
                    out[:, cols] = total.astype(BF16)
                else:
                    keep(slot, total)
        for p in range(NP):
            for k in range(4):
                unit(mt_s.at[p, k])
            for k in range(2):
                unit(r1_s.at[p, k])
            unit(r2_s.at[p])

    def send_direct(l, which):
        for n in SPLIT:
            send_gu(l, n, which)

    send_gu(0, 0)
    starts = [pltpu.make_async_copy(src, dst, l_sem.at[2 + k]) for k, (src, dst) in enumerate(
        ((x_in, u.at[my_slot]), (ga_in, ga.at[me]), (gm_in, gm.at[me]), (cos_in, cos_t), (sin_in, sin_t)))]
    for cp in starts:
        cp.start()
    for cp in starts:
        cp.wait()
    gather_start(by_rows)
    for src, dst, k in ((ga_in, ga, 0), (gm_in, gm, 1)):
        for f in flips:
            remote(src, dst.at[me], s_gain.at[k], s_gain.at[2 + k], dev(*f)).start()
    relayout(0)
    gather_forward(by_rows)
    send_qkv(0)
    send_wo(0)
    send_direct(0, "b")
    relayout(1)
    gather_finish(by_rows)
    bytes_wait(ga.at[pl.ds(0, DEV - 1)], s_gain.at[2])
    bytes_wait(gm.at[pl.ds(0, DEV - 1)], s_gain.at[3])

    def column_block(slot, carry):
        xcol[slot] = u[slot, :, mycols]
        return carry
    lax.fori_loop(0, DEV, column_block, 0)
    norm_all(ga, 0)

    def layer(l, carry):
        ld_d = pltpu.make_async_copy(wd_in.at[l], wd, l_sem.at[1])
        ld_d.start()
        bytes_wait(land_qkv.at[l, pl.ds(0, OTHER), :], rs_qkv.at[l])
        load_qkv(l)
        bytes_wait(wqkv, ld_sem.at[0])

        def qkv_block(i, carry):
            prod = jnp.dot(u[pl.ds(i * 2, 2)].reshape(2 * SEQ, DIM), wqkv[...], preferred_element_type=F32)
            cos, sin = cos_t[...], sin_t[...]
            for s in range(2):
                rows = slice(s * SEQ, (s + 1) * SEQ)
                for h in range(QH + 1):
                    head = prod[rows, h * HD:(h + 1) * HD]
                    rot = (head * cos + pltpu.roll(head, HD // 2, 1) * sin).astype(BF16)
                    if h < QH:
                        qb[i * 2 + s, pl.ds(h * SEQ, SEQ), :] = rot
                    else:
                        kb[i * 2 + s] = rot
                vb[i * 2 + s] = prod[rows, (QH + 1) * HD:].astype(BF16)
            return carry
        lax.fori_loop(0, DEV // 2, qkv_block, 0)

        def attend(s, carry):
            scores = lax.dot_general(qb[s], kb[s], (((1,), (1,)), ((), ())), preferred_element_type=F32) * HD ** -0.5
            row = lax.broadcasted_iota(jnp.int32, (QH * SEQ, SEQ), 0) % SEQ
            col = lax.broadcasted_iota(jnp.int32, (QH * SEQ, SEQ), 1)
            scores = jnp.where(row >= col, scores, -jnp.inf)
            e = jnp.exp(scores - jnp.max(scores, axis=-1, keepdims=True))
            probs = (e / jnp.sum(e, axis=-1, keepdims=True)).astype(BF16)
            o = jnp.dot(probs, vb[s], preferred_element_type=F32).astype(BF16)
            for h in range(QH):
                ob[s, :, h * HD:(h + 1) * HD] = o[h * SEQ:(h + 1) * SEQ]
            return carry
        lax.fori_loop(0, DEV, attend, 0)

        def after_exchange():
            for n in SPLIT:
                if n not in AHEAD:
                    send_gu(l, n, "a")

            @pl.when(l == 0)
            def _():
                for n in AHEAD:
                    send_gu(l, n, "a")

            bytes_wait(land_wo.at[l], rs_wo.at[l])
            load_wo(l)
            bytes_wait(wo, l_sem.at[0])

        out_proj(l, after_exchange, lambda: send_gu(l, LAST, "b"))

        gather_start(by_cols)
        gather_forward(by_cols)
        send_gu(l, LAST, "a")
        send_direct(l, "d")
        send_gu(l, LAST, "d")

        @pl.when(l + 1 < LAYERS)
        def _():
            send_qkv(l + 1)

        own_last(l)
        gather_finish(by_cols)
        norm_all(gm, l)
        group_arrives(l, 0)

        def activate(prod, n, i):
            off, w = CHUNKS[n]
            gate = prod[:, :w].astype(BF16).astype(F32)
            up = prod[:, w:].astype(BF16).astype(F32)
            z = (gate * jax.nn.sigmoid(gate) * up).astype(BF16)
            zb[pl.ds(i * CHIPS, CHIPS), :, off:off + w] = z.reshape(CHIPS, SEQ, w)

        def mlp_group(g):
            chunks, slot = GROUPS[g]
            first, width = group_cols(g)
            bytes_wait(wgu.at[slot, :, pl.ds(0, width)], ld_sem.at[1 + g])

            def block(i, carry):
                rows = u[pl.ds(i * CHIPS, CHIPS)].reshape(CHIPS * SEQ, DIM)
                prod = jnp.dot(rows, wgu[slot, :, :width], preferred_element_type=F32)
                for n in chunks:
                    base = 2 * CHUNKS[n][0] - first
                    activate(prod[:, base:base + 2 * CHUNKS[n][1]], n, i)
                return carry
            lax.fori_loop(0, 2, block, 0)

        def last_term(i, k):
            depth = pl.ds(pl.multiple_of(k * PAIR, PAIR), PAIR)
            rows = u[pl.ds(i * CHIPS, CHIPS), :, depth].reshape(CHIPS * SEQ, PAIR)
            return jnp.dot(rows, wlast[depth, :], preferred_element_type=F32)

        def last_near(i, carry):
            lsum[i] = (last_term(i, chip) + last_term(i, chip_x)) + last_term(i, chip_y)
            return carry

        def last_block(i):
            activate(lsum[i] + last_term(i, chip_d), LAST, i)

        mlp_group(0)
        group_arrives(l, 1)
        mlp_group(1)
        group_arrives(l, 2)
        mlp_group(2)
        ld_d.wait()

        def before_last(i, carry):
            slots = pl.ds(i * CHIPS, CHIPS)
            z = zb[slots, :, :KPRE].reshape(CHIPS * SEQ, KPRE)
            for p in range(NP):
                prod = jnp.dot(z, wd[:KPRE, p * PW:(p + 1) * PW], preferred_element_type=F32)
                part[slots, :, p * PW:(p + 1) * PW] = prod.reshape(CHIPS, SEQ, PW)
            return carry
        lax.fori_loop(0, 2, before_last, 0)
        group_arrives(l, 3)
        bytes_wait(wlast.at[pl.ds(0, OTHER - PAIR), :], rs_gu.at[l, LAST])
        bytes_wait(wlast.at[pl.ds(0, ROWS), :], ld_sem.at[1 + len(GROUPS)])
        lax.fori_loop(0, 2, last_near, 0)
        mlp_group(3)
        bytes_wait(wlast.at[pl.ds(0, PAIR), :], rs_gu.at[l, LAST + 1])

        @pl.when(l + 1 < LAYERS)
        def _():
            last_block(0)
            last_block(1)
            reduce_scatter(False, zb, wd, KPRE, None, lambda: send_gu(l + 1, 0))
            gather_start(by_cols)
            gather_forward(by_cols)
            send_wo(l + 1)
            for n in AHEAD:
                send_gu(l + 1, n, "a")
            send_direct(l + 1, "b")
            gather_finish(by_cols)
            norm_all(ga, l + 1)

        @pl.when(l + 1 == LAYERS)
        def _():
            def residual(slot, carry):
                part[slot, :, mycols] = part[slot, :, mycols] + xcol[slot].astype(F32)
                return carry
            lax.fori_loop(0, DEV, residual, 0)
            last_block(1 - c)
            reduce_scatter(True, zb, wd, KPRE, lambda: last_block(c), lambda: None)

        bytes_wait(land_wo.at[l], ss_wo.at[l])
        bytes_wait(land_qkv.at[l, pl.ds(0, OTHER), :], ss_qkv.at[l])
        for n in range(NCH):
            bytes_wait(gu_bytes(l, n), ss_gu.at[l, n])
        return carry

    lax.fori_loop(0, LAYERS, layer, 0)
    bytes_wait(ga.at[pl.ds(0, DEV - 1)], s_gain.at[0])
    bytes_wait(gm.at[pl.ds(0, DEV - 1)], s_gain.at[1])


def solution(mesh):
    batch_spec = P(("dp", "fsdp"), None, None)
    gain_spec = P(None, "fsdp")
    proj_spec = P(None, "fsdp", None, None)
    mat_spec = P(None, "fsdp", None)
    cos, sin = rope_tables()

    def local_forward(hidden, attn_norm, w_q, w_k, w_v, w_o, mlp_norm, w_gate, w_up, w_down):
        hbm = pl.BlockSpec(memory_space=pltpu.HBM)
        vmem = pl.BlockSpec(memory_space=pltpu.VMEM)
        dma = pltpu.SemaphoreType.DMA
        out = pl.pallas_call(
            body,
            name="two_layers",
            out_shape=(pltpu.VMEM((SEQ, DIM), BF16),
                       jax.ShapeDtypeStruct((LAYERS, DEV, ROWS, QKV), BF16),
                       jax.ShapeDtypeStruct((LAYERS, DIM, QKV), BF16),
                       jax.ShapeDtypeStruct((LAYERS, DIM, 2 * FCOLS), BF16),
                       jax.ShapeDtypeStruct((LAYERS, ROWS, 2 * PAIR), BF16)),
            in_specs=[hbm] * 12,
            out_specs=(vmem, hbm, hbm, hbm, hbm),
            scratch_shapes=[
                pltpu.VMEM((2, RB, DEV * QH, HD), BF16),
                pltpu.VMEM((2, RB, DEV, HD), BF16),
                pltpu.VMEM((2, RB, DEV, HD), BF16),
                pltpu.VMEM((2, DEV, RB, QKV), BF16),
                pltpu.VMEM((DEV, SEQ, ROWS), BF16),
                pltpu.VMEM((DEV, SEQ, DIM), BF16),
                pltpu.VMEM((DEV, SEQ, DIM), F32),
                pltpu.VMEM((NP, CHIPS, 2, SEQ, ROWS), F32),
                pltpu.VMEM((NP, 2, 2, SEQ, ROWS), F32),
                pltpu.VMEM((NP, 2, SEQ, ROWS), F32),
                pltpu.VMEM((DIM, QKV), BF16),
                pltpu.VMEM((2 * ROWS, 2 * PAIR), BF16),
                pltpu.VMEM((FCOLS, DIM), BF16),
                pltpu.VMEM((2, DIM, WIDE), BF16),
                pltpu.VMEM((DIM, 2 * CHUNKS[LAST][1]), BF16),
                pltpu.VMEM((2, CHIPS * SEQ, 2 * CHUNKS[LAST][1]), F32),
                pltpu.VMEM((DEV, QH * SEQ, HD), BF16),
                pltpu.VMEM((DEV, SEQ, HD), BF16),
                pltpu.VMEM((DEV, SEQ, HD), BF16),
                pltpu.VMEM((DEV, SEQ, QCOLS), BF16),
                pltpu.VMEM((DEV, SEQ, QCOLS), BF16),
                pltpu.VMEM((DEV, SEQ, FCOLS), BF16),
                pltpu.VMEM((DEV, LAYERS, ROWS), BF16),
                pltpu.VMEM((DEV, LAYERS, ROWS), BF16),
                pltpu.VMEM((SEQ, HD), F32),
                pltpu.VMEM((SEQ, HD), F32),
                dma((LAYERS,)), dma((LAYERS,)), dma((LAYERS,)), dma((LAYERS,)), dma((2,)), dma((2,)), dma((LAYERS, NCH)), dma((LAYERS, NCH + 1)), dma((4,)), dma((7,)), dma((2 + len(GROUPS),)),
                dma((2, 3)), dma((2,)),
                dma((10,)), dma((10,)), dma((NP, 4)), dma((NP, 4)), dma((NP, 2)), dma((NP, 2)), dma((NP,)), dma((NP,)),
            ],
            compiler_params=pltpu.CompilerParams(collective_id=0, has_side_effects=True, vmem_limit_bytes=65_000_000),
        )(hidden[0], attn_norm, mlp_norm, cos, sin, w_q, w_k, w_v, w_o, w_gate, w_up, w_down)[0]
        return out[None]

    return jax.shard_map(local_forward, mesh=mesh, in_specs=(batch_spec, gain_spec, proj_spec, proj_spec, proj_spec, mat_spec, gain_spec, mat_spec, mat_spec, mat_spec), out_specs=batch_spec, check_vma=False)
```

```python
import functools

import jax
import jax.numpy as jnp
import numpy as np
from jax import lax
from jax.experimental import pallas as pl
from jax.experimental.pallas import tpu as pltpu
from jax.sharding import PartitionSpec as P

ROPE_THETA = 500000.0
NORM_EPS = 1e-5
MESH = pl.DeviceIdType.MESH
F32 = jnp.float32
BF16 = jnp.bfloat16

DEV = 8
CHIPS = 4
SEQ = 128
DIM = 3072
HALF = DIM // 2
ROWS = DIM // DEV
HD = 128
QH = 3
QCOLS = QH * HD
QKV = QCOLS + 2 * HD
FFN = 8192
FCOLS = FFN // DEV
PAIR = 2 * ROWS
CHUNKS = ((0, 128), (256, 256), (512, 256), (128, 128), (768, 128), (896, 128))
NCH = len(CHUNKS)
LAST = NCH - 1
GROUPS = (((1,), 0), ((2,), 1), ((0, 3), 0), ((4,), 1))
AHEAD = (3, 4)
WIDE = 512
SPLIT = (1, 2, 3, 4)
KPRE = CHUNKS[LAST - 1][0]
LAYERS = 2
RB = 96
NP = 4
PW = DIM // NP


def rope_tables():
    half = HD // 2
    inv_freq = np.power(np.float32(ROPE_THETA), -(np.arange(half, dtype=np.float32) * np.float32(2.0) / np.float32(HD)))
    angles = (np.arange(SEQ, dtype=np.float32)[:, None] * inv_freq.astype(np.float32)[None, :]).astype(np.float64)
    cos, sin = np.cos(angles).astype(np.float32), np.sin(angles).astype(np.float32)
    return np.concatenate([cos, cos], axis=1), np.concatenate([-sin, sin], axis=1)


def body(x_in, ga_in, gm_in, cos_in, sin_in, wq_in, wk_in, wv_in, wo_in, wg_in, wu_in, wd_in,
         out, stage_qkv, land_qkv, land_gu, land_wo,
         rq, rk, rv, st, xcol, u, part, rm, r1, r2, wqkv, wo, wd, wgu, wlast, lsum, qb, kb, vb, ob, ob2, zb, ga, gm, cos_t, sin_t,
         ss_qkv, rs_qkv, ss_wo, rs_wo, oe_s, oe_r, ss_gu, rs_gu, s_gain, l_sem, ld_sem,
         rl_in, rl_out, ag_s, ag_r, mt_s, mt_r, r1_s, r1_r, r2_s, r2_r):
    me = lax.axis_index("fsdp")
    c = me % 2
    cx = (me // 2) % 2
    cy = me // 4
    chip = me // 2

    def dev(fy, fx, fc):
        yy = 1 - cy if fy else cy
        xx = 1 - cx if fx else cx
        cc = 1 - c if fc else c
        return yy * 4 + xx * 2 + cc

    mate, xn, yn = dev(0, 0, 1), dev(0, 1, 0), dev(1, 0, 0)
    dn = dev(1, 1, 0)
    chip_x, chip_y, chip_d = xn // 2, yn // 2, dn // 2
    mycols = pl.ds(pl.multiple_of(me * ROWS, 128), ROWS)

    def axes(l):
        return yn + l * (xn - yn), xn + l * (yn - xn)
    flips = ((0, 1, 0), (1, 0, 0), (0, 1, 1), (1, 0, 1), (1, 1, 0), (1, 1, 1), (0, 0, 1))

    def remote(src, dst, ssem, rsem, target):
        return pltpu.make_async_remote_copy(src, dst, ssem, rsem, device_id={"fsdp": target}, device_id_type=MESH)

    def bytes_wait(ref, sem):
        pltpu.make_async_copy(ref, ref, sem).wait()

    barrier = pltpu.get_barrier_semaphore()
    for f in flips:
        pl.semaphore_signal(barrier, inc=1, device_id={"fsdp": dev(*f)}, device_id_type=MESH)
    pl.semaphore_wait(barrier, DEV - 1)

    def targets(l, which):
        if which is None:
            return [(dev(*f), f[0] and f[1]) for f in flips]
        an, bn = axes(l)
        e = {"a": an, "b": bn, "d": dn}[which]
        return [(e, which == "d"), (e + 1 - 2 * c, which == "d")] + ([(mate, False)] if which == "b" else [])

    def send_qkv(l, which=None):
        for e, diagonal in targets(l, which):
            remote(stage_qkv.at[l, e],
                   land_qkv.at[l, pl.ds(pl.multiple_of(me * ROWS, ROWS), ROWS), :],
                   ss_qkv.at[l], rs_qkv.at[l], e).start()

    def send_wo(l):
        an = axes(l)[0]
        for k, to in ((0, an // 2), (1, chip_d)):
            remote(wo_in.at[l, :, pl.ds(pl.multiple_of(to * PAIR, 128), PAIR)], land_wo.at[l, :, pl.ds(k * PAIR, PAIR)],
                   ss_wo.at[l], rs_wo.at[l], an).start()

    def load_wo(l):
        for k, of in ((0, chip), (1, axes(l)[1] // 2)):
            pltpu.make_async_copy(wo_in.at[l, :, pl.ds(pl.multiple_of(of * PAIR, 128), PAIR)],
                                  wo.at[pl.ds(0, ROWS), pl.ds(k * PAIR, PAIR)], l_sem.at[0]).start()
        pltpu.make_async_copy(land_wo.at[l], wo.at[pl.ds(ROWS, ROWS), :], l_sem.at[0]).start()

    def send_gu(l, n, which=None):
        off, w = CHUNKS[n]
        rows = pl.ds(pl.multiple_of(me * ROWS, ROWS), ROWS)
        for e, diagonal in targets(l, which):
            cols = pl.ds(pl.multiple_of(e * FCOLS + off, 128), w)
            for src, k in ((wg_in, 0), (wu_in, 1)):
                dst = wlast.at[rows, pl.ds(k * w, w)] if n == LAST else land_gu.at[l, rows, pl.ds(2 * off + k * w, w)]
                got = n + 1 if n == LAST and diagonal else n
                remote(src.at[l, :, cols], dst, ss_gu.at[l, n], rs_gu.at[l, got], e).start()

    def gu_bytes(l, n):
        off, w = CHUNKS[n]
        if n == LAST:
            return wlast.at[pl.ds(0, OTHER), :]
        return land_gu.at[l, pl.ds(0, OTHER), pl.ds(2 * off, 2 * w)]

    OTHER = (DEV - 1) * ROWS

    def load_qkv(l):
        for f in flips:
            rows = pl.ds(pl.multiple_of(dev(*f) * ROWS, ROWS), ROWS)
            pltpu.make_async_copy(land_qkv.at[l, rows, :], wqkv.at[rows, :], ld_sem.at[0]).start()
        mine = pl.ds(pl.multiple_of(me * ROWS, ROWS), ROWS)
        pltpu.make_async_copy(stage_qkv.at[l, me], wqkv.at[mine, :], ld_sem.at[0]).start()

    def own_gu(l, n, dst_of, sem):
        off, w = CHUNKS[n]
        cols = pl.ds(pl.multiple_of(me * FCOLS + off, 128), w)
        for src, k in ((wg_in, 0), (wu_in, 1)):
            pltpu.make_async_copy(src.at[l, :, cols], dst_of(k * w, w), sem).start()

    def own_last(l):
        mine = pl.ds(pl.multiple_of(me * ROWS, ROWS), ROWS)
        own_gu(l, LAST, lambda at, w: wlast.at[mine, pl.ds(at, w)], ld_sem.at[1 + len(GROUPS)])

    def group_cols(g):
        chunks = GROUPS[g][0]
        return 2 * CHUNKS[chunks[0]][0], 2 * sum(CHUNKS[n][1] for n in chunks)

    def group_arrives(l, g):
        chunks, slot = GROUPS[g]
        first, width = group_cols(g)
        sem = ld_sem.at[1 + g]
        for n in chunks:
            bytes_wait(gu_bytes(l, n), rs_gu.at[l, n])
        for f in flips:
            rows = pl.ds(pl.multiple_of(dev(*f) * ROWS, ROWS), ROWS)
            pltpu.make_async_copy(land_gu.at[l, rows, pl.ds(first, width)], wgu.at[slot, rows, pl.ds(0, width)], sem).start()
        mine = pl.ds(pl.multiple_of(me * ROWS, ROWS), ROWS)
        for n in chunks:
            base = 2 * CHUNKS[n][0] - first
            own_gu(l, n, lambda at, w, base=base: wgu.at[slot, mine, pl.ds(base + at, w)], sem)

    def relayout(l):
        def fetch(i):
            slot = i % 2
            rows = pl.ds(pl.multiple_of(i * RB, RB), RB)
            return [pltpu.make_async_copy(src.at[l, rows], dst.at[slot], rl_in.at[slot, k])
                    for k, (src, dst) in enumerate(((wq_in, rq), (wk_in, rk), (wv_in, rv)))]

        def put(i):
            slot = i % 2
            rows = pl.ds(pl.multiple_of(i * RB, RB), RB)
            return pltpu.make_async_copy(st.at[slot], stage_qkv.at[l, :, rows, :], rl_out.at[slot])

        steps = ROWS // RB
        for cp in fetch(0):
            cp.start()

        def step(i, carry):
            slot = i % 2

            @pl.when(i + 1 < steps)
            def _():
                for cp in fetch(i + 1):
                    cp.start()
            for cp in fetch(i):
                cp.wait()

            @pl.when(i >= 2)
            def _():
                put(i - 2).wait()

            def block(b, carry):
                rows = pl.ds(pl.multiple_of(b * 16, 16), 16)
                q = rq[slot, rows].astype(F32).reshape(16, DEV * QCOLS).astype(BF16)
                k = rk[slot, rows].astype(F32).reshape(16, DEV * HD).astype(BF16)
                v = rv[slot, rows].astype(F32).reshape(16, DEV * HD).astype(BF16)
                for e in range(DEV):
                    st[slot, e, rows, :QCOLS] = q[:, e * QCOLS:(e + 1) * QCOLS]
                    st[slot, e, rows, QCOLS:QCOLS + HD] = k[:, e * HD:(e + 1) * HD]
                    st[slot, e, rows, QCOLS + HD:] = v[:, e * HD:(e + 1) * HD]
                return carry
            lax.fori_loop(0, RB // 16, block, 0)
            put(i).start()
            return carry
        lax.fori_loop(0, steps, step, 0)
        put(steps - 2).wait()
        put(steps - 1).wait()

    my_slot = c * CHIPS + chip

    def norm_all(gains, l):
        def one(i, carry):
            slot = i // (SEQ // 16)
            rows = pl.ds(pl.multiple_of((i % (SEQ // 16)) * 16, 16), 16)
            wide = u[slot, rows, :].astype(F32)
            inv = lax.rsqrt(jnp.mean(wide * wide, axis=-1, keepdims=True) + NORM_EPS)
            for s in range(DEV):
                cols = slice(s * ROWS, (s + 1) * ROWS)
                both = gains[s].astype(F32)
                g = jnp.where(l == 0, both[0:1], both[1:2])
                u[slot, rows, cols] = (wide[:, cols] * inv * g).astype(BF16)
            return carry
        lax.fori_loop(0, DEV * SEQ // 16, one, 0)

    def by_rows(who, half):
        slot = c * CHIPS + {"me": chip, "x": chip_x, "y": chip_y, "d": chip_d}[who]
        return u.at[slot] if half is None else u.at[slot, :, pl.ds(half * HALF, HALF)]

    def by_cols(who, half):
        e = {"me": me, "x": xn, "y": yn, "d": dn}[who]
        cols = pl.ds(pl.multiple_of(e * ROWS, 128), ROWS)
        return u.at[:, :, cols] if half is None else u.at[pl.ds(half * CHIPS, CHIPS), :, cols]

    def u_copy(ref, k, target):
        return remote(ref, ref, ag_s.at[k], ag_r.at[k], target)

    def gather_start(at):
        u_copy(at("me", 0), 0, xn).start()
        u_copy(at("me", 1), 1, yn).start()
        u_copy(at("me", 1), 2, xn).start()
        u_copy(at("me", 0), 3, yn).start()
        u_copy(at("me", None), 6, mate).start()

    def gather_forward(at):
        u_copy(at("x", 0), 0, xn).wait_recv()
        u_copy(at("x", 0), 4, yn).start()
        u_copy(at("y", 1), 1, yn).wait_recv()
        u_copy(at("y", 1), 5, xn).start()

    def gather_finish(at):
        u_copy(at("x", 1), 2, xn).wait_recv()
        u_copy(at("x", None), 7, mate).start()
        u_copy(at("y", 0), 3, yn).wait_recv()
        u_copy(at("y", None), 8, mate).start()
        u_copy(at("d", 0), 4, yn).wait_recv()
        u_copy(at("d", 1), 5, xn).wait_recv()
        u_copy(at("d", None), 9, mate).start()
        for k in (6, 7, 8, 9):
            u_copy(at("me", None), k, mate).wait_recv()
        for k in range(6):
            u_copy(at("me", 0), k, xn).wait_send()
        for k in (6, 7, 8, 9):
            u_copy(at("me", None), k, mate).wait_send()

    def keep(slot, total):
        new = (xcol[slot].astype(F32) + total).astype(BF16)
        xcol[slot] = new
        u[slot, :, mycols] = new

    def out_proj(l, after_exchange, after_sums):
        an, bn = axes(l)

        def o_copy(g):
            return remote(ob.at[pl.ds(g * CHIPS, CHIPS)], ob2.at[pl.ds(g * CHIPS, CHIPS)], oe_s.at[g], oe_r.at[g], an)

        def mate_copy(p, b):
            return remote(part.at[pl.ds(2 * p, 2), :, pl.ds(pl.multiple_of(b * PAIR + (1 - c) * ROWS, 128), ROWS)], rm.at[p, b],
                          mt_s.at[p, b], mt_r.at[p, b], mate)

        def sums(p):
            return remote(part.at[pl.ds(2 * p, 2), :, pl.ds(pl.multiple_of(PAIR + c * ROWS, 128), ROWS)], r1.at[p, 0],
                          r1_s.at[p, 0], r1_r.at[p, 0], bn)

        def fold(p):
            mate_copy(p, 1).wait_recv()
            for t in range(2):
                cols = pl.ds(pl.multiple_of(PAIR + c * ROWS, 128), ROWS)
                part[2 * p + t, :, cols] = part[2 * p + t, :, cols] + rm[p, 1, t]
            sums(p).start()

        for g in range(2):
            o_copy(g).start()
        after_exchange()
        for p in range(NP):
            if p % 2 == 0:
                o_copy(p // 2).wait_recv()
            a = jnp.concatenate([r[pl.ds(2 * p, 2)].reshape(2 * SEQ, QCOLS) for r in (ob, ob2)], axis=1)
            for b in (1, 0):
                prod = jnp.dot(a, wo[:, b * PAIR:(b + 1) * PAIR], preferred_element_type=F32)
                part[pl.ds(2 * p, 2), :, b * PAIR:(b + 1) * PAIR] = prod.reshape(2, SEQ, PAIR)
                mate_copy(p, b).start()
            if p:
                fold(p - 1)
        fold(NP - 1)
        after_sums()
        for p in range(NP):
            mate_copy(p, 0).wait_recv()
            sums(p).wait_recv()
            for t in range(2):
                keep(2 * p + t, (part[2 * p + t, :, pl.ds(pl.multiple_of(c * ROWS, 128), ROWS)] + rm[p, 0, t]) + r1[p, 0, t])
        for g in range(2):
            o_copy(g).wait_send()
        for p in range(NP):
            for b in range(2):
                mate_copy(p, b).wait_send()
            sums(p).wait_send()

    def reduce_scatter(rows_form, act, rhs, k0, between, then):
        own, other = c, 1 - c
        order = ((chip_d, chip_x, chip_y, chip), (chip_d, chip_y, chip_x, chip))
        first = (xn, yn)
        second = (yn, xn)

        def sub(p, j, core, t):
            if rows_form:
                return core * CHIPS + j, pl.ds(p * PW + t * ROWS, ROWS)
            return 2 * p + t, pl.ds(pl.multiple_of(j * PAIR + core * ROWS, 128), ROWS)

        def pieces(p, j, core, dst, ssem, rsem, target):
            for t in range(2):
                slot, cols = sub(p, j, core, t)
                remote(part.at[slot, :, cols], dst.at[t], ssem, rsem, target).start()

        def unit(sem):
            bytes_wait(r2.at[0], sem)

        def send_mate(p, k):
            j = order[p % 2][k]
            pieces(p, j, other, rm.at[p, j], mt_s.at[p, k], mt_r.at[p, k], mate)

        def fold(p, k, extra):
            j = order[p % 2][k]
            for t in range(2):
                slot, cols = sub(p, j, own, t)
                total = part[slot, :, cols] + rm[p, j, t]
                part[slot, :, cols] = total if extra is None else total + extra[t]

        def products(p, grp, ks):
            slots = [grp * CHIPS + order[p % 2][k] for k in ks]
            a = jnp.concatenate([act[slot, :, k0:] for slot in slots], axis=0)
            cols = slice(p * PW, (p + 1) * PW)
            prod = jnp.dot(a, rhs[k0:, cols], preferred_element_type=F32)
            for i, slot in enumerate(slots):
                part[slot, :, cols] = part[slot, :, cols] + prod[i * SEQ:(i + 1) * SEQ]

        def column_products(p, k):
            cols = pl.ds(pl.multiple_of(order[p % 2][k] * PAIR, 128), PAIR)
            slots = pl.ds(2 * p, 2)
            prod = jnp.dot(act[slots, :, k0:].reshape(2 * SEQ, FCOLS - k0), rhs[k0:, cols], preferred_element_type=F32)
            part[slots, :, cols] = part[slots, :, cols] + prod.reshape(2, SEQ, PAIR)

        for pair in range(NP // 2):
            both = (2 * pair, 2 * pair + 1)
            for p in both:
                if rows_form:
                    products(p, other, (0, 1))
                else:
                    column_products(p, 0)
                send_mate(p, 0)
            for p in both:
                if not rows_form:
                    column_products(p, 1)
                send_mate(p, 1)
            if pair == 0 and between is not None:
                between()
            if rows_form:
                for p in both:
                    products(p, own, (0, 1))
            for k in (0, 1):
                for p in both:
                    unit(mt_r.at[p, k])
                    fold(p, k, None)
                    pieces(p, order[p % 2][k], own, r1.at[p, k], r1_s.at[p, k], r1_r.at[p, k], first[p % 2])
        for p in range(NP):
            if rows_form:
                products(p, other, (2, 3))
            for k in (2, 3):
                if not rows_form:
                    column_products(p, k)
                send_mate(p, k)
            if rows_form:
                products(p, own, (2, 3))
        for p in range(NP):
            unit(mt_r.at[p, 2])
            unit(r1_r.at[p, 0])
            fold(p, 2, r1.at[p, 0])
            pieces(p, order[p % 2][2], own, r2.at[p], r2_s.at[p], r2_r.at[p], second[p % 2])
        for p in range(NP):
            if p == 0:
                then()
            unit(mt_r.at[p, 3])
            unit(r1_r.at[p, 1])
            unit(r2_r.at[p])
            for t in range(2):
                slot, cols = sub(p, chip, own, t)
                total = (part[slot, :, cols] + rm[p, chip, t]) + (r1[p, 1, t] + r2[p, t])
                if rows_form:
                    out[:, cols] = total.astype(BF16)
                else:
                    keep(slot, total)
        for p in range(NP):
            for k in range(4):
                unit(mt_s.at[p, k])
            for k in range(2):
                unit(r1_s.at[p, k])
            unit(r2_s.at[p])

    def send_direct(l, which):
        for n in SPLIT:
            send_gu(l, n, which)

    send_gu(0, 0)
    starts = [pltpu.make_async_copy(src, dst, l_sem.at[2 + k]) for k, (src, dst) in enumerate(
        ((x_in, u.at[my_slot]), (ga_in, ga.at[me]), (gm_in, gm.at[me]), (cos_in, cos_t), (sin_in, sin_t)))]
    for cp in starts:
        cp.start()
    for cp in starts:
        cp.wait()
    gather_start(by_rows)
    for src, dst, k in ((ga_in, ga, 0), (gm_in, gm, 1)):
        for f in flips:
            remote(src, dst.at[me], s_gain.at[k], s_gain.at[2 + k], dev(*f)).start()
    relayout(0)
    gather_forward(by_rows)
    send_qkv(0)
    send_wo(0)
    send_direct(0, "b")
    relayout(1)
    gather_finish(by_rows)
    bytes_wait(ga.at[pl.ds(0, DEV - 1)], s_gain.at[2])
    bytes_wait(gm.at[pl.ds(0, DEV - 1)], s_gain.at[3])

    def column_block(slot, carry):
        xcol[slot] = u[slot, :, mycols]
        return carry
    lax.fori_loop(0, DEV, column_block, 0)
    norm_all(ga, 0)

    def layer(l, carry):
        ld_d = pltpu.make_async_copy(wd_in.at[l], wd, l_sem.at[1])
        ld_d.start()
        bytes_wait(land_qkv.at[l, pl.ds(0, OTHER), :], rs_qkv.at[l])
        load_qkv(l)
        bytes_wait(wqkv, ld_sem.at[0])

        def qkv_block(i, carry):
            prod = jnp.dot(u[pl.ds(i * 2, 2)].reshape(2 * SEQ, DIM), wqkv[...], preferred_element_type=F32)
            cos, sin = cos_t[...], sin_t[...]
            for s in range(2):
                rows = slice(s * SEQ, (s + 1) * SEQ)
                for h in range(QH + 1):
                    head = prod[rows, h * HD:(h + 1) * HD]
                    rot = (head * cos + pltpu.roll(head, HD // 2, 1) * sin).astype(BF16)
                    if h < QH:
                        qb[i * 2 + s, pl.ds(h * SEQ, SEQ), :] = rot
                    else:
                        kb[i * 2 + s] = rot
                vb[i * 2 + s] = prod[rows, (QH + 1) * HD:].astype(BF16)
            return carry
        lax.fori_loop(0, DEV // 2, qkv_block, 0)

        def attend(s, carry):
            scores = lax.dot_general(qb[s], kb[s], (((1,), (1,)), ((), ())), preferred_element_type=F32) * HD ** -0.5
            row = lax.broadcasted_iota(jnp.int32, (QH * SEQ, SEQ), 0) % SEQ
            col = lax.broadcasted_iota(jnp.int32, (QH * SEQ, SEQ), 1)
            scores = jnp.where(row >= col, scores, -jnp.inf)
            e = jnp.exp(scores - jnp.max(scores, axis=-1, keepdims=True))
            probs = (e / jnp.sum(e, axis=-1, keepdims=True)).astype(BF16)
            o = jnp.dot(probs, vb[s], preferred_element_type=F32).astype(BF16)
            for h in range(QH):
                ob[s, :, h * HD:(h + 1) * HD] = o[h * SEQ:(h + 1) * SEQ]
            return carry
        lax.fori_loop(0, DEV, attend, 0)

        def after_exchange():
            for n in SPLIT:
                if n not in AHEAD:
                    send_gu(l, n, "a")

            @pl.when(l == 0)
            def _():
                for n in AHEAD:
                    send_gu(l, n, "a")

            bytes_wait(land_wo.at[l], rs_wo.at[l])
            load_wo(l)
            bytes_wait(wo, l_sem.at[0])

        out_proj(l, after_exchange, lambda: send_gu(l, LAST, "b"))

        gather_start(by_cols)
        gather_forward(by_cols)
        send_gu(l, LAST, "a")
        send_direct(l, "d")
        send_gu(l, LAST, "d")

        @pl.when(l + 1 < LAYERS)
        def _():
            send_qkv(l + 1)

        own_last(l)
        gather_finish(by_cols)
        norm_all(gm, l)
        group_arrives(l, 0)

        def activate(prod, n, i):
            off, w = CHUNKS[n]
            gate = prod[:, :w].astype(BF16).astype(F32)
            up = prod[:, w:].astype(BF16).astype(F32)
            z = (gate * jax.nn.sigmoid(gate) * up).astype(BF16)
            zb[pl.ds(i * CHIPS, CHIPS), :, off:off + w] = z.reshape(CHIPS, SEQ, w)

        def mlp_group(g):
            chunks, slot = GROUPS[g]
            first, width = group_cols(g)
            bytes_wait(wgu.at[slot, :, pl.ds(0, width)], ld_sem.at[1 + g])

            def block(i, carry):
                rows = u[pl.ds(i * CHIPS, CHIPS)].reshape(CHIPS * SEQ, DIM)
                prod = jnp.dot(rows, wgu[slot, :, :width], preferred_element_type=F32)
                for n in chunks:
                    base = 2 * CHUNKS[n][0] - first
                    activate(prod[:, base:base + 2 * CHUNKS[n][1]], n, i)
                return carry
            lax.fori_loop(0, 2, block, 0)

        def last_term(i, k):
            depth = pl.ds(pl.multiple_of(k * PAIR, PAIR), PAIR)
            rows = u[pl.ds(i * CHIPS, CHIPS), :, depth].reshape(CHIPS * SEQ, PAIR)
            return jnp.dot(rows, wlast[depth, :], preferred_element_type=F32)

        def last_near(i, carry):
            lsum[i] = (last_term(i, chip) + last_term(i, chip_x)) + last_term(i, chip_y)
            return carry

        def last_block(i):
            activate(lsum[i] + last_term(i, chip_d), LAST, i)

        mlp_group(0)
        group_arrives(l, 1)
        mlp_group(1)
        group_arrives(l, 2)
        mlp_group(2)
        ld_d.wait()

        def before_last(i, carry):
            slots = pl.ds(i * CHIPS, CHIPS)
            z = zb[slots, :, :KPRE].reshape(CHIPS * SEQ, KPRE)
            for p in range(NP):
                prod = jnp.dot(z, wd[:KPRE, p * PW:(p + 1) * PW], preferred_element_type=F32)
                part[slots, :, p * PW:(p + 1) * PW] = prod.reshape(CHIPS, SEQ, PW)
            return carry
        lax.fori_loop(0, 2, before_last, 0)
        group_arrives(l, 3)
        bytes_wait(wlast.at[pl.ds(0, OTHER - PAIR), :], rs_gu.at[l, LAST])
        bytes_wait(wlast.at[pl.ds(0, ROWS), :], ld_sem.at[1 + len(GROUPS)])
        lax.fori_loop(0, 2, last_near, 0)
        mlp_group(3)
        bytes_wait(wlast.at[pl.ds(0, PAIR), :], rs_gu.at[l, LAST + 1])

        @pl.when(l + 1 < LAYERS)
        def _():
            last_block(0)
            last_block(1)
            reduce_scatter(False, zb, wd, KPRE, None, lambda: send_gu(l + 1, 0))
            gather_start(by_cols)
            gather_forward(by_cols)
            send_wo(l + 1)
            for n in AHEAD:
                send_gu(l + 1, n, "a")
            send_direct(l + 1, "b")
            gather_finish(by_cols)
            norm_all(ga, l + 1)

        @pl.when(l + 1 == LAYERS)
        def _():
            def residual(slot, carry):
                part[slot, :, mycols] = part[slot, :, mycols] + xcol[slot].astype(F32)
                return carry
            lax.fori_loop(0, DEV, residual, 0)
            last_block(1 - c)
            reduce_scatter(True, zb, wd, KPRE, lambda: last_block(c), lambda: None)

        bytes_wait(land_wo.at[l], ss_wo.at[l])
        bytes_wait(land_qkv.at[l, pl.ds(0, OTHER), :], ss_qkv.at[l])
        for n in range(NCH):
            bytes_wait(gu_bytes(l, n), ss_gu.at[l, n])
        return carry

    lax.fori_loop(0, LAYERS, layer, 0)
    bytes_wait(ga.at[pl.ds(0, DEV - 1)], s_gain.at[0])
    bytes_wait(gm.at[pl.ds(0, DEV - 1)], s_gain.at[1])


def solution(mesh):
    batch_spec = P(("dp", "fsdp"), None, None)
    gain_spec = P(None, "fsdp")
    proj_spec = P(None, "fsdp", None, None)
    mat_spec = P(None, "fsdp", None)
    cos, sin = rope_tables()

    def local_forward(hidden, attn_norm, w_q, w_k, w_v, w_o, mlp_norm, w_gate, w_up, w_down):
        hbm = pl.BlockSpec(memory_space=pltpu.HBM)
        vmem = pl.BlockSpec(memory_space=pltpu.VMEM)
        dma = pltpu.SemaphoreType.DMA
        out = pl.pallas_call(
            body,
            name="two_layers",
            out_shape=(pltpu.VMEM((SEQ, DIM), BF16),
                       jax.ShapeDtypeStruct((LAYERS, DEV, ROWS, QKV), BF16),
                       jax.ShapeDtypeStruct((LAYERS, DIM, QKV), BF16),
                       jax.ShapeDtypeStruct((LAYERS, DIM, 2 * FCOLS), BF16),
                       jax.ShapeDtypeStruct((LAYERS, ROWS, 2 * PAIR), BF16)),
            in_specs=[hbm] * 12,
            out_specs=(vmem, hbm, hbm, hbm, hbm),
            scratch_shapes=[
                pltpu.VMEM((2, RB, DEV * QH, HD), BF16),
                pltpu.VMEM((2, RB, DEV, HD), BF16),
                pltpu.VMEM((2, RB, DEV, HD), BF16),
                pltpu.VMEM((2, DEV, RB, QKV), BF16),
                pltpu.VMEM((DEV, SEQ, ROWS), BF16),
                pltpu.VMEM((DEV, SEQ, DIM), BF16),
                pltpu.VMEM((DEV, SEQ, DIM), F32),
                pltpu.VMEM((NP, CHIPS, 2, SEQ, ROWS), F32),
                pltpu.VMEM((NP, 2, 2, SEQ, ROWS), F32),
                pltpu.VMEM((NP, 2, SEQ, ROWS), F32),
                pltpu.VMEM((DIM, QKV), BF16),
                pltpu.VMEM((2 * ROWS, 2 * PAIR), BF16),
                pltpu.VMEM((FCOLS, DIM), BF16),
                pltpu.VMEM((2, DIM, WIDE), BF16),
                pltpu.VMEM((DIM, 2 * CHUNKS[LAST][1]), BF16),
                pltpu.VMEM((2, CHIPS * SEQ, 2 * CHUNKS[LAST][1]), F32),
                pltpu.VMEM((DEV, QH * SEQ, HD), BF16),
                pltpu.VMEM((DEV, SEQ, HD), BF16),
                pltpu.VMEM((DEV, SEQ, HD), BF16),
                pltpu.VMEM((DEV, SEQ, QCOLS), BF16),
                pltpu.VMEM((DEV, SEQ, QCOLS), BF16),
                pltpu.VMEM((DEV, SEQ, FCOLS), BF16),
                pltpu.VMEM((DEV, LAYERS, ROWS), BF16),
                pltpu.VMEM((DEV, LAYERS, ROWS), BF16),
                pltpu.VMEM((SEQ, HD), F32),
                pltpu.VMEM((SEQ, HD), F32),
                dma((LAYERS,)), dma((LAYERS,)), dma((LAYERS,)), dma((LAYERS,)), dma((2,)), dma((2,)), dma((LAYERS, NCH)), dma((LAYERS, NCH + 1)), dma((4,)), dma((7,)), dma((2 + len(GROUPS),)),
                dma((2, 3)), dma((2,)),
                dma((10,)), dma((10,)), dma((NP, 4)), dma((NP, 4)), dma((NP, 2)), dma((NP, 2)), dma((NP,)), dma((NP,)),
            ],
            compiler_params=pltpu.CompilerParams(collective_id=0, has_side_effects=True, vmem_limit_bytes=65_000_000),
        )(hidden[0], attn_norm, mlp_norm, cos, sin, w_q, w_k, w_v, w_o, w_gate, w_up, w_down)[0]
        return out[None]

    return jax.shard_map(local_forward, mesh=mesh, in_specs=(batch_spec, gain_spec, proj_spec, proj_spec, proj_spec, mat_spec, gain_spec, mat_spec, mat_spec, mat_spec), out_specs=batch_spec, check_vma=False)
```
